256 devices in a mesh: px: 8 (over z_lo, core), pz: 32 (over z_hi, y, x).
Axes of the slice: x: 4, y: 4, z: 8 (z_hi: 2, z_lo: 4; z = z_hi * 4 + z_lo), core: 2. Of those that a mesh axis runs over, the one named last changes fastest.
Arguments:
- velocity: float32 [3, 256, 64, 1024], P(None, 'pz', None, 'px'), may hold values from -8 to 8, as said below
- filter_inverse: float32 [256, 256], replicated, may hold values from 0 to 2, as said below
- filter_block: int32 [256], replicated, may hold values from 0 to 7, never falling along the last dimension, each value on 1 to 128 neighbouring positions
- plane_bin: int32 [256], replicated, may hold values from 0 to 63, never falling along the last dimension, each value on 1 to 16 neighbouring positions
Outputs:
- leonard: float32 [6, 256, 64, 1024], P(None, 'pz', None, 'px')
- viscosity: float32 [256, 64, 1024], P('pz', None, 'px')
- coefficient: float32 [256], replicated
The draws below stay inside these ranges and needn't reach their ends.
Inputs may be any that keep to these rules, and one draw needn't show every extreme that they name: `velocity`: each component is a rough random field. `filter_inverse`: entries are positive. `filter_block`: never falls along the planes; each of the 8 blocks holds 1 to 128 consecutive planes, one exactly 128. `plane_bin`: never falls along the planes; each of the 64 bins holds 1 to 16 consecutive planes, one exactly 16.
All inputs are finite; a program needn't handle non-finite values.
Results may differ from the reference program's by a relative error of at most 0.0003.
Values sent between devices are 32-bit elements; how exact they have to be, the bound alone decides.
A program may use at most 128 MiB of HBM per device.

```python
import math
import jax
import jax.numpy as jnp
import numpy as np
from jax import lax

NY = 256
NFB = 8
FBMOST = 128
NBIN = 64
BINMOST = 16
NX = 1024
NZ = 64


def draw_velocity(key, part):
    noise_key, scale_key = jax.random.split(jax.random.fold_in(key, 11))
    base = jax.random.normal(noise_key, (3, NY, NZ, NX), jnp.float32)
    amplitude = jnp.exp(jax.random.uniform(scale_key, (1, 1, NZ, NX // 8), jnp.float32, -0.7, 0.7))
    amplitude = jnp.repeat(amplitude, 8, axis=3)
    return jnp.clip(base * amplitude, -8.0, 8.0)


def draw_filter_inverse(key, part):
    entry_key = jax.random.fold_in(key, 23)
    rows = jnp.arange(NY, dtype=jnp.float32)
    distance = jnp.abs(rows[:, None] - rows[None, :])
    factors = jax.random.uniform(entry_key, (NY, NY), jnp.float32, 0.5, 1.5)
    return jnp.exp(-distance / 256.0) * factors


def split_up(number_of, total, bound, slope):
    loads = [(1 << 20) // math.isqrt(grade ** slope) + 1 for grade in range(2, number_of + 1)]
    spare, holding = total - bound - (number_of - 1), [1] * (number_of - 1)
    while spare > 0:
        free = [i for i in range(number_of - 1) if holding[i] < bound]
        whole, budget = sum([loads[i] for i in free]), spare
        for i in free:
            extra = min(bound - holding[i], max(1, budget * loads[i] // whole), spare)
            holding[i] = holding[i] + extra
            spare = spare - extra
    return np.array([bound] + holding)


def ragged_sizes(rng, count, total, reach, lean):
    if count == 2:
        one = jax.random.randint(rng, (), max(1, total - reach), min(reach, total - 1) + 1)
        return jnp.stack([one, total - one])
    sizes = jnp.asarray(split_up(count, total, reach, lean), jnp.int32)
    couples = (count - 1) // 2
    donor, sink = sizes[1:1 + 2 * couples:2], sizes[2:2 + 2 * couples:2]
    room = jnp.minimum(donor - 1, reach - sink)
    shifted = jax.random.randint(jax.random.fold_in(rng, 1), (couples,), 0, 1 << 20) % (room + 1)
    sizes = sizes.at[1:1 + 2 * couples:2].set(donor - shifted).at[2:2 + 2 * couples:2].set(sink + shifted)
    return sizes[jax.random.permutation(jax.random.fold_in(rng, 2), count)]


def setup_inputs(seed: int = 0) -> dict:
    keys = jax.random.split(jax.random.key(seed), 5)
    velocity = draw_velocity(jax.random.fold_in(keys[4], 71), 0)
    filter_inverse = draw_filter_inverse(jax.random.fold_in(keys[4], 71), 0)
    filter_block = jnp.searchsorted(jnp.cumsum(ragged_sizes(keys[2], NFB, NY, FBMOST, 1)), jnp.arange(NY), side="right").astype(jnp.int32)
    plane_bin = jnp.searchsorted(jnp.cumsum(ragged_sizes(keys[3], NBIN, NY, BINMOST, 1)), jnp.arange(NY), side="right").astype(jnp.int32)
    return dict(velocity=velocity, filter_inverse=filter_inverse, filter_block=filter_block, plane_bin=plane_bin)


def block_weights(filter_inverse, filter_block):
    same = (filter_block[:, None] == filter_block[None, :]).astype(jnp.float32)
    masked = filter_inverse * same
    return masked / lax.optimization_barrier(jnp.sum(masked, axis=1, keepdims=True))

def quantities(padded):
    centre = padded[:, 1:-1, 1:-1, 1:-1]
    along_y = (padded[:, 2:, 1:-1, 1:-1] - padded[:, :-2, 1:-1, 1:-1]) * 0.5
    along_z = (padded[:, 1:-1, 2:, 1:-1] - padded[:, 1:-1, :-2, 1:-1]) * 0.5
    along_x = (padded[:, 1:-1, 1:-1, 2:] - padded[:, 1:-1, 1:-1, :-2]) * 0.5
    strain = jnp.stack([along_x[0], along_y[1], along_z[2], 0.5 * (along_y[0] + along_x[1]), 0.5 * (along_z[0] + along_x[2]), 0.5 * (along_z[1] + along_y[2])])
    magnitude = jnp.sqrt(2.0 * lax.optimization_barrier(jnp.sum(strain[:3] * strain[:3], axis=0)) + 4.0 * lax.optimization_barrier(jnp.sum(strain[3:] * strain[3:], axis=0)))
    products = jnp.stack([centre[0] * centre[0], centre[1] * centre[1], centre[2] * centre[2], centre[0] * centre[1], centre[0] * centre[2], centre[1] * centre[2]])
    fields = jnp.concatenate([centre, strain, products, magnitude[None] * strain], axis=0)
    along = (fields[..., :-2] + 2.0 * fields[..., 1:-1] + fields[..., 2:]) * 0.25
    boxed = (along[:, :, :-2] + 2.0 * along[:, :, 1:-1] + along[:, :, 2:]) * 0.25
    return (boxed, magnitude[:, 1:-1, 1:-1])

def contract(filtered):
    speed = filtered[0:3]
    strain = filtered[3:9]
    products = filtered[9:15]
    scaled = filtered[15:21]
    leonard = products - jnp.stack([speed[0] * speed[0], speed[1] * speed[1], speed[2] * speed[2], speed[0] * speed[1], speed[0] * speed[2], speed[1] * speed[2]])
    fmag = jnp.sqrt(2.0 * lax.optimization_barrier(jnp.sum(strain[:3] * strain[:3], axis=0)) + 4.0 * lax.optimization_barrier(jnp.sum(strain[3:] * strain[3:], axis=0)))
    model = scaled - 4.0 * fmag[None] * strain
    weights = jnp.array([1.0, 1.0, 1.0, 2.0, 2.0, 2.0], jnp.float32).reshape(6, 1, 1, 1)
    product_lm = lax.optimization_barrier(jnp.sum(weights * leonard * model, axis=0))
    product_mm = lax.optimization_barrier(jnp.sum(weights * model * model, axis=0))
    return (leonard, product_lm, product_mm)

def reference(velocity, filter_inverse, filter_block, plane_bin):
    weights = block_weights(filter_inverse, filter_block)

    def one_plane(plane):
        indices = ((plane + jnp.arange(-2, 3, dtype=jnp.int32)) % NZ).astype(jnp.int32)
        window = jnp.take(velocity, indices, axis=2)
        window = jnp.pad(window, ((0, 0), (1, 1), (0, 0), (0, 0)))
        window = jnp.concatenate([window[..., -2:], window, window[..., :2]], axis=3)
        boxed, magnitude = quantities(window)
        filtered = jnp.einsum('ab,kbzx->kazx', weights, boxed, precision=lax.Precision.HIGHEST)
        leonard, product_lm, product_mm = contract(filtered)
        return (leonard[:, :, 0, :], lax.optimization_barrier(jnp.sum(product_lm, axis=(1, 2))), lax.optimization_barrier(jnp.sum(product_mm, axis=(1, 2))), magnitude[:, 0, :])
    leonard, plane_lm, plane_mm, magnitude = lax.map(one_plane, jnp.arange(NZ, dtype=jnp.int32))
    plane_lm = lax.optimization_barrier(jnp.sum(plane_lm, axis=0))
    plane_mm = lax.optimization_barrier(jnp.sum(plane_mm, axis=0))
    onehot = (plane_bin[:, None] == jnp.arange(NBIN, dtype=jnp.int32)[None, :]).astype(jnp.float32)
    numer = jnp.dot(plane_lm, onehot, precision=lax.Precision.HIGHEST)
    denom = jnp.dot(plane_mm, onehot, precision=lax.Precision.HIGHEST)
    per_bin = numer / jnp.maximum(denom, jnp.float32(NX * NZ))
    coefficient = jnp.dot(onehot, per_bin, precision=lax.Precision.HIGHEST)
    leonard = jnp.transpose(leonard, (1, 2, 0, 3))
    viscosity = coefficient[:, None, None] * jnp.transpose(magnitude, (1, 0, 2))
    return (leonard, viscosity, coefficient)
```

```python
import functools

import jax
import jax.numpy as jnp
from jax import lax
from jax.experimental import pallas as pl
from jax.experimental.pallas import tpu as pltpu
from jax.sharding import PartitionSpec as P

NBIN = 64
MESH = pl.DeviceIdType.MESH
F32 = jnp.float32
BF16 = jnp.bfloat16
VMEM = pltpu.VMEM
UNITS = 9
READY = (3, 6, 8, 9)


def to_columns(vel_ref, x_ref, mix):
    even = lax.broadcasted_iota(jnp.int32, (64, 128), 1) % 2 == 0

    def plane(y, _):
        for f in range(3):
            v = vel_ref[f, y]
            mix[f, pl.ds(0, 64, stride=2), :] = v
            mix[f, pl.ds(1, 64, stride=2), :] = v
            t = mix[f].T
            x_ref[pl.ds(f * 8 + y, 64, stride=24), :] = jnp.where(even, t[:64], t[64:])
        return 0

    lax.fori_loop(0, 8, plane, 0)


def where_am_i():
    px, pz = lax.axis_index("px"), lax.axis_index("pz")
    return px, pz, pz // 16, (pz % 16) // 4, pz % 4


def spread(x_ref, r_ref, partner, send_a, recv_a, send_b, recv_b, send_c, recv_c, local):
    px, pz, h, yy, xx = where_am_i()
    i = pz % 16
    other = 1 - h
    barrier = pltpu.get_barrier_semaphore()
    pl.semaphore_signal(barrier, inc=1, device_id=(px, other * 16 + i), device_id_type=MESH)
    for k in range(1, 16):
        j = ((yy + k // 4) % 4) * 4 + (xx + k % 4) % 4
        pl.semaphore_signal(barrier, inc=1, device_id=(px, h * 16 + j), device_id_type=MESH)
    pl.semaphore_wait(barrier, 16)

    def unit(n):
        u = (2 * yy + n) % UNITS
        return pltpu.make_async_remote_copy(
            src_ref=x_ref.at[pl.ds(other * 32 + u * 4, 4)],
            dst_ref=partner.at[pl.ds(u * 4, 4)],
            send_sem=send_a.at[n],
            recv_sem=recv_a.at[n],
            device_id=(px, other * 16 + i),
            device_id_type=MESH,
        )

    def own(k):
        j = ((yy + k // 4) % 4) * 4 + (xx + k % 4) % 4
        return pltpu.make_async_remote_copy(
            src_ref=x_ref.at[pl.ds((h * 16 + j) * 2, 6)],
            dst_ref=r_ref.at[:, :, pl.ds(pl.multiple_of(pz * 8, 8), 8), :],
            send_sem=send_b.at[k],
            recv_sem=recv_b.at[k],
            device_id=(px, h * 16 + j),
            device_id_type=MESH,
        )

    def theirs(k):
        j = ((yy + k // 4) % 4) * 4 + (xx + k % 4) % 4
        return pltpu.make_async_remote_copy(
            src_ref=partner.at[pl.ds(j * 2, 6)],
            dst_ref=r_ref.at[:, :, pl.ds(pl.multiple_of((other * 16 + i) * 8, 8), 8), :],
            send_sem=send_c.at[k],
            recv_sem=recv_c.at[k],
            device_id=(px, h * 16 + j),
            device_id_type=MESH,
        )

    for n in range(UNITS):
        unit(n).start()
    for k in range(1, 16):
        own(k).start()
    here = pltpu.make_async_copy(
        x_ref.at[pl.ds(pz * 2, 6)],
        r_ref.at[:, :, pl.ds(pl.multiple_of(pz * 8, 8), 8), :],
        local.at[0],
    )
    here.start()
    there = pltpu.make_async_copy(
        partner.at[pl.ds(i * 2, 6)],
        r_ref.at[:, :, pl.ds(pl.multiple_of((other * 16 + i) * 8, 8), 8), :],
        local.at[1],
    )
    done = 0
    for row in range(4):
        while done < READY[row]:
            unit(done).wait_recv()
            done += 1
        for col in range(4):
            k = row * 4 + col
            if k == 0:
                there.start()
            else:
                theirs(k).start()
    here.wait()
    there.wait()
    for n in range(UNITS):
        unit(n).wait_send()
    for k in range(1, 16):
        own(k).wait()
        theirs(k).wait()


def fields_of(u, gx, up, down):
    def d_x(f):
        return (u[f][gx + 1] - u[f][gx - 1]) * 0.5

    def d_z(f):
        return (pltpu.roll(u[f][gx], 126, 1) - pltpu.roll(u[f][gx], 2, 1)) * 0.5

    def d_y(f):
        return (up[f] - down[f]) * 0.5

    s = [
        d_x(0),
        d_y(1),
        d_z(2),
        0.5 * (d_y(0) + d_x(1)),
        0.5 * (d_z(0) + d_x(2)),
        0.5 * (d_z(1) + d_y(2)),
    ]
    mag = jnp.sqrt(
        2.0 * (s[0] * s[0] + s[1] * s[1] + s[2] * s[2])
        + 4.0 * (s[3] * s[3] + s[4] * s[4] + s[5] * s[5])
    )
    a, b, c = u[0][gx], u[1][gx], u[2][gx]
    return [a, b, c] + s + [a * a, b * b, c * c, a * b, a * c, b * c] + [mag * t for t in s], mag


def math(r_ref, inv_ref, fbc_ref, fbr_ref, pbc_ref, l_ref, part_ref, g, bh, bl, ff, wh, wl):
    masked = jnp.where(fbc_ref[...] == fbr_ref[...], inv_ref[...], 0.0)
    w = masked / jnp.sum(masked, axis=1, keepdims=True)
    w_hi = w.astype(BF16)
    wh[...] = w_hi
    wl[...] = (w - w_hi.astype(F32)).astype(BF16)

    def strip(c, _):
        y0 = pl.multiple_of(c * 16, 16)
        before = pl.multiple_of(jnp.maximum(y0 - 8, 0), 8)
        after = pl.multiple_of(jnp.minimum(y0 + 16, 248), 8)
        first, last = c == 0, c == 15
        u = [[r_ref[x, f, pl.ds(y0, 16), :] for x in range(6)] for f in range(3)]
        for gx in range(1, 5):
            up, down = [], []
            for f in range(3):
                prev = jnp.where(first, 0.0, r_ref[gx, f, pl.ds(before, 8), :])
                succ = jnp.where(last, 0.0, r_ref[gx, f, pl.ds(after, 8), :])
                down.append(jnp.concatenate([prev[7:], u[f][gx][:15]], axis=0))
                up.append(jnp.concatenate([u[f][gx][1:], succ[:1]], axis=0))
            out, mag = fields_of(u, gx, up, down)
            for k in range(21):
                g[k, gx - 1] = out[k]
            if gx in (2, 3):
                l_ref[2 * c, gx - 2, 6] = mag[:8]
                l_ref[2 * c + 1, gx - 2, 6] = mag[8:]
        for k in range(21):
            g1, g2 = g[k, 1], g[k, 2]
            for x, total in ((0, g[k, 0] + 2.0 * g1 + g2), (1, g1 + 2.0 * g2 + g[k, 3])):
                box = (pltpu.roll(total, 2, 1) + 2.0 * total + pltpu.roll(total, 126, 1)) * 0.0625
                hi = box.astype(BF16)
                bh[k, pl.ds(y0, 16), pl.ds(x * 128, 128)] = hi
                bl[k, pl.ds(y0, 16), pl.ds(x * 128, 128)] = (box - hi.astype(F32)).astype(BF16)
        return 0

    lax.fori_loop(0, 16, strip, 0)

    def product(k, _):
        hi, lo = bh[k], bl[k]
        acc = jnp.dot(wh[...], lo, preferred_element_type=F32)
        acc += jnp.dot(wl[...], hi, preferred_element_type=F32)
        ff[k] = acc + jnp.dot(wh[...], hi, preferred_element_type=F32)
        return 0

    lax.fori_loop(0, 21, product, 0)

    lanes = lax.broadcasted_iota(jnp.int32, (8, 128), 1)

    def contract(c, sums):
        y0 = pl.multiple_of(c * 8, 8)
        lm_sum, mm_sum = 0.0, 0.0
        for x in range(2):
            f = [ff[k, pl.ds(y0, 8), pl.ds(x * 128, 128)] for k in range(21)]
            a, b, d = f[0], f[1], f[2]
            s, p, m = f[3:9], f[9:15], f[15:21]
            uu = [a * a, b * b, d * d, a * b, a * d, b * d]
            fmag = jnp.sqrt(
                2.0 * (s[0] * s[0] + s[1] * s[1] + s[2] * s[2])
                + 4.0 * (s[3] * s[3] + s[4] * s[4] + s[5] * s[5])
            )
            lm, mm = [], []
            for k in range(6):
                leo = p[k] - uu[k]
                l_ref[c, x, k] = leo
                mod = m[k] - 4.0 * fmag * s[k]
                lm.append(leo * mod)
                mm.append(mod * mod)
            lm_sum += lm[0] + lm[1] + lm[2] + 2.0 * (lm[3] + lm[4] + lm[5])
            mm_sum += mm[0] + mm[1] + mm[2] + 2.0 * (mm[3] + mm[4] + mm[5])
        hot = pbc_ref[pl.ds(y0, 8), :] == lanes
        num = sums[0] + jnp.where(hot, jnp.sum(lm_sum, axis=1, keepdims=True), 0.0)
        den = sums[1] + jnp.where(hot, jnp.sum(mm_sum, axis=1, keepdims=True), 0.0)
        return num, den

    zero = jnp.zeros((8, 128), F32)
    num, den = lax.fori_loop(0, 32, contract, (zero, zero))
    row = lax.broadcasted_iota(jnp.int32, (8, 128), 0)
    num = jnp.sum(num, axis=0, keepdims=True)
    den = jnp.sum(den, axis=0, keepdims=True)
    part_ref[...] = jnp.where(row == 0, num, jnp.where(row == 1, den, 0.0))


def give_back(l_ref, part_ref, o_ref, tot_ref, a1, a2, s1, ss1, rs1, ss2, rs2, sb, rb, local):
    px, pz, h, yy, xx = where_am_i()

    def peer(k):
        return ((h + k // 16) % 2) * 16 + ((yy + (k % 16) // 4) % 4) * 4 + (xx + k % 4) % 4

    barrier = pltpu.get_barrier_semaphore()
    for k in range(1, 32):
        pl.semaphore_signal(barrier, inc=1, device_id=(px, peer(k)), device_id_type=MESH)
    for k in range(1, 8):
        pl.semaphore_signal(barrier, inc=1, device_id=((px + k) % 8, pz), device_id_type=MESH)
    pl.semaphore_wait(barrier, 38)

    def small(k):
        return pltpu.make_async_remote_copy(
            src_ref=part_ref,
            dst_ref=a1.at[pz],
            send_sem=ss1.at[k],
            recv_sem=rs1.at[k],
            device_id=(px, peer(k)),
            device_id_type=MESH,
        )

    def second(k):
        return pltpu.make_async_remote_copy(
            src_ref=s1,
            dst_ref=a2.at[px],
            send_sem=ss2.at[k],
            recv_sem=rs2.at[k],
            device_id=((px + k) % 8, pz),
            device_id_type=MESH,
        )

    def big(k):
        return pltpu.make_async_remote_copy(
            src_ref=l_ref.at[peer(k)],
            dst_ref=o_ref.at[pz],
            send_sem=sb.at[k],
            recv_sem=rb.at[k],
            device_id=(px, peer(k)),
            device_id_type=MESH,
        )

    for k in range(1, 32):
        small(k).start()
    for k in range(1, 16):
        big(k).start()
    a1[pz] = part_ref[...]
    for k in range(1, 32):
        small(k).wait_recv()
    total = a1[0]
    for q in range(1, 32):
        total = total + a1[q]
    s1[...] = total
    a2[px] = total
    here = pltpu.make_async_copy(l_ref.at[pz], o_ref.at[pz], local.at[0])
    here.start()
    for k in range(1, 8):
        second(k).start()
    for k in range(16, 32):
        big(k).start()
    for k in range(1, 8):
        second(k).wait_recv()
    total = a2[0]
    for q in range(1, 8):
        total = total + a2[q]
    tot_ref[...] = total
    here.wait()
    for k in range(1, 32):
        small(k).wait_send()
    for k in range(1, 8):
        second(k).wait_send()
    for k in range(1, 32):
        big(k).wait()


def to_planes(coef_ref, o_ref, leo_ref, visc_ref, mix):
    low = lax.broadcasted_iota(jnp.int32, (64, 128), 1) < 64

    def plane(y, _):
        for f in range(7):
            m = o_ref[pl.ds(f * 8 + y, 64, stride=56), :]
            mix[f] = jnp.concatenate([m, m], axis=0).T
            v = jnp.where(low, mix[f, pl.ds(0, 64, stride=2), :], mix[f, pl.ds(1, 64, stride=2), :])
            if f < 6:
                leo_ref[f, y] = v
            else:
                visc_ref[y] = coef_ref[y] * v
        return 0

    lax.fori_loop(0, 8, plane, 0)


def spec(space):
    return pl.BlockSpec(memory_space=space)


def params(**kw):
    return pltpu.CompilerParams(vmem_limit_bytes=56 * 1024 * 1024, **kw)


DMA = pltpu.SemaphoreType.DMA


def local_step(velocity, filter_inverse, filter_block, plane_bin):
    pz = lax.axis_index("pz")
    rows = pl.pallas_call(
        to_columns,
        out_shape=jax.ShapeDtypeStruct((64 * 24, 128), F32),
        in_specs=[spec(VMEM)],
        out_specs=spec(VMEM),
        scratch_shapes=[VMEM((3, 128, 128), F32)],
        compiler_params=params(),
        name="to_columns",
    )(velocity).reshape(64, 3, 8, 128)
    head, tail = rows[:2], rows[62:]
    left = lax.ppermute(tail, "px", [(i, (i + 1) % 8) for i in range(8)])
    right = lax.ppermute(head, "px", [((i + 1) % 8, i) for i in range(8)])
    even = lax.broadcasted_iota(jnp.int32, (2, 3, 8, 128), 3) % 2 == 0
    below = jnp.where(even, jnp.roll(left, -1, axis=3), jnp.roll(tail, 1, axis=3))
    above = jnp.where(even, jnp.roll(head, -1, axis=3), jnp.roll(right, 1, axis=3))
    rows = jnp.concatenate([below, rows, above], axis=0)
    columns = pl.pallas_call(
        spread,
        out_shape=jax.ShapeDtypeStruct((6, 3, 256, 128), F32),
        in_specs=[spec(VMEM)],
        out_specs=spec(pl.ANY),
        scratch_shapes=[
            VMEM((36, 3, 8, 128), F32),
            DMA((UNITS,)),
            DMA((UNITS,)),
            DMA((16,)),
            DMA((16,)),
            DMA((16,)),
            DMA((16,)),
            DMA((2,)),
        ],
        compiler_params=params(collective_id=0, has_side_effects=True),
        name="spread",
    )(rows)
    leo, part = pl.pallas_call(
        math,
        out_shape=(
            jax.ShapeDtypeStruct((32, 2, 7, 8, 128), F32),
            jax.ShapeDtypeStruct((8, 128), F32),
        ),
        in_specs=[spec(VMEM)] * 5,
        out_specs=(spec(VMEM), spec(VMEM)),
        scratch_shapes=[
            VMEM((21, 4, 16, 128), F32),
            VMEM((21, 256, 256), BF16),
            VMEM((21, 256, 256), BF16),
            VMEM((21, 256, 256), F32),
            VMEM((256, 256), BF16),
            VMEM((256, 256), BF16),
        ],
        compiler_params=params(),
        name="math",
    )(
        columns,
        filter_inverse,
        filter_block.reshape(256, 1),
        filter_block.reshape(1, 256),
        plane_bin.reshape(256, 1),
    )
    back, total = pl.pallas_call(
        give_back,
        out_shape=(
            jax.ShapeDtypeStruct((32, 2, 7, 8, 128), F32),
            jax.ShapeDtypeStruct((8, 128), F32),
        ),
        in_specs=[spec(VMEM)] * 2,
        out_specs=(spec(pl.ANY), spec(VMEM)),
        scratch_shapes=[
            VMEM((32, 8, 128), F32),
            VMEM((8, 8, 128), F32),
            VMEM((8, 128), F32),
            DMA((32,)),
            DMA((32,)),
            DMA((8,)),
            DMA((8,)),
            DMA((32,)),
            DMA((32,)),
            DMA((1,)),
        ],
        compiler_params=params(collective_id=1, has_side_effects=True),
        name="give_back",
    )(leo, part)
    per_bin = total[0, :NBIN] / jnp.maximum(total[1, :NBIN], jnp.float32(65536))
    hot = plane_bin[:, None] == jnp.arange(NBIN, dtype=jnp.int32)[None, :]
    coefficient = jnp.sum(jnp.where(hot, per_bin[None, :], 0.0), axis=1)
    mine = lax.dynamic_slice(coefficient, (pz * 8,), (8,))
    leonard, viscosity = pl.pallas_call(
        to_planes,
        out_shape=(
            jax.ShapeDtypeStruct((6, 8, 64, 128), F32),
            jax.ShapeDtypeStruct((8, 64, 128), F32),
        ),
        in_specs=[spec(pltpu.SMEM), spec(VMEM)],
        out_specs=(spec(VMEM), spec(VMEM)),
        scratch_shapes=[VMEM((7, 128, 128), F32)],
        compiler_params=params(),
        name="to_planes",
    )(mine, back.reshape(32 * 2 * 56, 128))
    return leonard, viscosity, coefficient


def solution(mesh):
    return jax.shard_map(
        local_step,
        mesh=mesh,
        in_specs=(P(None, "pz", None, "px"), P(), P(), P()),
        out_specs=(P(None, "pz", None, "px"), P("pz", None, "px"), P()),
        check_vma=False,
    )
```

```python
import functools

import jax
import jax.numpy as jnp
from jax import lax
from jax.experimental import pallas as pl
from jax.experimental.pallas import tpu as pltpu
from jax.sharding import PartitionSpec as P

NBIN = 64
MESH = pl.DeviceIdType.MESH
F32 = jnp.float32
BF16 = jnp.bfloat16
VMEM = pltpu.VMEM
def to_columns(vel_ref, x_ref, right_ref, left_ref, mix):
    even = lax.broadcasted_iota(jnp.int32, (64, 128), 1) % 2 == 0

    def plane(y, _):
        for f in range(3):
            v = vel_ref[f, y]
            mix[f, pl.ds(0, 64, stride=2), :] = v
            mix[f, pl.ds(1, 64, stride=2), :] = v
            t = mix[f].T
            x_ref[pl.ds(48 + f * 8 + y, 64, stride=24), :] = jnp.where(even, t[:64], t[64:])
        return 0

    lax.fori_loop(0, 8, plane, 0)
    first, last = x_ref[48:96, :], x_ref[64 * 24 : 66 * 24, :]
    x_ref[0:48, :] = pltpu.roll(last, 1, 1)
    x_ref[66 * 24 : 68 * 24, :] = pltpu.roll(first, 127, 1)
    right_ref[...] = pltpu.roll(last, 127, 1)
    left_ref[...] = pltpu.roll(first, 1, 1)


def where_am_i():
    px, pz = lax.axis_index("px"), lax.axis_index("pz")
    return px, pz, pz // 16, (pz % 16) // 4, pz % 4


def spread(x_ref, below_ref, above_ref, r_ref, rows, partner, send_a, recv_a, send_b, recv_b, send_c, recv_c, local):
    px, pz, h, yy, xx = where_am_i()
    i = pz % 16
    other = 1 - h
    fetch = pltpu.make_async_copy(x_ref, rows, local.at[0])
    fetch.start()
    barrier = pltpu.get_barrier_semaphore()
    pl.semaphore_signal(barrier, inc=1, device_id=(px, other * 16 + i), device_id_type=MESH)
    for k in range(1, 16):
        j = ((yy + k // 4) % 4) * 4 + (xx + k % 4) % 4
        pl.semaphore_signal(barrier, inc=1, device_id=(px, h * 16 + j), device_id_type=MESH)
    fetch.wait()
    even = lax.broadcasted_iota(jnp.int32, (2, 3, 8, 128), 3) % 2 == 0
    rows[0:2] = jnp.where(even, below_ref[...], rows[0:2])
    rows[66:68] = jnp.where(even, rows[66:68], above_ref[...])
    pl.semaphore_wait(barrier, 16)

    def across(f):
        return pltpu.make_async_remote_copy(
            src_ref=rows.at[:, f],
            dst_ref=partner.at[:, f],
            send_sem=send_a.at[f],
            recv_sem=recv_a.at[f],
            device_id=(px, other * 16 + i),
            device_id_type=MESH,
        )

    def own(k):
        j = ((yy + k // 4) % 4) * 4 + (xx + k % 4) % 4
        return pltpu.make_async_remote_copy(
            src_ref=rows.at[pl.ds(j * 4, 8)],
            dst_ref=r_ref.at[:, :, pl.ds(pl.multiple_of(pz * 8, 8), 8), :],
            send_sem=send_b.at[k],
            recv_sem=recv_b.at[k],
            device_id=(px, h * 16 + j),
            device_id_type=MESH,
        )

    def theirs(f, k):
        j = ((yy + k // 4) % 4) * 4 + (xx + k % 4) % 4
        return pltpu.make_async_remote_copy(
            src_ref=partner.at[pl.ds(j * 4, 8), f],
            dst_ref=r_ref.at[:, f, pl.ds(pl.multiple_of((other * 16 + i) * 8, 8), 8), :],
            send_sem=send_c.at[f, k],
            recv_sem=recv_c.at[f, k],
            device_id=(px, h * 16 + j),
            device_id_type=MESH,
        )

    def there(f):
        return pltpu.make_async_copy(
            partner.at[pl.ds(i * 4, 8), f],
            r_ref.at[:, f, pl.ds(pl.multiple_of((other * 16 + i) * 8, 8), 8), :],
            local.at[1 + f],
        )

    for f in range(3):
        across(f).start()
    for k in range(1, 16):
        own(k).start()
    here = pltpu.make_async_copy(
        rows.at[pl.ds(i * 4, 8)],
        r_ref.at[:, :, pl.ds(pl.multiple_of(pz * 8, 8), 8), :],
        local.at[0],
    )
    here.start()
    for f in range(3):
        across(f).wait_recv()
        for k in range(1, 16):
            theirs(f, k).start()
        there(f).start()
    here.wait()
    for f in range(3):
        across(f).wait_send()
        there(f).wait()
        for k in range(1, 16):
            theirs(f, k).wait()
    for k in range(1, 16):
        own(k).wait()


def fields_of(u, gx, up, down):
    def d_x(f):
        return (u[f][gx + 1] - u[f][gx - 1]) * 0.5

    def d_z(f):
        return (pltpu.roll(u[f][gx], 126, 1) - pltpu.roll(u[f][gx], 2, 1)) * 0.5

    def d_y(f):
        return (up[f] - down[f]) * 0.5

    s = [
        d_x(0),
        d_y(1),
        d_z(2),
        0.5 * (d_y(0) + d_x(1)),
        0.5 * (d_z(0) + d_x(2)),
        0.5 * (d_z(1) + d_y(2)),
    ]
    mag = jnp.sqrt(
        2.0 * (s[0] * s[0] + s[1] * s[1] + s[2] * s[2])
        + 4.0 * (s[3] * s[3] + s[4] * s[4] + s[5] * s[5])
    )
    a, b, c = u[0][gx], u[1][gx], u[2][gx]
    return [a, b, c] + s + [a * a, b * b, c * c, a * b, a * c, b * c] + [mag * t for t in s], mag


def column(row):
    return jnp.broadcast_to(row, (128, 256)).T


def math(r_ref, inv_ref, fb_ref, pb_ref, l_ref, part_ref, g, bh, bl, ff, wh, wl, bins):
    h = lax.axis_index("pz") // 16
    r0 = pl.multiple_of(h * 128, 128)
    bins[0] = column(fb_ref[...])
    bins[1] = column(pb_ref[...])
    mine = bins[0, pl.ds(r0, 128), :]
    masked = jnp.where(jnp.concatenate([mine, mine], axis=1) == fb_ref[...], inv_ref[pl.ds(r0, 128), :], 0.0)
    w = masked / jnp.sum(masked, axis=1, keepdims=True)
    w_hi = w.astype(BF16)
    wh[...] = w_hi
    wl[...] = (w - w_hi.astype(F32)).astype(BF16)

    def strip(c, _):
        y0 = pl.multiple_of(c * 16, 16)
        before = pl.multiple_of(jnp.maximum(y0 - 8, 0), 8)
        after = pl.multiple_of(jnp.minimum(y0 + 16, 248), 8)
        first, last = c == 0, c == 15
        block = jnp.clip(2 * c - 16 * h, 0, 14)
        u = [[r_ref[x, f, pl.ds(y0, 16), :] for x in range(8)] for f in range(3)]
        for gx in range(1, 7):
            up, down = [], []
            for f in range(3):
                prev = jnp.where(first, 0.0, r_ref[gx, f, pl.ds(before, 8), :])
                succ = jnp.where(last, 0.0, r_ref[gx, f, pl.ds(after, 8), :])
                down.append(jnp.concatenate([prev[7:], u[f][gx][:15]], axis=0))
                up.append(jnp.concatenate([u[f][gx][1:], succ[:1]], axis=0))
            out, mag = fields_of(u, gx, up, down)
            for k in range(21):
                g[k, gx - 1] = out[k]
            if 2 <= gx <= 5:

                @pl.when(c // 8 == h)
                def _(mag=mag, gx=gx):
                    l_ref[block, gx - 2, 6] = mag[:8]
                    l_ref[block + 1, gx - 2, 6] = mag[8:]

        for k in range(21):
            gs = [g[k, t] for t in range(6)]
            for x in range(4):
                total = gs[x] + 2.0 * gs[x + 1] + gs[x + 2]
                box = (pltpu.roll(total, 2, 1) + 2.0 * total + pltpu.roll(total, 126, 1)) * 0.0625
                hi = box.astype(BF16)
                bh[k, pl.ds(y0, 16), pl.ds(x * 128, 128)] = hi
                bl[k, pl.ds(y0, 16), pl.ds(x * 128, 128)] = (box - hi.astype(F32)).astype(BF16)
        return 0

    lax.fori_loop(0, 16, strip, 0)

    def product(k, _):
        hi, lo = bh[k], bl[k]
        acc = jnp.dot(wh[...], lo, preferred_element_type=F32)
        acc += jnp.dot(wl[...], hi, preferred_element_type=F32)
        ff[k] = acc + jnp.dot(wh[...], hi, preferred_element_type=F32)
        return 0

    lax.fori_loop(0, 21, product, 0)

    lanes = lax.broadcasted_iota(jnp.int32, (8, 128), 1)

    def contract(c, sums):
        y0 = pl.multiple_of(c * 8, 8)
        lm_sum, mm_sum = 0.0, 0.0
        for x in range(4):
            f = [ff[k, pl.ds(y0, 8), pl.ds(x * 128, 128)] for k in range(21)]
            a, b, d = f[0], f[1], f[2]
            s, p, m = f[3:9], f[9:15], f[15:21]
            uu = [a * a, b * b, d * d, a * b, a * d, b * d]
            fmag = jnp.sqrt(
                2.0 * (s[0] * s[0] + s[1] * s[1] + s[2] * s[2])
                + 4.0 * (s[3] * s[3] + s[4] * s[4] + s[5] * s[5])
            )
            lm, mm = [], []
            for k in range(6):
                leo = p[k] - uu[k]
                l_ref[c, x, k] = leo
                mod = m[k] - 4.0 * fmag * s[k]
                lm.append(leo * mod)
                mm.append(mod * mod)
            lm_sum += lm[0] + lm[1] + lm[2] + 2.0 * (lm[3] + lm[4] + lm[5])
            mm_sum += mm[0] + mm[1] + mm[2] + 2.0 * (mm[3] + mm[4] + mm[5])
        hot = bins[1, pl.ds(pl.multiple_of(r0 + y0, 8), 8), :] == lanes
        num = sums[0] + jnp.where(hot, jnp.sum(lm_sum, axis=1, keepdims=True), 0.0)
        den = sums[1] + jnp.where(hot, jnp.sum(mm_sum, axis=1, keepdims=True), 0.0)
        return num, den

    zero = jnp.zeros((8, 128), F32)
    num, den = lax.fori_loop(0, 16, contract, (zero, zero))
    row = lax.broadcasted_iota(jnp.int32, (8, 128), 0)
    num = jnp.sum(num, axis=0, keepdims=True)
    den = jnp.sum(den, axis=0, keepdims=True)
    part_ref[...] = jnp.where(row == 0, num, jnp.where(row == 1, den, 0.0))


def give_back(l_ref, part_ref, o_ref, tot_ref, a1, a2, s1, ss1, rs1, ss2, rs2, sb, rb, local):
    px, pz, h, yy, xx = where_am_i()

    def peer(k):
        return ((h + k // 16) % 2) * 16 + ((yy + (k % 16) // 4) % 4) * 4 + (xx + k % 4) % 4

    barrier = pltpu.get_barrier_semaphore()
    for k in range(1, 32):
        pl.semaphore_signal(barrier, inc=1, device_id=(px, peer(k)), device_id_type=MESH)
    for k in range(1, 8):
        pl.semaphore_signal(barrier, inc=1, device_id=((px + k) % 8, pz), device_id_type=MESH)
    pl.semaphore_wait(barrier, 38)

    def small(k):
        return pltpu.make_async_remote_copy(
            src_ref=part_ref,
            dst_ref=a1.at[pz],
            send_sem=ss1.at[k],
            recv_sem=rs1.at[k],
            device_id=(px, peer(k)),
            device_id_type=MESH,
        )

    def second(k):
        return pltpu.make_async_remote_copy(
            src_ref=s1,
            dst_ref=a2.at[px],
            send_sem=ss2.at[k],
            recv_sem=rs2.at[k],
            device_id=((px + k) % 8, pz),
            device_id_type=MESH,
        )

    def big(k):
        return pltpu.make_async_remote_copy(
            src_ref=l_ref.at[peer(k) % 16],
            dst_ref=o_ref.at[pz % 16],
            send_sem=sb.at[k],
            recv_sem=rb.at[k],
            device_id=(px, peer(k)),
            device_id_type=MESH,
        )

    for k in range(1, 32):
        small(k).start()
    for k in range(1, 16):
        big(k).start()
    a1[pz] = part_ref[...]
    for k in range(1, 32):
        small(k).wait_recv()
    total = a1[0]
    for q in range(1, 32):
        total = total + a1[q]
    s1[...] = total
    a2[px] = total
    here = pltpu.make_async_copy(l_ref.at[pz % 16], o_ref.at[pz % 16], local.at[0])
    here.start()
    for k in range(1, 8):
        second(k).start()
    for k in range(1, 8):
        second(k).wait_recv()
    total = a2[0]
    for q in range(1, 8):
        total = total + a2[q]
    tot_ref[...] = total
    here.wait()
    for k in range(1, 32):
        small(k).wait_send()
    for k in range(1, 8):
        second(k).wait_send()
    for k in range(1, 16):
        big(k).wait()


def to_planes(tot_ref, pb_ref, o_ref, leo_ref, visc_ref, coef_ref, mix):
    pz = lax.axis_index("pz")
    per_bin = tot_ref[0:1, :] / jnp.maximum(tot_ref[1:2, :], 65536.0)
    per_bin = jnp.broadcast_to(per_bin, (128, 128)).T
    hot = lax.broadcasted_iota(jnp.int32, (128, 256), 0) == pb_ref[...]
    both = jnp.concatenate([per_bin, per_bin], axis=1)
    coef = jnp.sum(jnp.where(hot, both, 0.0), axis=0, keepdims=True)
    coef_ref[...] = coef
    at = lax.broadcasted_iota(jnp.int32, (1, 256), 1) - pz * 8
    low = lax.broadcasted_iota(jnp.int32, (64, 128), 1) < 64

    def plane(y, _):
        mine = jnp.sum(jnp.where(at == y, coef, 0.0), axis=1, keepdims=True)
        for f in range(7):
            m = o_ref[pl.ds(f * 8 + y, 64, stride=56), :]
            mix[f] = jnp.concatenate([m, m], axis=0).T
            v = jnp.where(low, mix[f, pl.ds(0, 64, stride=2), :], mix[f, pl.ds(1, 64, stride=2), :])
            if f < 6:
                leo_ref[f, y] = v
            else:
                visc_ref[y] = mine * v
        return 0

    lax.fori_loop(0, 8, plane, 0)


def spec(space):
    return pl.BlockSpec(memory_space=space)


def params(**kw):
    return pltpu.CompilerParams(vmem_limit_bytes=56 * 1024 * 1024, **kw)


DMA = pltpu.SemaphoreType.DMA


def local_step(velocity, filter_inverse, filter_block, plane_bin):
    edge = jax.ShapeDtypeStruct((48, 128), F32)
    rows, right, left = pl.pallas_call(
        to_columns,
        out_shape=(jax.ShapeDtypeStruct((68 * 24, 128), F32), edge, edge),
        in_specs=[spec(VMEM)],
        out_specs=(spec(VMEM),) * 3,
        scratch_shapes=[VMEM((3, 128, 128), F32)],
        compiler_params=params(),
        name="to_columns",
    )(velocity)
    below = lax.ppermute(right, "px", [(i, (i + 1) % 8) for i in range(8)])
    above = lax.ppermute(left, "px", [((i + 1) % 8, i) for i in range(8)])
    columns = pl.pallas_call(
        spread,
        out_shape=jax.ShapeDtypeStruct((8, 3, 256, 128), F32),
        in_specs=[spec(pl.ANY), spec(VMEM), spec(VMEM)],
        out_specs=spec(pl.ANY),
        scratch_shapes=[
            VMEM((68, 3, 8, 128), F32),
            VMEM((68, 3, 8, 128), F32),
            DMA((3,)),
            DMA((3,)),
            DMA((16,)),
            DMA((16,)),
            DMA((3, 16)),
            DMA((3, 16)),
            DMA((4,)),
        ],
        compiler_params=params(collective_id=0, has_side_effects=True),
        name="spread",
    )(rows.reshape(68, 3, 8, 128), below.reshape(2, 3, 8, 128), above.reshape(2, 3, 8, 128))
    bins = plane_bin.reshape(1, 256)
    leo, part = pl.pallas_call(
        math,
        out_shape=(
            jax.ShapeDtypeStruct((16, 4, 7, 8, 128), F32),
            jax.ShapeDtypeStruct((8, 128), F32),
        ),
        in_specs=[spec(VMEM)] * 4,
        out_specs=(spec(VMEM), spec(VMEM)),
        scratch_shapes=[
            VMEM((21, 6, 16, 128), F32),
            VMEM((21, 256, 512), BF16),
            VMEM((21, 256, 512), BF16),
            VMEM((21, 128, 512), F32),
            VMEM((128, 256), BF16),
            VMEM((128, 256), BF16),
            VMEM((2, 256, 128), jnp.int32),
        ],
        compiler_params=params(),
        name="math",
    )(columns, filter_inverse, filter_block.reshape(1, 256), bins)
    back, total = pl.pallas_call(
        give_back,
        out_shape=(
            jax.ShapeDtypeStruct((16, 4, 7, 8, 128), F32),
            jax.ShapeDtypeStruct((8, 128), F32),
        ),
        in_specs=[spec(VMEM)] * 2,
        out_specs=(spec(pl.ANY), spec(VMEM)),
        scratch_shapes=[
            VMEM((32, 8, 128), F32),
            VMEM((8, 8, 128), F32),
            VMEM((8, 128), F32),
            DMA((32,)),
            DMA((32,)),
            DMA((8,)),
            DMA((8,)),
            DMA((16,)),
            DMA((16,)),
            DMA((1,)),
        ],
        compiler_params=params(collective_id=1, has_side_effects=True),
        name="give_back",
    )(leo, part)
    leonard, viscosity, coefficient = pl.pallas_call(
        to_planes,
        out_shape=(
            jax.ShapeDtypeStruct((6, 8, 64, 128), F32),
            jax.ShapeDtypeStruct((8, 64, 128), F32),
            jax.ShapeDtypeStruct((1, 256), F32),
        ),
        in_specs=[spec(VMEM)] * 3,
        out_specs=(spec(VMEM),) * 3,
        scratch_shapes=[VMEM((7, 128, 128), F32)],
        compiler_params=params(),
        name="to_planes",
    )(total, bins, back.reshape(16 * 4 * 56, 128))
    return leonard, viscosity, coefficient.reshape(256)


def solution(mesh):
    return jax.shard_map(
        local_step,
        mesh=mesh,
        in_specs=(P(None, "pz", None, "px"), P(), P(), P()),
        out_specs=(P(None, "pz", None, "px"), P("pz", None, "px"), P()),
        check_vma=False,
    )
```

```python
import functools

import jax
import jax.numpy as jnp
from jax import lax
from jax.experimental import pallas as pl
from jax.experimental.pallas import tpu as pltpu
from jax.sharding import PartitionSpec as P

NBIN = 64
MESH = pl.DeviceIdType.MESH
F32 = jnp.float32
BF16 = jnp.bfloat16
VMEM = pltpu.VMEM
def to_columns(vel_ref, x_ref, right_ref, left_ref, mix):
    even = lax.broadcasted_iota(jnp.int32, (64, 128), 1) % 2 == 0

    def plane(y, _):
        for f in range(3):
            v = vel_ref[f, y]
            mix[f, pl.ds(0, 64, stride=2), :] = v
            mix[f, pl.ds(1, 64, stride=2), :] = v
            t = mix[f].T
            x_ref[pl.ds(48 + f * 8 + y, 64, stride=24), :] = jnp.where(even, t[:64], t[64:])
        return 0

    lax.fori_loop(0, 8, plane, 0)
    first, last = x_ref[48:96, :], x_ref[64 * 24 : 66 * 24, :]
    x_ref[0:48, :] = pltpu.roll(last, 1, 1)
    x_ref[66 * 24 : 68 * 24, :] = pltpu.roll(first, 127, 1)
    right_ref[...] = pltpu.roll(last, 127, 1)
    left_ref[...] = pltpu.roll(first, 1, 1)


ORDER = (10, 6, 14, 8, 9, 11, 2, 5, 15, 13, 7, 1, 3, 4, 12)


def where_am_i():
    px, pz = lax.axis_index("px"), lax.axis_index("pz")
    return px, pz, pz // 16, (pz % 16) // 4, pz % 4


def spread(x_ref, below_ref, above_ref, r_ref, rows, partner, send_a, recv_a, send_b, recv_b, send_c, recv_c, local):
    px, pz, h, yy, xx = where_am_i()
    i = pz % 16
    other = 1 - h
    fetch = pltpu.make_async_copy(x_ref, rows, local.at[0])
    fetch.start()
    barrier = pltpu.get_barrier_semaphore()
    pl.semaphore_signal(barrier, inc=1, device_id=(px, other * 16 + i), device_id_type=MESH)
    for k in range(1, 16):
        j = ((yy + k // 4) % 4) * 4 + (xx + k % 4) % 4
        pl.semaphore_signal(barrier, inc=1, device_id=(px, h * 16 + j), device_id_type=MESH)
    fetch.wait()
    even = lax.broadcasted_iota(jnp.int32, (2, 3, 8, 128), 3) % 2 == 0
    rows[0:2] = jnp.where(even, below_ref[...], rows[0:2])
    rows[66:68] = jnp.where(even, rows[66:68], above_ref[...])
    pl.semaphore_wait(barrier, 16)

    def across(f):
        return pltpu.make_async_remote_copy(
            src_ref=rows.at[:, f],
            dst_ref=partner.at[:, f],
            send_sem=send_a.at[f],
            recv_sem=recv_a.at[f],
            device_id=(px, other * 16 + i),
            device_id_type=MESH,
        )

    def own(k):
        j = ((yy + k // 4) % 4) * 4 + (xx + k % 4) % 4
        return pltpu.make_async_remote_copy(
            src_ref=rows.at[pl.ds(j * 4, 8)],
            dst_ref=r_ref.at[:, :, pl.ds(pl.multiple_of(pz * 8, 8), 8), :],
            send_sem=send_b.at[k],
            recv_sem=recv_b.at[k],
            device_id=(px, h * 16 + j),
            device_id_type=MESH,
        )

    def theirs(f, k):
        j = ((yy + k // 4) % 4) * 4 + (xx + k % 4) % 4
        return pltpu.make_async_remote_copy(
            src_ref=partner.at[pl.ds(j * 4, 8), f],
            dst_ref=r_ref.at[:, f, pl.ds(pl.multiple_of((other * 16 + i) * 8, 8), 8), :],
            send_sem=send_c.at[f, k],
            recv_sem=recv_c.at[f, k],
            device_id=(px, h * 16 + j),
            device_id_type=MESH,
        )

    def there(f):
        return pltpu.make_async_copy(
            partner.at[pl.ds(i * 4, 8), f],
            r_ref.at[:, f, pl.ds(pl.multiple_of((other * 16 + i) * 8, 8), 8), :],
            local.at[1 + f],
        )

    for f in range(3):
        across(f).start()
    for k in ORDER:
        own(k).start()
    here = pltpu.make_async_copy(
        rows.at[pl.ds(i * 4, 8)],
        r_ref.at[:, :, pl.ds(pl.multiple_of(pz * 8, 8), 8), :],
        local.at[0],
    )
    here.start()
    for f in range(3):
        across(f).wait_recv()
        for k in ORDER:
            theirs(f, k).start()
        there(f).start()
    here.wait()
    for f in range(3):
        across(f).wait_send()
        there(f).wait()
        for k in range(1, 16):
            theirs(f, k).wait()
    for k in range(1, 16):
        own(k).wait()


def fields_of(u, gx, up, down):
    def d_x(f):
        return (u[f][gx + 1] - u[f][gx - 1]) * 0.5

    def d_z(f):
        return (pltpu.roll(u[f][gx], 126, 1) - pltpu.roll(u[f][gx], 2, 1)) * 0.5

    def d_y(f):
        return (up[f] - down[f]) * 0.5

    s = [
        d_x(0),
        d_y(1),
        d_z(2),
        0.5 * (d_y(0) + d_x(1)),
        0.5 * (d_z(0) + d_x(2)),
        0.5 * (d_z(1) + d_y(2)),
    ]
    mag = jnp.sqrt(
        2.0 * (s[0] * s[0] + s[1] * s[1] + s[2] * s[2])
        + 4.0 * (s[3] * s[3] + s[4] * s[4] + s[5] * s[5])
    )
    a, b, c = u[0][gx], u[1][gx], u[2][gx]
    return [a, b, c] + s + [a * a, b * b, c * c, a * b, a * c, b * c] + [mag * t for t in s], mag


def column(row):
    return jnp.broadcast_to(row, (128, 256)).T


def math(r_ref, inv_ref, fb_ref, pb_ref, l_ref, part_ref, g, bh, bl, ff, wh, wl, bins):
    h = lax.axis_index("pz") // 16
    r0 = pl.multiple_of(h * 128, 128)
    bins[0] = column(fb_ref[...])
    bins[1] = column(pb_ref[...])
    mine = bins[0, pl.ds(r0, 128), :]
    masked = jnp.where(jnp.concatenate([mine, mine], axis=1) == fb_ref[...], inv_ref[pl.ds(r0, 128), :], 0.0)
    w = masked / jnp.sum(masked, axis=1, keepdims=True)
    w_hi = w.astype(BF16)
    wh[...] = w_hi
    wl[...] = (w - w_hi.astype(F32)).astype(BF16)

    def strip(c, _):
        y0 = pl.multiple_of(c * 16, 16)
        before = pl.multiple_of(jnp.maximum(y0 - 8, 0), 8)
        after = pl.multiple_of(jnp.minimum(y0 + 16, 248), 8)
        first, last = c == 0, c == 15
        block = jnp.clip(2 * c - 16 * h, 0, 14)
        u = [[r_ref[x, f, pl.ds(y0, 16), :] for x in range(8)] for f in range(3)]
        for gx in range(1, 7):
            up, down = [], []
            for f in range(3):
                prev = jnp.where(first, 0.0, r_ref[gx, f, pl.ds(before, 8), :])
                succ = jnp.where(last, 0.0, r_ref[gx, f, pl.ds(after, 8), :])
                down.append(jnp.concatenate([prev[7:], u[f][gx][:15]], axis=0))
                up.append(jnp.concatenate([u[f][gx][1:], succ[:1]], axis=0))
            out, mag = fields_of(u, gx, up, down)
            for k in range(21):
                g[k, gx - 1] = out[k]
            if 2 <= gx <= 5:

                @pl.when(c // 8 == h)
                def _(mag=mag, gx=gx):
                    l_ref[block, gx - 2, 6] = mag[:8]
                    l_ref[block + 1, gx - 2, 6] = mag[8:]

        for k in range(21):
            gs = [g[k, t] for t in range(6)]
            for x in range(4):
                total = gs[x] + 2.0 * gs[x + 1] + gs[x + 2]
                box = (pltpu.roll(total, 2, 1) + 2.0 * total + pltpu.roll(total, 126, 1)) * 0.0625
                hi = box.astype(BF16)
                bh[k, pl.ds(y0, 16), pl.ds(x * 128, 128)] = hi
                bl[k, pl.ds(y0, 16), pl.ds(x * 128, 128)] = (box - hi.astype(F32)).astype(BF16)
        return 0

    lax.fori_loop(0, 16, strip, 0)

    def product(k, _):
        hi, lo = bh[k], bl[k]
        acc = jnp.dot(wh[...], lo, preferred_element_type=F32)
        acc += jnp.dot(wl[...], hi, preferred_element_type=F32)
        ff[k] = acc + jnp.dot(wh[...], hi, preferred_element_type=F32)
        return 0

    lax.fori_loop(0, 21, product, 0)

    lanes = lax.broadcasted_iota(jnp.int32, (8, 128), 1)

    def contract(c, sums):
        y0 = pl.multiple_of(c * 8, 8)
        lm_sum, mm_sum = 0.0, 0.0
        for x in range(4):
            f = [ff[k, pl.ds(y0, 8), pl.ds(x * 128, 128)] for k in range(21)]
            a, b, d = f[0], f[1], f[2]
            s, p, m = f[3:9], f[9:15], f[15:21]
            uu = [a * a, b * b, d * d, a * b, a * d, b * d]
            fmag = jnp.sqrt(
                2.0 * (s[0] * s[0] + s[1] * s[1] + s[2] * s[2])
                + 4.0 * (s[3] * s[3] + s[4] * s[4] + s[5] * s[5])
            )
            lm, mm = [], []
            for k in range(6):
                leo = p[k] - uu[k]
                l_ref[c, x, k] = leo
                mod = m[k] - 4.0 * fmag * s[k]
                lm.append(leo * mod)
                mm.append(mod * mod)
            lm_sum += lm[0] + lm[1] + lm[2] + 2.0 * (lm[3] + lm[4] + lm[5])
            mm_sum += mm[0] + mm[1] + mm[2] + 2.0 * (mm[3] + mm[4] + mm[5])
        hot = bins[1, pl.ds(pl.multiple_of(r0 + y0, 8), 8), :] == lanes
        num = sums[0] + jnp.where(hot, jnp.sum(lm_sum, axis=1, keepdims=True), 0.0)
        den = sums[1] + jnp.where(hot, jnp.sum(mm_sum, axis=1, keepdims=True), 0.0)
        return num, den

    zero = jnp.zeros((8, 128), F32)
    num, den = lax.fori_loop(0, 16, contract, (zero, zero))
    row = lax.broadcasted_iota(jnp.int32, (8, 128), 0)
    num = jnp.sum(num, axis=0, keepdims=True)
    den = jnp.sum(den, axis=0, keepdims=True)
    part_ref[...] = jnp.where(row == 0, num, jnp.where(row == 1, den, 0.0))


def give_back(l_ref, part_ref, o_ref, tot_ref, a1, a2, s1, ss1, rs1, ss2, rs2, sb, rb, local):
    px, pz, h, yy, xx = where_am_i()

    def peer(k):
        return ((h + k // 16) % 2) * 16 + ((yy + (k % 16) // 4) % 4) * 4 + (xx + k % 4) % 4

    barrier = pltpu.get_barrier_semaphore()
    for k in range(1, 32):
        pl.semaphore_signal(barrier, inc=1, device_id=(px, peer(k)), device_id_type=MESH)
    for k in range(1, 8):
        pl.semaphore_signal(barrier, inc=1, device_id=((px + k) % 8, pz), device_id_type=MESH)
    pl.semaphore_wait(barrier, 38)

    def small(k):
        return pltpu.make_async_remote_copy(
            src_ref=part_ref,
            dst_ref=a1.at[pz],
            send_sem=ss1.at[k],
            recv_sem=rs1.at[k],
            device_id=(px, peer(k)),
            device_id_type=MESH,
        )

    def second(k):
        return pltpu.make_async_remote_copy(
            src_ref=s1,
            dst_ref=a2.at[px],
            send_sem=ss2.at[k],
            recv_sem=rs2.at[k],
            device_id=((px + k) % 8, pz),
            device_id_type=MESH,
        )

    def big(k):
        return pltpu.make_async_remote_copy(
            src_ref=l_ref.at[peer(k) % 16],
            dst_ref=o_ref.at[pz % 16],
            send_sem=sb.at[k],
            recv_sem=rb.at[k],
            device_id=(px, peer(k)),
            device_id_type=MESH,
        )

    for k in range(1, 32):
        small(k).start()
    for k in ORDER:
        big(k).start()
    a1[pz] = part_ref[...]
    for k in range(1, 32):
        small(k).wait_recv()
    total = a1[0]
    for q in range(1, 32):
        total = total + a1[q]
    s1[...] = total
    a2[px] = total
    here = pltpu.make_async_copy(l_ref.at[pz % 16], o_ref.at[pz % 16], local.at[0])
    here.start()
    for k in range(1, 8):
        second(k).start()
    for k in range(1, 8):
        second(k).wait_recv()
    total = a2[0]
    for q in range(1, 8):
        total = total + a2[q]
    tot_ref[...] = total
    here.wait()
    for k in range(1, 32):
        small(k).wait_send()
    for k in range(1, 8):
        second(k).wait_send()
    for k in range(1, 16):
        big(k).wait()


def to_planes(tot_ref, pb_ref, o_ref, leo_ref, visc_ref, coef_ref, mix):
    pz = lax.axis_index("pz")
    per_bin = tot_ref[0:1, :] / jnp.maximum(tot_ref[1:2, :], 65536.0)
    per_bin = jnp.broadcast_to(per_bin, (128, 128)).T
    hot = lax.broadcasted_iota(jnp.int32, (128, 256), 0) == pb_ref[...]
    both = jnp.concatenate([per_bin, per_bin], axis=1)
    coef = jnp.sum(jnp.where(hot, both, 0.0), axis=0, keepdims=True)
    coef_ref[...] = coef
    at = lax.broadcasted_iota(jnp.int32, (1, 256), 1) - pz * 8
    low = lax.broadcasted_iota(jnp.int32, (64, 128), 1) < 64

    def plane(y, _):
        mine = jnp.sum(jnp.where(at == y, coef, 0.0), axis=1, keepdims=True)
        for f in range(7):
            m = o_ref[pl.ds(f * 8 + y, 64, stride=56), :]
            mix[f] = jnp.concatenate([m, m], axis=0).T
            v = jnp.where(low, mix[f, pl.ds(0, 64, stride=2), :], mix[f, pl.ds(1, 64, stride=2), :])
            if f < 6:
                leo_ref[f, y] = v
            else:
                visc_ref[y] = mine * v
        return 0

    lax.fori_loop(0, 8, plane, 0)


def spec(space):
    return pl.BlockSpec(memory_space=space)


def params(**kw):
    return pltpu.CompilerParams(vmem_limit_bytes=56 * 1024 * 1024, **kw)


DMA = pltpu.SemaphoreType.DMA


def local_step(velocity, filter_inverse, filter_block, plane_bin):
    edge = jax.ShapeDtypeStruct((48, 128), F32)
    rows, right, left = pl.pallas_call(
        to_columns,
        out_shape=(jax.ShapeDtypeStruct((68 * 24, 128), F32), edge, edge),
        in_specs=[spec(VMEM)],
        out_specs=(spec(VMEM),) * 3,
        scratch_shapes=[VMEM((3, 128, 128), F32)],
        compiler_params=params(),
        name="to_columns",
    )(velocity)
    below = lax.ppermute(right, "px", [(i, (i + 1) % 8) for i in range(8)])
    above = lax.ppermute(left, "px", [((i + 1) % 8, i) for i in range(8)])
    columns = pl.pallas_call(
        spread,
        out_shape=jax.ShapeDtypeStruct((8, 3, 256, 128), F32),
        in_specs=[spec(pl.ANY), spec(VMEM), spec(VMEM)],
        out_specs=spec(pl.ANY),
        scratch_shapes=[
            VMEM((68, 3, 8, 128), F32),
            VMEM((68, 3, 8, 128), F32),
            DMA((3,)),
            DMA((3,)),
            DMA((16,)),
            DMA((16,)),
            DMA((3, 16)),
            DMA((3, 16)),
            DMA((4,)),
        ],
        compiler_params=params(collective_id=0, has_side_effects=True),
        name="spread",
    )(rows.reshape(68, 3, 8, 128), below.reshape(2, 3, 8, 128), above.reshape(2, 3, 8, 128))
    bins = plane_bin.reshape(1, 256)
    leo, part = pl.pallas_call(
        math,
        out_shape=(
            jax.ShapeDtypeStruct((16, 4, 7, 8, 128), F32),
            jax.ShapeDtypeStruct((8, 128), F32),
        ),
        in_specs=[spec(VMEM)] * 4,
        out_specs=(spec(VMEM), spec(VMEM)),
        scratch_shapes=[
            VMEM((21, 6, 16, 128), F32),
            VMEM((21, 256, 512), BF16),
            VMEM((21, 256, 512), BF16),
            VMEM((21, 128, 512), F32),
            VMEM((128, 256), BF16),
            VMEM((128, 256), BF16),
            VMEM((2, 256, 128), jnp.int32),
        ],
        compiler_params=params(),
        name="math",
    )(columns, filter_inverse, filter_block.reshape(1, 256), bins)
    back, total = pl.pallas_call(
        give_back,
        out_shape=(
            jax.ShapeDtypeStruct((16, 4, 7, 8, 128), F32),
            jax.ShapeDtypeStruct((8, 128), F32),
        ),
        in_specs=[spec(VMEM)] * 2,
        out_specs=(spec(pl.ANY), spec(VMEM)),
        scratch_shapes=[
            VMEM((32, 8, 128), F32),
            VMEM((8, 8, 128), F32),
            VMEM((8, 128), F32),
            DMA((32,)),
            DMA((32,)),
            DMA((8,)),
            DMA((8,)),
            DMA((16,)),
            DMA((16,)),
            DMA((1,)),
        ],
        compiler_params=params(collective_id=1, has_side_effects=True),
        name="give_back",
    )(leo, part)
    leonard, viscosity, coefficient = pl.pallas_call(
        to_planes,
        out_shape=(
            jax.ShapeDtypeStruct((6, 8, 64, 128), F32),
            jax.ShapeDtypeStruct((8, 64, 128), F32),
            jax.ShapeDtypeStruct((1, 256), F32),
        ),
        in_specs=[spec(VMEM)] * 3,
        out_specs=(spec(VMEM),) * 3,
        scratch_shapes=[VMEM((7, 128, 128), F32)],
        compiler_params=params(),
        name="to_planes",
    )(total, bins, back.reshape(16 * 4 * 56, 128))
    return leonard, viscosity, coefficient.reshape(256)


def solution(mesh):
    return jax.shard_map(
        local_step,
        mesh=mesh,
        in_specs=(P(None, "pz", None, "px"), P(), P(), P()),
        out_specs=(P(None, "pz", None, "px"), P("pz", None, "px"), P()),
        check_vma=False,
    )
```

```python
import functools

import jax
import jax.numpy as jnp
from jax import lax
from jax.experimental import pallas as pl
from jax.experimental.pallas import tpu as pltpu
from jax.sharding import PartitionSpec as P

NBIN = 64
MESH = pl.DeviceIdType.MESH
F32 = jnp.float32
BF16 = jnp.bfloat16
VMEM = pltpu.VMEM
def to_columns(vel_ref, x_ref, right_ref, left_ref, mix):
    even = lax.broadcasted_iota(jnp.int32, (64, 128), 1) % 2 == 0

    def plane(y, _):
        for f in range(3):
            v = vel_ref[f, y]
            mix[f, pl.ds(0, 64, stride=2), :] = v
            mix[f, pl.ds(1, 64, stride=2), :] = v
            t = mix[f].T
            x_ref[pl.ds(48 + f * 8 + y, 64, stride=24), :] = jnp.where(even, t[:64], t[64:])
        return 0

    lax.fori_loop(0, 8, plane, 0)
    first, last = x_ref[48:96, :], x_ref[64 * 24 : 66 * 24, :]
    x_ref[0:48, :] = pltpu.roll(last, 1, 1)
    x_ref[66 * 24 : 68 * 24, :] = pltpu.roll(first, 127, 1)
    right_ref[...] = pltpu.roll(last, 127, 1)
    left_ref[...] = pltpu.roll(first, 1, 1)


ORDER = (10, 6, 14, 8, 9, 11, 2, 5, 15, 13, 7, 1, 3, 4, 12)


def where_am_i():
    px, pz = lax.axis_index("px"), lax.axis_index("pz")
    return px, pz, pz // 16, (pz % 16) // 4, pz % 4


def fields_of(u, gx, up, down):
    def d_x(f):
        return u[f][gx + 1] - u[f][gx - 1]

    def d_z(f):
        return pltpu.roll(u[f][gx], 126, 1) - pltpu.roll(u[f][gx], 2, 1)

    def d_y(f):
        return up[f] - down[f]

    t = [d_x(0), d_y(1), d_z(2), d_y(0) + d_x(1), d_z(0) + d_x(2), d_z(1) + d_y(2)]
    mag = twice_norm(t)
    a, b, c = u[0][gx], u[1][gx], u[2][gx]
    return [a, b, c] + t + [a * a, b * b, c * c, a * b, a * c, b * c] + [mag * q for q in t], mag


def twice_norm(t):
    return jnp.sqrt(
        2.0 * (t[0] * t[0] + t[1] * t[1] + t[2] * t[2]) + (t[3] * t[3] + t[4] * t[4] + t[5] * t[5])
    )


def column(row):
    return jnp.broadcast_to(row, (128, 256)).T


def core(
    x_ref, below_ref, above_ref, inv_ref, fb_ref, pb_ref, o_ref, tot_ref,
    rows, partner, r, g, bh, bl, ff, ww, bins, leo, part, a1, a2, s1,
    send_a, recv_a, send_b, recv_b, send_c, recv_c, ss1, rs1, ss2, rs2, sb, rb, local,
):
    px, pz, h, yy, xx = where_am_i()
    i = pz % 16
    other = 1 - h

    def mate(k):
        return ((yy + k // 4) % 4) * 4 + (xx + k % 4) % 4

    def peer(k):
        return ((h + k // 16) % 2) * 16 + mate(k % 16)

    def send(src, dst, sems, recvs, where):
        return pltpu.make_async_remote_copy(
            src_ref=src, dst_ref=dst, send_sem=sems, recv_sem=recvs, device_id=where, device_id_type=MESH
        )

    fetch = pltpu.make_async_copy(x_ref, rows, local.at[0])
    fetch.start()
    barrier = pltpu.get_barrier_semaphore()
    for k in range(1, 32):
        pl.semaphore_signal(barrier, inc=1, device_id=(px, peer(k)), device_id_type=MESH)
    for k in range(1, 8):
        pl.semaphore_signal(barrier, inc=1, device_id=((px + k) % 8, pz), device_id_type=MESH)
    fetch.wait()
    even = lax.broadcasted_iota(jnp.int32, (2, 3, 8, 128), 3) % 2 == 0
    rows[0:2] = jnp.where(even, below_ref[...], rows[0:2])
    rows[66:68] = jnp.where(even, rows[66:68], above_ref[...])
    pl.semaphore_wait(barrier, 38)

    own_planes = pl.ds(pl.multiple_of(pz * 8, 8), 8)
    their_planes = pl.ds(pl.multiple_of((other * 16 + i) * 8, 8), 8)

    def across(f):
        return send(rows.at[:, f], partner.at[:, f], send_a.at[f], recv_a.at[f], (px, other * 16 + i))

    def own(k):
        return send(
            rows.at[pl.ds(mate(k) * 4, 8)], r.at[:, :, own_planes, :],
            send_b.at[k], recv_b.at[k], (px, h * 16 + mate(k)),
        )

    def theirs(f, k):
        return send(
            partner.at[pl.ds(mate(k) * 4, 8), f], r.at[:, f, their_planes, :],
            send_c.at[f, k], recv_c.at[f, k], (px, h * 16 + mate(k)),
        )

    def there(f):
        return pltpu.make_async_copy(partner.at[pl.ds(i * 4, 8), f], r.at[:, f, their_planes, :], local.at[1 + f])

    for f in range(3):
        across(f).start()
    for k in ORDER:
        own(k).start()
    here = pltpu.make_async_copy(rows.at[pl.ds(i * 4, 8)], r.at[:, :, own_planes, :], local.at[0])
    here.start()

    r0 = pl.multiple_of(h * 128, 128)
    bins[0] = column(fb_ref[...])
    bins[1] = column(pb_ref[...])
    mine = bins[0, pl.ds(r0, 128), :]
    masked = jnp.where(jnp.concatenate([mine, mine], axis=1) == fb_ref[...], inv_ref[pl.ds(r0, 128), :], 0.0)
    w = masked / jnp.sum(masked, axis=1, keepdims=True) * 0.0625
    w_hi = w.astype(BF16)
    ww[0:128, :] = w_hi
    ww[128:256, :] = (w - w_hi.astype(F32)).astype(BF16)

    def strip(c, mags):
        y0 = pl.multiple_of(c * 16, 16)
        before = pl.multiple_of(jnp.maximum(y0 - 8, 0), 8)
        after = pl.multiple_of(jnp.minimum(y0 + 16, 248), 8)
        first, last = c == 0, c == 15
        u = [[r[x, f, pl.ds(y0, 16), :] for x in range(8)] for f in range(3)]
        for gx in range(1, 7):
            up, down = [], []
            for f in range(3):
                prev = jnp.where(first, 0.0, r[gx, f, pl.ds(before, 8), :])
                succ = jnp.where(last, 0.0, r[gx, f, pl.ds(after, 8), :])
                down.append(jnp.concatenate([prev[7:], u[f][gx][:15]], axis=0))
                up.append(jnp.concatenate([u[f][gx][1:], succ[:1]], axis=0))
            out, mag = fields_of(u, gx, up, down)
            for k in range(21):
                g[k, gx - 1] = out[k]
            if 2 <= gx <= 5:
                mags(c, gx - 2, mag)
        for k in range(21):
            gs = [g[k, t] for t in range(6)]
            pairs = [gs[t] + gs[t + 1] for t in range(5)]
            for x in range(4):
                total = pairs[x] + pairs[x + 1]
                total = total + pltpu.roll(total, 2, 1)
                box = total + pltpu.roll(total, 126, 1)
                hi = box.astype(BF16)
                bh[k, pl.ds(y0, 16), pl.ds(x * 128, 128)] = hi
                bl[k, pl.ds(y0, 16), pl.ds(x * 128, 128)] = (box - hi.astype(F32)).astype(BF16)

    def keep(c, x, mag):
        block = 2 * c - 16 * h
        leo[block, x, 6] = mag[:8]
        leo[block + 1, x, 6] = mag[8:]

    def keep_own(c, x, mag):
        @pl.when(c // 8 == h)
        def _():
            keep(jnp.clip(c, 8 * h, 8 * h + 7), x, mag)

    def early(t, _):
        strip(9 * h + t, keep)
        return 0

    def late(t, _):
        strip(7 * other + t, keep_own)
        return 0

    across(0).wait_recv()
    for k in ORDER:
        theirs(0, k).start()
    there(0).start()
    here.wait()
    for k in range(1, 16):
        own(k).wait_recv()
    lax.fori_loop(0, 7, early, 0)
    for f in (1, 2):
        across(f).wait_recv()
        for k in ORDER:
            theirs(f, k).start()
        there(f).start()
    for f in range(3):
        there(f).wait()
        for k in range(1, 16):
            theirs(f, k).wait_recv()
    lax.fori_loop(0, 9, late, 0)

    lanes = lax.broadcasted_iota(jnp.int32, (8, 128), 1)

    def products(x0):
        def product(q, _):
            for t in range(3):
                k = q * 3 + t
                hi = bh[k, :, pl.ds(x0 * 128, 256)]
                lo = bl[k, :, pl.ds(x0 * 128, 256)]
                both = jnp.dot(ww[...], hi, preferred_element_type=F32)
                rest = jnp.dot(ww[0:128, :], lo, preferred_element_type=F32)
                ff[k] = both[:128] + (both[128:] + rest)
            return 0

        lax.fori_loop(0, 7, product, 0)

    def contracts(x0, sums):
        def contract(c, sums):
            y0 = pl.multiple_of(c * 8, 8)
            lm_sum, mm_sum = 0.0, 0.0
            for x in range(2):
                f = [ff[k, pl.ds(y0, 8), pl.ds(x * 128, 128)] for k in range(21)]
                a, b, d = f[0], f[1], f[2]
                t, p, m = f[3:9], f[9:15], f[15:21]
                uu = [a * a, b * b, d * d, a * b, a * d, b * d]
                fmag = 4.0 * twice_norm(t)
                lm, mm = [], []
                for k in range(6):
                    stress = p[k] - uu[k]
                    leo[c, x0 + x, k] = stress
                    mod = m[k] - fmag * t[k]
                    lm.append(stress * mod)
                    mm.append(mod * mod)
                lm_sum += lm[0] + lm[1] + lm[2] + lm[3] + lm[4] + lm[5]
                mm_sum += 2.0 * (mm[0] + mm[1] + mm[2]) + (mm[3] + mm[4] + mm[5])
            hot = bins[1, pl.ds(pl.multiple_of(r0 + y0, 8), 8), :] == lanes
            num = sums[0] + jnp.where(hot, jnp.sum(lm_sum, axis=1, keepdims=True), 0.0)
            den = sums[1] + jnp.where(hot, jnp.sum(mm_sum, axis=1, keepdims=True), 0.0)
            return num, den

        return lax.fori_loop(0, 16, contract, sums)

    def big(half, k):
        return send(
            leo.at[mate(k), pl.ds(half * 2, 2)], o_ref.at[i, pl.ds(half * 2, 2)],
            sb.at[half, k], rb.at[half, k], (px, h * 16 + mate(k)),
        )

    def small(k):
        return send(part, a1.at[pz], ss1.at[k], rs1.at[k], (px, peer(k)))

    def second(k):
        return send(s1, a2.at[px], ss2.at[k], rs2.at[k], ((px + k) % 8, pz))

    zero = jnp.zeros((8, 128), F32)
    products(0)
    sums = contracts(0, (zero, zero))
    products(2)
    for k in ORDER:
        big(0, k).start()
    num, den = contracts(2, sums)
    row = lax.broadcasted_iota(jnp.int32, (8, 128), 0)
    num = jnp.sum(num, axis=0, keepdims=True) * 0.25
    den = jnp.sum(den, axis=0, keepdims=True) * 0.03125
    mine = jnp.where(row == 0, num, jnp.where(row == 1, den, 0.0))
    part[...] = mine
    a1[pz] = mine
    for f in range(3):
        across(f).wait_send()
        for k in range(1, 16):
            theirs(f, k).wait_send()
    for k in range(1, 16):
        own(k).wait_send()
    for k in range(1, 32):
        small(k).start()
    for k in ORDER:
        big(1, k).start()
    keep_here = pltpu.make_async_copy(leo.at[i], o_ref.at[i], local.at[0])
    keep_here.start()
    for k in range(1, 32):
        small(k).wait_recv()
    total = a1[0]
    for q in range(1, 32):
        total = total + a1[q]
    s1[...] = total
    a2[px] = total
    for k in range(1, 32):
        small(k).wait_send()
    for k in range(1, 8):
        second(k).start()
    for k in range(1, 8):
        second(k).wait_recv()
    total = a2[0]
    for q in range(1, 8):
        total = total + a2[q]
    tot_ref[...] = total
    keep_here.wait()
    for k in range(1, 8):
        second(k).wait_send()
    for half in range(2):
        for k in range(1, 16):
            big(half, k).wait()


def to_planes(tot_ref, pb_ref, o_ref, leo_ref, visc_ref, coef_ref, mix):
    pz = lax.axis_index("pz")
    per_bin = tot_ref[0:1, :] / jnp.maximum(tot_ref[1:2, :], 65536.0)
    per_bin = jnp.broadcast_to(per_bin, (128, 128)).T
    hot = lax.broadcasted_iota(jnp.int32, (128, 256), 0) == pb_ref[...]
    both = jnp.concatenate([per_bin, per_bin], axis=1)
    coef = jnp.sum(jnp.where(hot, both, 0.0), axis=0, keepdims=True)
    coef_ref[...] = coef
    at = lax.broadcasted_iota(jnp.int32, (1, 256), 1) - pz * 8
    low = lax.broadcasted_iota(jnp.int32, (64, 128), 1) < 64

    def plane(y, _):
        mine = jnp.sum(jnp.where(at == y, coef, 0.0), axis=1, keepdims=True)
        for f in range(7):
            m = o_ref[pl.ds(f * 8 + y, 64, stride=56), :]
            mix[f] = jnp.concatenate([m, m], axis=0).T
            v = jnp.where(low, mix[f, pl.ds(0, 64, stride=2), :], mix[f, pl.ds(1, 64, stride=2), :])
            if f < 6:
                leo_ref[f, y] = v
            else:
                visc_ref[y] = mine * 0.5 * v
        return 0

    lax.fori_loop(0, 8, plane, 0)


def spec(space):
    return pl.BlockSpec(memory_space=space)


def params(**kw):
    return pltpu.CompilerParams(vmem_limit_bytes=56 * 1024 * 1024, **kw)


DMA = pltpu.SemaphoreType.DMA


def local_step(velocity, filter_inverse, filter_block, plane_bin):
    edge = jax.ShapeDtypeStruct((48, 128), F32)
    rows, right, left = pl.pallas_call(
        to_columns,
        out_shape=(jax.ShapeDtypeStruct((68 * 24, 128), F32), edge, edge),
        in_specs=[spec(VMEM)],
        out_specs=(spec(VMEM),) * 3,
        scratch_shapes=[VMEM((3, 128, 128), F32)],
        compiler_params=params(),
        name="to_columns",
    )(velocity)
    below = lax.ppermute(right, "px", [(i, (i + 1) % 8) for i in range(8)])
    above = lax.ppermute(left, "px", [((i + 1) % 8, i) for i in range(8)])
    bins = plane_bin.reshape(1, 256)
    part = VMEM((68, 3, 8, 128), F32)
    back, total = pl.pallas_call(
        core,
        out_shape=(
            jax.ShapeDtypeStruct((16, 4, 7, 8, 128), F32),
            jax.ShapeDtypeStruct((8, 128), F32),
        ),
        in_specs=[spec(pl.ANY)] + [spec(VMEM)] * 5,
        out_specs=(spec(pl.ANY), spec(VMEM)),
        scratch_shapes=[
            part,
            part,
            VMEM((8, 3, 256, 128), F32),
            VMEM((21, 6, 16, 128), F32),
            VMEM((21, 256, 512), BF16),
            VMEM((21, 256, 512), BF16),
            VMEM((21, 128, 256), F32),
            VMEM((256, 256), BF16),
            VMEM((2, 256, 128), jnp.int32),
            VMEM((16, 4, 7, 8, 128), F32),
            VMEM((8, 128), F32),
            VMEM((32, 8, 128), F32),
            VMEM((8, 8, 128), F32),
            VMEM((8, 128), F32),
            DMA((3,)),
            DMA((3,)),
            DMA((16,)),
            DMA((16,)),
            DMA((3, 16)),
            DMA((3, 16)),
            DMA((32,)),
            DMA((32,)),
            DMA((8,)),
            DMA((8,)),
            DMA((2, 16)),
            DMA((2, 16)),
            DMA((4,)),
        ],
        compiler_params=params(collective_id=0, has_side_effects=True),
        name="core",
    )(
        rows.reshape(68, 3, 8, 128),
        below.reshape(2, 3, 8, 128),
        above.reshape(2, 3, 8, 128),
        filter_inverse,
        filter_block.reshape(1, 256),
        bins,
    )
    leonard, viscosity, coefficient = pl.pallas_call(
        to_planes,
        out_shape=(
            jax.ShapeDtypeStruct((6, 8, 64, 128), F32),
            jax.ShapeDtypeStruct((8, 64, 128), F32),
            jax.ShapeDtypeStruct((1, 256), F32),
        ),
        in_specs=[spec(VMEM)] * 3,
        out_specs=(spec(VMEM),) * 3,
        scratch_shapes=[VMEM((7, 128, 128), F32)],
        compiler_params=params(),
        name="to_planes",
    )(total, bins, back.reshape(16 * 4 * 56, 128))
    return leonard, viscosity, coefficient.reshape(256)


def solution(mesh):
    return jax.shard_map(
        local_step,
        mesh=mesh,
        in_specs=(P(None, "pz", None, "px"), P(), P(), P()),
        out_specs=(P(None, "pz", None, "px"), P("pz", None, "px"), P()),
        check_vma=False,
    )
```

```python
import functools

import jax
import jax.numpy as jnp
from jax import lax
from jax.experimental import pallas as pl
from jax.experimental.pallas import tpu as pltpu
from jax.sharding import PartitionSpec as P

NBIN = 64
MESH = pl.DeviceIdType.MESH
F32 = jnp.float32
BF16 = jnp.bfloat16
VMEM = pltpu.VMEM
def to_columns(vel_ref, x_ref, right_ref, left_ref, mix):
    even = lax.broadcasted_iota(jnp.int32, (64, 128), 1) % 2 == 0

    def plane(y, _):
        for f in range(3):
            v = vel_ref[f, y]
            mix[f, pl.ds(0, 64, stride=2), :] = v
            mix[f, pl.ds(1, 64, stride=2), :] = v
            t = mix[f].T
            x_ref[pl.ds(48 + f * 8 + y, 64, stride=24), :] = jnp.where(even, t[:64], t[64:])
        return 0

    lax.fori_loop(0, 8, plane, 0)
    first, last = x_ref[48:96, :], x_ref[64 * 24 : 66 * 24, :]
    x_ref[0:48, :] = pltpu.roll(last, 1, 1)
    x_ref[66 * 24 : 68 * 24, :] = pltpu.roll(first, 127, 1)
    right_ref[...] = pltpu.roll(last, 127, 1)
    left_ref[...] = pltpu.roll(first, 1, 1)


ORDER = (10, 6, 14, 8, 9, 11, 2, 5, 15, 13, 7, 1, 3, 4, 12)


def where_am_i():
    px, pz = lax.axis_index("px"), lax.axis_index("pz")
    return px, pz, pz // 16, (pz % 16) // 4, pz % 4


def fields_of(u, gx, up, down):
    def d_x(f):
        return u[f][gx + 1] - u[f][gx - 1]

    def d_z(f):
        return pltpu.roll(u[f][gx], 126, 1) - pltpu.roll(u[f][gx], 2, 1)

    def d_y(f):
        return up[f] - down[f]

    t = [d_x(0), d_y(1), d_z(2), d_y(0) + d_x(1), d_z(0) + d_x(2), d_z(1) + d_y(2)]
    mag = twice_norm(t)
    a, b, c = u[0][gx], u[1][gx], u[2][gx]
    return [a, b, c] + t + [a * a, b * b, c * c, a * b, a * c, b * c] + [mag * q for q in t], mag


def twice_norm(t):
    return jnp.sqrt(
        2.0 * (t[0] * t[0] + t[1] * t[1] + t[2] * t[2]) + (t[3] * t[3] + t[4] * t[4] + t[5] * t[5])
    )


def column(row):
    return jnp.broadcast_to(row, (128, 256)).T


def core(
    x_ref, below_ref, above_ref, inv_ref, fb_ref, pb_ref, o_ref, tot_ref,
    rows, partner, r, g, bh, bl, ff, ww, bins, leo, part, a1, a2, s1,
    send_a, recv_a, send_b, recv_b, send_c, recv_c, ss1, rs1, ss2, rs2, sb, rb, local,
):
    px, pz, h, yy, xx = where_am_i()
    i = pz % 16
    other = 1 - h

    def mate(k):
        return ((yy + k // 4) % 4) * 4 + (xx + k % 4) % 4

    def peer(k):
        return ((h + k // 16) % 2) * 16 + mate(k % 16)

    def send(src, dst, sems, recvs, where):
        return pltpu.make_async_remote_copy(
            src_ref=src, dst_ref=dst, send_sem=sems, recv_sem=recvs, device_id=where, device_id_type=MESH
        )

    fetch = pltpu.make_async_copy(x_ref, rows, local.at[0])
    fetch.start()
    barrier = pltpu.get_barrier_semaphore()
    for k in range(1, 32):
        pl.semaphore_signal(barrier, inc=1, device_id=(px, peer(k)), device_id_type=MESH)
    for k in range(1, 8):
        pl.semaphore_signal(barrier, inc=1, device_id=((px + k) % 8, pz), device_id_type=MESH)
    fetch.wait()
    even = lax.broadcasted_iota(jnp.int32, (2, 3, 8, 128), 3) % 2 == 0
    rows[0:2] = jnp.where(even, below_ref[...], rows[0:2])
    rows[66:68] = jnp.where(even, rows[66:68], above_ref[...])
    pl.semaphore_wait(barrier, 38)

    own_planes = pl.ds(pl.multiple_of(pz * 8, 8), 8)
    their_planes = pl.ds(pl.multiple_of((other * 16 + i) * 8, 8), 8)

    def across(f):
        return send(rows.at[:, f], partner.at[:, f], send_a.at[f], recv_a.at[f], (px, other * 16 + i))

    def own(k):
        return send(
            rows.at[pl.ds(mate(k) * 4, 8)], r.at[:, :, own_planes, :],
            send_b.at[k], recv_b.at[k], (px, h * 16 + mate(k)),
        )

    def theirs(f, k):
        return send(
            partner.at[pl.ds(mate(k) * 4, 8), f], r.at[:, f, their_planes, :],
            send_c.at[f, k], recv_c.at[f, k], (px, h * 16 + mate(k)),
        )

    def there(f):
        return pltpu.make_async_copy(partner.at[pl.ds(i * 4, 8), f], r.at[:, f, their_planes, :], local.at[1 + f])

    for f in range(3):
        across(f).start()
    for k in ORDER:
        own(k).start()
    here = pltpu.make_async_copy(rows.at[pl.ds(i * 4, 8)], r.at[:, :, own_planes, :], local.at[0])
    here.start()

    r0 = pl.multiple_of(h * 128, 128)
    bins[0] = column(fb_ref[...])
    bins[1] = column(pb_ref[...])
    mine = bins[0, pl.ds(r0, 128), :]
    masked = jnp.where(jnp.concatenate([mine, mine], axis=1) == fb_ref[...], inv_ref[pl.ds(r0, 128), :], 0.0)
    w = masked / jnp.sum(masked, axis=1, keepdims=True) * 0.0625
    w_hi = w.astype(BF16)
    ww[0:128, :] = w_hi
    ww[128:256, :] = (w - w_hi.astype(F32)).astype(BF16)

    def strip(c):
        y0 = pl.multiple_of(c * 16, 16)
        before = pl.multiple_of(jnp.maximum(y0 - 8, 0), 8)
        after = pl.multiple_of(jnp.minimum(y0 + 16, 248), 8)
        first, last = c == 0, c == 15
        u = [[r[x, f, pl.ds(y0, 16), :] for x in range(8)] for f in range(3)]
        for gx in range(1, 7):
            up, down = [], []
            for f in range(3):
                prev = jnp.where(first, 0.0, r[gx, f, pl.ds(before, 8), :])
                succ = jnp.where(last, 0.0, r[gx, f, pl.ds(after, 8), :])
                down.append(jnp.concatenate([prev[7:], u[f][gx][:15]], axis=0))
                up.append(jnp.concatenate([u[f][gx][1:], succ[:1]], axis=0))
            out, mag = fields_of(u, gx, up, down)
            for k in range(21):
                g[k, gx - 1] = out[k]
            if 2 <= gx <= 5:
                keep(c, gx - 2, mag)
        for k in range(21):
            gs = [g[k, t] for t in range(6)]
            pairs = [gs[t] + gs[t + 1] for t in range(5)]
            for x in range(4):
                total = pairs[x] + pairs[x + 1]
                box = (pltpu.roll(total, 2, 1) + pltpu.roll(total, 126, 1)) + (total + total)
                hi = box.astype(BF16)
                bh[k, pl.ds(y0, 16), pl.ds(x * 128, 128)] = hi
                bl[k, pl.ds(y0, 16), pl.ds(x * 128, 128)] = (box - hi.astype(F32)).astype(BF16)

    def keep(c, x, mag):
        block = jnp.where(c // 8 == h, 2 * c - 16 * h, 16)
        leo[block, x, 6] = mag[:8]
        leo[block + 1, x, 6] = mag[8:]

    def early(t, _):
        strip(9 * h + t)
        return 0

    def late(t, _):
        strip(7 * other + t)
        return 0

    across(0).wait_recv()
    for k in ORDER:
        theirs(0, k).start()
    there(0).start()
    here.wait()
    for k in range(1, 16):
        own(k).wait_recv()
    lax.fori_loop(0, 7, early, 0)
    for f in (1, 2):
        across(f).wait_recv()
        for k in ORDER:
            theirs(f, k).start()
        there(f).start()
    for f in range(3):
        there(f).wait()
        for k in range(1, 16):
            theirs(f, k).wait_recv()
    lax.fori_loop(0, 9, late, 0)

    lanes = lax.broadcasted_iota(jnp.int32, (8, 128), 1)

    def products(x0):
        def product(q, _):
            for t in range(3):
                k = q * 3 + t
                hi = bh[k, :, pl.ds(x0 * 128, 256)]
                lo = bl[k, :, pl.ds(x0 * 128, 256)]
                both = jnp.dot(ww[...], hi, preferred_element_type=F32)
                rest = jnp.dot(ww[0:128, :], lo, preferred_element_type=F32)
                ff[k] = both[:128] + (both[128:] + rest)
            return 0

        lax.fori_loop(0, 7, product, 0)

    def contracts(x0, sums):
        def contract(c, sums):
            y0 = pl.multiple_of(c * 8, 8)
            lm_sum, mm_sum = 0.0, 0.0
            for x in range(2):
                f = [ff[k, pl.ds(y0, 8), pl.ds(x * 128, 128)] for k in range(21)]
                a, b, d = f[0], f[1], f[2]
                t, p, m = f[3:9], f[9:15], f[15:21]
                uu = [a * a, b * b, d * d, a * b, a * d, b * d]
                fmag = 4.0 * twice_norm(t)
                lm, mm = [], []
                for k in range(6):
                    stress = p[k] - uu[k]
                    leo[c, x0 + x, k] = stress
                    mod = m[k] - fmag * t[k]
                    lm.append(stress * mod)
                    mm.append(mod * mod)
                lm_sum += lm[0] + lm[1] + lm[2] + lm[3] + lm[4] + lm[5]
                mm_sum += 2.0 * (mm[0] + mm[1] + mm[2]) + (mm[3] + mm[4] + mm[5])
            hot = bins[1, pl.ds(pl.multiple_of(r0 + y0, 8), 8), :] == lanes
            num = sums[0] + jnp.where(hot, jnp.sum(lm_sum, axis=1, keepdims=True), 0.0)
            den = sums[1] + jnp.where(hot, jnp.sum(mm_sum, axis=1, keepdims=True), 0.0)
            return num, den

        return lax.fori_loop(0, 16, contract, sums)

    def big(half, k):
        return send(
            leo.at[mate(k), pl.ds(half * 2, 2)], o_ref.at[i, pl.ds(half * 2, 2)],
            sb.at[half, k], rb.at[half, k], (px, h * 16 + mate(k)),
        )

    def small(k):
        return send(part, a1.at[pz], ss1.at[k], rs1.at[k], (px, peer(k)))

    def second(k):
        return send(s1, a2.at[px], ss2.at[k], rs2.at[k], ((px + k) % 8, pz))

    zero = jnp.zeros((8, 128), F32)
    products(0)
    sums = contracts(0, (zero, zero))
    products(2)
    for k in ORDER:
        big(0, k).start()
    num, den = contracts(2, sums)
    row = lax.broadcasted_iota(jnp.int32, (8, 128), 0)
    num = jnp.sum(num, axis=0, keepdims=True) * 0.25
    den = jnp.sum(den, axis=0, keepdims=True) * 0.03125
    mine = jnp.where(row == 0, num, jnp.where(row == 1, den, 0.0))
    part[...] = mine
    a1[pz] = mine
    for f in range(3):
        across(f).wait_send()
        for k in range(1, 16):
            theirs(f, k).wait_send()
    for k in range(1, 16):
        own(k).wait_send()
    for k in range(1, 32):
        small(k).start()
    for k in ORDER:
        big(1, k).start()
    keep_here = pltpu.make_async_copy(leo.at[i], o_ref.at[i], local.at[0])
    keep_here.start()
    for k in range(1, 32):
        small(k).wait_recv()
    total = a1[0]
    for q in range(1, 32):
        total = total + a1[q]
    s1[...] = total
    a2[px] = total
    for k in range(1, 32):
        small(k).wait_send()
    for k in range(1, 8):
        second(k).start()
    for k in range(1, 8):
        second(k).wait_recv()
    total = a2[0]
    for q in range(1, 8):
        total = total + a2[q]
    tot_ref[...] = total
    keep_here.wait()
    for k in range(1, 8):
        second(k).wait_send()
    for half in range(2):
        for k in range(1, 16):
            big(half, k).wait()


def to_planes(tot_ref, pb_ref, o_ref, leo_ref, visc_ref, coef_ref, mix):
    pz = lax.axis_index("pz")
    per_bin = tot_ref[0:1, :] / jnp.maximum(tot_ref[1:2, :], 65536.0)
    per_bin = jnp.broadcast_to(per_bin, (128, 128)).T
    hot = lax.broadcasted_iota(jnp.int32, (128, 256), 0) == pb_ref[...]
    both = jnp.concatenate([per_bin, per_bin], axis=1)
    coef = jnp.sum(jnp.where(hot, both, 0.0), axis=0, keepdims=True)
    coef_ref[...] = coef
    at = lax.broadcasted_iota(jnp.int32, (1, 256), 1) - pz * 8
    low = lax.broadcasted_iota(jnp.int32, (64, 128), 1) < 64

    def plane(y, _):
        mine = jnp.sum(jnp.where(at == y, coef, 0.0), axis=1, keepdims=True)
        for f in range(7):
            m = o_ref[pl.ds(f * 8 + y, 64, stride=56), :]
            mix[f] = jnp.concatenate([m, m], axis=0).T
            v = jnp.where(low, mix[f, pl.ds(0, 64, stride=2), :], mix[f, pl.ds(1, 64, stride=2), :])
            if f < 6:
                leo_ref[f, y] = v
            else:
                visc_ref[y] = mine * 0.5 * v
        return 0

    lax.fori_loop(0, 8, plane, 0)


def spec(space):
    return pl.BlockSpec(memory_space=space)


def params(**kw):
    return pltpu.CompilerParams(vmem_limit_bytes=56 * 1024 * 1024, **kw)


DMA = pltpu.SemaphoreType.DMA


def local_step(velocity, filter_inverse, filter_block, plane_bin):
    edge = jax.ShapeDtypeStruct((48, 128), F32)
    rows, right, left = pl.pallas_call(
        to_columns,
        out_shape=(jax.ShapeDtypeStruct((68 * 24, 128), F32), edge, edge),
        in_specs=[spec(VMEM)],
        out_specs=(spec(VMEM),) * 3,
        scratch_shapes=[VMEM((3, 128, 128), F32)],
        compiler_params=params(),
        name="to_columns",
    )(velocity)
    below = lax.ppermute(right, "px", [(i, (i + 1) % 8) for i in range(8)])
    above = lax.ppermute(left, "px", [((i + 1) % 8, i) for i in range(8)])
    bins = plane_bin.reshape(1, 256)
    part = VMEM((68, 3, 8, 128), F32)
    back, total = pl.pallas_call(
        core,
        out_shape=(
            jax.ShapeDtypeStruct((16, 4, 7, 8, 128), F32),
            jax.ShapeDtypeStruct((8, 128), F32),
        ),
        in_specs=[spec(pl.ANY)] + [spec(VMEM)] * 5,
        out_specs=(spec(pl.ANY), spec(VMEM)),
        scratch_shapes=[
            part,
            part,
            VMEM((8, 3, 256, 128), F32),
            VMEM((21, 6, 16, 128), F32),
            VMEM((21, 256, 512), BF16),
            VMEM((21, 256, 512), BF16),
            VMEM((21, 128, 256), F32),
            VMEM((256, 256), BF16),
            VMEM((2, 256, 128), jnp.int32),
            VMEM((18, 4, 7, 8, 128), F32),
            VMEM((8, 128), F32),
            VMEM((32, 8, 128), F32),
            VMEM((8, 8, 128), F32),
            VMEM((8, 128), F32),
            DMA((3,)),
            DMA((3,)),
            DMA((16,)),
            DMA((16,)),
            DMA((3, 16)),
            DMA((3, 16)),
            DMA((32,)),
            DMA((32,)),
            DMA((8,)),
            DMA((8,)),
            DMA((2, 16)),
            DMA((2, 16)),
            DMA((4,)),
        ],
        compiler_params=params(collective_id=0, has_side_effects=True),
        name="core",
    )(
        rows.reshape(68, 3, 8, 128),
        below.reshape(2, 3, 8, 128),
        above.reshape(2, 3, 8, 128),
        filter_inverse,
        filter_block.reshape(1, 256),
        bins,
    )
    leonard, viscosity, coefficient = pl.pallas_call(
        to_planes,
        out_shape=(
            jax.ShapeDtypeStruct((6, 8, 64, 128), F32),
            jax.ShapeDtypeStruct((8, 64, 128), F32),
            jax.ShapeDtypeStruct((1, 256), F32),
        ),
        in_specs=[spec(VMEM)] * 3,
        out_specs=(spec(VMEM),) * 3,
        scratch_shapes=[VMEM((7, 128, 128), F32)],
        compiler_params=params(),
        name="to_planes",
    )(total, bins, back.reshape(16 * 4 * 56, 128))
    return leonard, viscosity, coefficient.reshape(256)


def solution(mesh):
    return jax.shard_map(
        local_step,
        mesh=mesh,
        in_specs=(P(None, "pz", None, "px"), P(), P(), P()),
        out_specs=(P(None, "pz", None, "px"), P("pz", None, "px"), P()),
        check_vma=False,
    )
```

```python
import functools

import jax
import jax.numpy as jnp
from jax import lax
from jax.experimental import pallas as pl
from jax.experimental.pallas import tpu as pltpu
from jax.sharding import PartitionSpec as P

NBIN = 64
MESH = pl.DeviceIdType.MESH
F32 = jnp.float32
BF16 = jnp.bfloat16
VMEM = pltpu.VMEM
ORDER = (10, 6, 14, 8, 9, 11, 2, 5, 15, 13, 7, 1, 3, 4, 12)


def where_am_i():
    px, pz = lax.axis_index("px"), lax.axis_index("pz")
    return px, pz, pz // 16, (pz % 16) // 4, pz % 4


def fields_of(u, gx, up, down):
    def d_x(f):
        return u[f][gx + 1] - u[f][gx - 1]

    def d_z(f):
        return pltpu.roll(u[f][gx], 126, 1) - pltpu.roll(u[f][gx], 2, 1)

    def d_y(f):
        return up[f] - down[f]

    t = [d_x(0), d_y(1), d_z(2), d_y(0) + d_x(1), d_z(0) + d_x(2), d_z(1) + d_y(2)]
    mag = twice_norm(t)
    a, b, c = u[0][gx], u[1][gx], u[2][gx]
    return [a, b, c] + t + [a * a, b * b, c * c, a * b, a * c, b * c] + [mag * q for q in t], mag


def twice_norm(t):
    return jnp.sqrt(
        2.0 * (t[0] * t[0] + t[1] * t[1] + t[2] * t[2]) + (t[3] * t[3] + t[4] * t[4] + t[5] * t[5])
    )


def column(row):
    return jnp.broadcast_to(row, (128, 256)).T


def core(
    vel_ref, inv_ref, fb_ref, pb_ref, o_ref, tot_ref,
    rows, partner, edge, near, mix, r, g, bh, bl, ff, ww, bins, leo, part, a1, a2, s1,
    send_a, recv_a, send_b, recv_b, send_c, recv_c, ss0, rs0, ss1, rs1, ss2, rs2, sb, rb, local,
):
    px, pz, h, yy, xx = where_am_i()
    i = pz % 16
    other = 1 - h

    def mate(k):
        return ((yy + k // 4) % 4) * 4 + (xx + k % 4) % 4

    def twin(k):
        return (px + k % 8) % 8, ((h + k // 8) % 2) * 16 + i

    def send(src, dst, sems, recvs, where):
        return pltpu.make_async_remote_copy(
            src_ref=src, dst_ref=dst, send_sem=sems, recv_sem=recvs, device_id=where, device_id_type=MESH
        )

    barrier = pltpu.get_barrier_semaphore()
    for k in range(1, 16):
        pl.semaphore_signal(barrier, inc=1, device_id=(px, h * 16 + mate(k)), device_id_type=MESH)
        pl.semaphore_signal(barrier, inc=1, device_id=twin(k), device_id_type=MESH)

    flat = rows.reshape(68 * 24, 128)
    lane = lax.broadcasted_iota(jnp.int32, (64, 128), 1)
    even = lane % 2 == 0

    def plane(y, _):
        for f in range(3):
            v = vel_ref[f, y]
            mix[f, pl.ds(0, 64, stride=2), :] = v
            mix[f, pl.ds(1, 64, stride=2), :] = v
            t = mix[f].T
            flat[pl.ds(48 + f * 8 + y, 64, stride=24), :] = jnp.where(even, t[:64], t[64:])
        return 0

    lax.fori_loop(0, 8, plane, 0)
    first, last = flat[48:96, :], flat[64 * 24 : 66 * 24, :]
    edge[0] = pltpu.roll(last, 127, 1)
    edge[1] = pltpu.roll(first, 1, 1)
    pl.semaphore_wait(barrier, 30)

    own_planes = pl.ds(pl.multiple_of(pz * 8, 8), 8)
    their_planes = pl.ds(pl.multiple_of((other * 16 + i) * 8, 8), 8)

    def across(n):
        piece = (
            (pl.ds(2, 64), 0),
            (pl.ds(2, 64), 1),
            (pl.ds(2, 40), 2),
            (pl.ds(42, 24), 2),
            (pl.ds(0, 2), slice(None)),
            (pl.ds(66, 2), slice(None)),
        )[n]
        return send(rows.at[piece], partner.at[piece], send_a.at[n], recv_a.at[n], (px, other * 16 + i))

    def sideways(n):
        return send(edge.at[n], near.at[n], ss0.at[n], rs0.at[n], ((px + (1, 7)[n]) % 8, pz))

    def own(k):
        return send(
            rows.at[pl.ds(mate(k) * 4, 8)], r.at[:, :, own_planes, :],
            send_b.at[k], recv_b.at[k], (px, h * 16 + mate(k)),
        )

    def theirs(f, k):
        return send(
            partner.at[pl.ds(mate(k) * 4, 8), f], r.at[:, f, their_planes, :],
            send_c.at[f, k], recv_c.at[f, k], (px, h * 16 + mate(k)),
        )

    def there(f):
        return pltpu.make_async_copy(partner.at[pl.ds(i * 4, 8), f], r.at[:, f, their_planes, :], local.at[1 + f])

    sideways(0).start()
    sideways(1).start()
    across(0).start()
    for k in ORDER:

        @pl.when(mate(k) % 15 != 0)
        def _(k=k):
            own(k).start()

    sideways(0).wait_recv()
    sideways(1).wait_recv()
    even = lax.broadcasted_iota(jnp.int32, (48, 128), 1) % 2 == 0
    flat[0:48, :] = jnp.where(even, near[0], pltpu.roll(last, 1, 1))
    flat[66 * 24 : 68 * 24, :] = jnp.where(even, pltpu.roll(first, 127, 1), near[1])

    r0 = pl.multiple_of(h * 128, 128)
    bins[0] = column(fb_ref[...])
    bins[1] = column(pb_ref[...])
    mine = bins[0, pl.ds(r0, 128), :]
    masked = jnp.where(jnp.concatenate([mine, mine], axis=1) == fb_ref[...], inv_ref[pl.ds(r0, 128), :], 0.0)
    w = masked / jnp.sum(masked, axis=1, keepdims=True) * 0.0625
    w_hi = w.astype(BF16)
    ww[0:128, :] = w_hi
    ww[128:256, :] = (w - w_hi.astype(F32)).astype(BF16)

    for n in (4, 5, 1, 2, 3):
        across(n).start()
    for k in ORDER:

        @pl.when(mate(k) % 15 == 0)
        def _(k=k):
            own(k).start()

    here = pltpu.make_async_copy(rows.at[pl.ds(i * 4, 8)], r.at[:, :, own_planes, :], local.at[0])
    here.start()

    def strip(c):
        y0 = pl.multiple_of(c * 16, 16)
        before = pl.multiple_of(jnp.maximum(y0 - 8, 0), 8)
        after = pl.multiple_of(jnp.minimum(y0 + 16, 248), 8)
        first, last = c == 0, c == 15
        u = [[r[x, f, pl.ds(y0, 16), :] for x in range(8)] for f in range(3)]
        for gx in range(1, 7):
            up, down = [], []
            for f in range(3):
                prev = jnp.where(first, 0.0, r[gx, f, pl.ds(before, 8), :])
                succ = jnp.where(last, 0.0, r[gx, f, pl.ds(after, 8), :])
                down.append(jnp.concatenate([prev[7:], u[f][gx][:15]], axis=0))
                up.append(jnp.concatenate([u[f][gx][1:], succ[:1]], axis=0))
            out, mag = fields_of(u, gx, up, down)
            for k in range(21):
                g[k, gx - 1] = out[k]
            if 2 <= gx <= 5:
                keep(c, gx - 2, mag)
        for k in range(21):
            gs = [g[k, t] for t in range(6)]
            pairs = [gs[t] + gs[t + 1] for t in range(5)]
            for x in range(4):
                total = pairs[x] + pairs[x + 1]
                box = (pltpu.roll(total, 2, 1) + pltpu.roll(total, 126, 1)) + (total + total)
                hi = box.astype(BF16)
                bh[k, pl.ds(y0, 16), pl.ds(x * 128, 128)] = hi
                bl[k, pl.ds(y0, 16), pl.ds(x * 128, 128)] = (box - hi.astype(F32)).astype(BF16)

    def keep(c, x, mag):
        block = jnp.where(c // 8 == h, 2 * c - 16 * h, 16)
        leo[block, x, 6] = mag[:8]
        leo[block + 1, x, 6] = mag[8:]

    def early(t, _):
        strip(9 * h + t)
        return 0

    def late(t, _):
        strip(7 * other + t)
        return 0

    across(0).wait_recv()
    across(4).wait_recv()
    across(5).wait_recv()
    for k in ORDER:
        theirs(0, k).start()
    there(0).start()
    here.wait()
    for k in range(1, 16):
        own(k).wait_recv()
    lax.fori_loop(0, 7, early, 0)
    across(1).wait_recv()
    for k in ORDER:
        theirs(1, k).start()
    there(1).start()
    across(2).wait_recv()
    for k in ORDER:

        @pl.when(mate(k) <= 8)
        def _(k=k):
            theirs(2, k).start()

    across(3).wait_recv()
    for k in ORDER:

        @pl.when(mate(k) > 8)
        def _(k=k):
            theirs(2, k).start()

    there(2).start()
    for f in range(3):
        there(f).wait()
        for k in range(1, 16):
            theirs(f, k).wait_recv()
    lax.fori_loop(0, 9, late, 0)

    lanes = lax.broadcasted_iota(jnp.int32, (8, 128), 1)

    def products(x0, start, stop):
        def product(q, _):
            for t in range(3):
                k = q * 3 + t
                hi = bh[k, :, pl.ds(x0 * 128, 256)]
                lo = bl[k, :, pl.ds(x0 * 128, 256)]
                both = jnp.dot(ww[...], hi, preferred_element_type=F32)
                rest = jnp.dot(ww[0:128, :], lo, preferred_element_type=F32)
                ff[k] = both[:128] + (both[128:] + rest)
            return 0

        lax.fori_loop(start, stop, product, 0)

    def contracts(x0, sums):
        def contract(c, sums):
            y0 = pl.multiple_of(c * 8, 8)
            lm_sum, mm_sum = 0.0, 0.0
            for x in range(2):
                f = [ff[k, pl.ds(y0, 8), pl.ds(x * 128, 128)] for k in range(21)]
                a, b, d = f[0], f[1], f[2]
                t, p, m = f[3:9], f[9:15], f[15:21]
                uu = [a * a, b * b, d * d, a * b, a * d, b * d]
                fmag = 4.0 * twice_norm(t)
                lm, mm = [], []
                for k in range(6):
                    stress = p[k] - uu[k]
                    leo[c, x0 + x, k] = stress
                    mod = m[k] - fmag * t[k]
                    lm.append(stress * mod)
                    mm.append(mod * mod)
                lm_sum += lm[0] + lm[1] + lm[2] + lm[3] + lm[4] + lm[5]
                mm_sum += 2.0 * (mm[0] + mm[1] + mm[2]) + (mm[3] + mm[4] + mm[5])
            hot = bins[1, pl.ds(pl.multiple_of(r0 + y0, 8), 8), :] == lanes
            num = sums[0] + jnp.where(hot, jnp.sum(lm_sum, axis=1, keepdims=True), 0.0)
            den = sums[1] + jnp.where(hot, jnp.sum(mm_sum, axis=1, keepdims=True), 0.0)
            return num, den

        return lax.fori_loop(0, 16, contract, sums)

    def big(half, k):
        return send(
            leo.at[mate(k), pl.ds(half * 2, 2)], o_ref.at[i, pl.ds(half * 2, 2)],
            sb.at[half, k], rb.at[half, k], (px, h * 16 + mate(k)),
        )

    def small(k):
        return send(part, a1.at[h * 8 + px], ss1.at[k], rs1.at[k], twin(k))

    def second(k):
        return send(s1, a2.at[i], ss2.at[k], rs2.at[k], (px, h * 16 + mate(k)))

    zero = jnp.zeros((8, 128), F32)
    products(0, 0, 7)
    sums = contracts(0, (zero, zero))
    products(2, 0, 1)
    for k in ORDER:
        big(0, k).start()
    products(2, 1, 7)
    num, den = contracts(2, sums)
    row = lax.broadcasted_iota(jnp.int32, (8, 128), 0)
    num = jnp.sum(num, axis=0, keepdims=True) * 0.25
    den = jnp.sum(den, axis=0, keepdims=True) * 0.03125
    mine = jnp.where(row == 0, num, jnp.where(row == 1, den, 0.0))
    part[...] = mine
    a1[h * 8 + px] = mine
    for n in range(6):
        across(n).wait_send()
    for n in range(2):
        sideways(n).wait_send()
    for k in range(1, 16):
        own(k).wait_send()
        for f in range(3):
            theirs(f, k).wait_send()
    for k in range(1, 16):
        small(k).start()
    for k in ORDER[:6]:
        big(1, k).start()
    keep_here = pltpu.make_async_copy(leo.at[i], o_ref.at[i], local.at[0])
    keep_here.start()
    for k in range(1, 16):
        small(k).wait_recv()
    total = a1[0]
    for q in range(1, 16):
        total = total + a1[q]
    s1[...] = total
    a2[i] = total
    for k in range(1, 16):
        small(k).wait_send()
    for k in range(1, 16):
        second(k).start()
    for k in ORDER[6:]:
        big(1, k).start()
    for k in range(1, 16):
        second(k).wait_recv()
    total = a2[0]
    for q in range(1, 16):
        total = total + a2[q]
    tot_ref[...] = total
    keep_here.wait()
    for k in range(1, 16):
        second(k).wait_send()
    for half in range(2):
        for k in range(1, 16):
            big(half, k).wait()


def to_planes(tot_ref, pb_ref, o_ref, leo_ref, visc_ref, coef_ref, mix):
    pz = lax.axis_index("pz")
    per_bin = tot_ref[0:1, :] / jnp.maximum(tot_ref[1:2, :], 65536.0)
    per_bin = jnp.broadcast_to(per_bin, (128, 128)).T
    hot = lax.broadcasted_iota(jnp.int32, (128, 256), 0) == pb_ref[...]
    both = jnp.concatenate([per_bin, per_bin], axis=1)
    coef = jnp.sum(jnp.where(hot, both, 0.0), axis=0, keepdims=True)
    coef_ref[...] = coef
    at = lax.broadcasted_iota(jnp.int32, (1, 256), 1) - pz * 8
    low = lax.broadcasted_iota(jnp.int32, (64, 128), 1) < 64

    def plane(y, _):
        mine = jnp.sum(jnp.where(at == y, coef, 0.0), axis=1, keepdims=True)
        for f in range(7):
            m = o_ref[pl.ds(f * 8 + y, 64, stride=56), :]
            mix[f] = jnp.concatenate([m, m], axis=0).T
            v = jnp.where(low, mix[f, pl.ds(0, 64, stride=2), :], mix[f, pl.ds(1, 64, stride=2), :])
            if f < 6:
                leo_ref[f, y] = v
            else:
                visc_ref[y] = mine * 0.5 * v
        return 0

    lax.fori_loop(0, 8, plane, 0)


def spec(space):
    return pl.BlockSpec(memory_space=space)


def params(**kw):
    return pltpu.CompilerParams(vmem_limit_bytes=56 * 1024 * 1024, **kw)


DMA = pltpu.SemaphoreType.DMA


def local_step(velocity, filter_inverse, filter_block, plane_bin):
    bins = plane_bin.reshape(1, 256)
    part = VMEM((68, 3, 8, 128), F32)
    back, total = pl.pallas_call(
        core,
        out_shape=(
            jax.ShapeDtypeStruct((16, 4, 7, 8, 128), F32),
            jax.ShapeDtypeStruct((8, 128), F32),
        ),
        in_specs=[spec(VMEM)] * 4,
        out_specs=(spec(pl.ANY), spec(VMEM)),
        scratch_shapes=[
            part,
            part,
            VMEM((2, 48, 128), F32),
            VMEM((2, 48, 128), F32),
            VMEM((3, 128, 128), F32),
            VMEM((8, 3, 256, 128), F32),
            VMEM((21, 6, 16, 128), F32),
            VMEM((21, 256, 512), BF16),
            VMEM((21, 256, 512), BF16),
            VMEM((21, 128, 256), F32),
            VMEM((256, 256), BF16),
            VMEM((2, 256, 128), jnp.int32),
            VMEM((18, 4, 7, 8, 128), F32),
            VMEM((8, 128), F32),
            VMEM((16, 8, 128), F32),
            VMEM((16, 8, 128), F32),
            VMEM((8, 128), F32),
            DMA((6,)),
            DMA((6,)),
            DMA((16,)),
            DMA((16,)),
            DMA((3, 16)),
            DMA((3, 16)),
            DMA((2,)),
            DMA((2,)),
            DMA((16,)),
            DMA((16,)),
            DMA((16,)),
            DMA((16,)),
            DMA((2, 16)),
            DMA((2, 16)),
            DMA((4,)),
        ],
        compiler_params=params(collective_id=0, has_side_effects=True),
        name="core",
    )(
        velocity,
        filter_inverse,
        filter_block.reshape(1, 256),
        bins,
    )
    leonard, viscosity, coefficient = pl.pallas_call(
        to_planes,
        out_shape=(
            jax.ShapeDtypeStruct((6, 8, 64, 128), F32),
            jax.ShapeDtypeStruct((8, 64, 128), F32),
            jax.ShapeDtypeStruct((1, 256), F32),
        ),
        in_specs=[spec(VMEM)] * 3,
        out_specs=(spec(VMEM),) * 3,
        scratch_shapes=[VMEM((7, 128, 128), F32)],
        compiler_params=params(),
        name="to_planes",
    )(total, bins, back.reshape(16 * 4 * 56, 128))
    return leonard, viscosity, coefficient.reshape(256)


def solution(mesh):
    return jax.shard_map(
        local_step,
        mesh=mesh,
        in_specs=(P(None, "pz", None, "px"), P(), P(), P()),
        out_specs=(P(None, "pz", None, "px"), P("pz", None, "px"), P()),
        check_vma=False,
    )
```

```python
import functools

import jax
import jax.numpy as jnp
from jax import lax
from jax.experimental import pallas as pl
from jax.experimental.pallas import tpu as pltpu
from jax.sharding import PartitionSpec as P

NBIN = 64
MESH = pl.DeviceIdType.MESH
F32 = jnp.float32
BF16 = jnp.bfloat16
VMEM = pltpu.VMEM
ORDER = (10, 6, 14, 8, 9, 11, 2, 5, 15, 13, 7, 1, 3, 4, 12)


def where_am_i():
    px, pz = lax.axis_index("px"), lax.axis_index("pz")
    return px, pz, pz // 16, (pz % 16) // 4, pz % 4


SLOT = (0, 1, 8, 2, 3, 9, 4, 10, 11, 5, 6, 12, 7, 13, 14, 15, 16, 17, 18, 19, 20)
EARLY = 8


def fields_of(u, gx, up, down):
    def d_x(f):
        return u[f][gx + 1] - u[f][gx - 1]

    def d_z(f):
        return pltpu.roll(u[f][gx], 126, 1) - pltpu.roll(u[f][gx], 2, 1)

    def d_y(f):
        return up[f] - down[f]

    t = [d_x(0), d_y(1), d_z(2), d_y(0) + d_x(1), d_z(0) + d_x(2), d_z(1) + d_y(2)]
    mag = twice_norm(t)
    a, b, c = u[0][gx], u[1][gx], u[2][gx]
    return [a, b, c] + t + [a * a, b * b, c * c, a * b, a * c, b * c] + [mag * q for q in t], mag


def twice_norm(t):
    return jnp.sqrt(
        2.0 * (t[0] * t[0] + t[1] * t[1] + t[2] * t[2]) + (t[3] * t[3] + t[4] * t[4] + t[5] * t[5])
    )


def column(row):
    return jnp.broadcast_to(row, (128, 256)).T


def core(
    vel_ref, inv_ref, fb_ref, pb_ref, o_ref, om_ref, tot_ref,
    rows, partner, edge, near, mix, r, g, bh, bl, ff, ww, bins, leo, mg, part, a1, a2, s1,
    send_a, recv_a, send_b, recv_b, send_c, recv_c, ss0, rs0, ss1, rs1, ss2, rs2, sb, rb, sm, rm, local,
):
    px, pz, h, yy, xx = where_am_i()
    i = pz % 16
    other = 1 - h

    def mate(k):
        return ((yy + k // 4) % 4) * 4 + (xx + k % 4) % 4

    def twin(k):
        return (px + k % 8) % 8, ((h + k // 8) % 2) * 16 + i

    def send(src, dst, sems, recvs, where):
        return pltpu.make_async_remote_copy(
            src_ref=src, dst_ref=dst, send_sem=sems, recv_sem=recvs, device_id=where, device_id_type=MESH
        )

    barrier = pltpu.get_barrier_semaphore()
    for k in range(1, 16):
        pl.semaphore_signal(barrier, inc=1, device_id=(px, h * 16 + mate(k)), device_id_type=MESH)
        pl.semaphore_signal(barrier, inc=1, device_id=twin(k), device_id_type=MESH)

    flat = rows.reshape(68 * 24, 128)
    lane = lax.broadcasted_iota(jnp.int32, (64, 128), 1)
    even = lane % 2 == 0

    def plane(y, _):
        for f in range(3):
            v = vel_ref[f, y]
            mix[f, pl.ds(0, 64, stride=2), :] = v
            mix[f, pl.ds(1, 64, stride=2), :] = v
            t = mix[f].T
            flat[pl.ds(48 + f * 8 + y, 64, stride=24), :] = jnp.where(even, t[:64], t[64:])
        return 0

    lax.fori_loop(0, 8, plane, 0)
    first, last = flat[48:96, :], flat[64 * 24 : 66 * 24, :]
    edge[0] = pltpu.roll(last, 127, 1)
    edge[1] = pltpu.roll(first, 1, 1)
    pl.semaphore_wait(barrier, 30)

    own_planes = pl.ds(pl.multiple_of(pz * 8, 8), 8)
    their_planes = pl.ds(pl.multiple_of((other * 16 + i) * 8, 8), 8)

    def across(n):
        piece = (
            (pl.ds(2, 64), 0),
            (pl.ds(2, 64), 1),
            (pl.ds(2, 40), 2),
            (pl.ds(42, 24), 2),
            (pl.ds(0, 2), slice(None)),
            (pl.ds(66, 2), slice(None)),
        )[n]
        return send(rows.at[piece], partner.at[piece], send_a.at[n], recv_a.at[n], (px, other * 16 + i))

    def sideways(n):
        return send(edge.at[n], near.at[n], ss0.at[n], rs0.at[n], ((px + (1, 7)[n]) % 8, pz))

    def own(k):
        return send(
            rows.at[pl.ds(mate(k) * 4, 8)], r.at[:, :, own_planes, :],
            send_b.at[k], recv_b.at[k], (px, h * 16 + mate(k)),
        )

    def theirs(f, k):
        return send(
            partner.at[pl.ds(mate(k) * 4, 8), f], r.at[:, f, their_planes, :],
            send_c.at[f, k], recv_c.at[f, k], (px, h * 16 + mate(k)),
        )

    def there(f):
        return pltpu.make_async_copy(partner.at[pl.ds(i * 4, 8), f], r.at[:, f, their_planes, :], local.at[1 + f])

    sideways(0).start()
    sideways(1).start()
    across(0).start()
    for k in ORDER:

        @pl.when(mate(k) % 15 != 0)
        def _(k=k):
            own(k).start()

    sideways(0).wait_recv()
    sideways(1).wait_recv()
    even = lax.broadcasted_iota(jnp.int32, (48, 128), 1) % 2 == 0
    flat[0:48, :] = jnp.where(even, near[0], pltpu.roll(last, 1, 1))
    flat[66 * 24 : 68 * 24, :] = jnp.where(even, pltpu.roll(first, 127, 1), near[1])

    r0 = pl.multiple_of(h * 128, 128)
    bins[0] = column(fb_ref[...])
    bins[1] = column(pb_ref[...])
    mine = bins[0, pl.ds(r0, 128), :]
    masked = jnp.where(jnp.concatenate([mine, mine], axis=1) == fb_ref[...], inv_ref[pl.ds(r0, 128), :], 0.0)
    w = masked / jnp.sum(masked, axis=1, keepdims=True) * 0.0625
    w_hi = w.astype(BF16)
    ww[0:128, :] = w_hi
    ww[128:256, :] = (w - w_hi.astype(F32)).astype(BF16)

    for n in (4, 5, 1, 2, 3):
        across(n).start()
    for k in ORDER:

        @pl.when(mate(k) % 15 == 0)
        def _(k=k):
            own(k).start()

    here = pltpu.make_async_copy(rows.at[pl.ds(i * 4, 8)], r.at[:, :, own_planes, :], local.at[0])
    here.start()

    def strip(c, slots):
        y0 = pl.multiple_of(c * 16, 16)
        before = pl.multiple_of(jnp.maximum(y0 - 8, 0), 8)
        after = pl.multiple_of(jnp.minimum(y0 + 16, 248), 8)
        first, last = c == 0, c == 15
        u = [[r[x, f, pl.ds(y0, 16), :] for x in range(8)] for f in range(3)]
        for gx in range(1, 7):
            up, down = [], []
            for f in range(3):
                prev = jnp.where(first, 0.0, r[gx, f, pl.ds(before, 8), :])
                succ = jnp.where(last, 0.0, r[gx, f, pl.ds(after, 8), :])
                down.append(jnp.concatenate([prev[7:], u[f][gx][:15]], axis=0))
                up.append(jnp.concatenate([u[f][gx][1:], succ[:1]], axis=0))
            out, mag = fields_of(u, gx, up, down)
            for k in range(21):
                if SLOT[k] in slots:
                    g[SLOT[k], gx - 1] = out[k]
            if 2 <= gx <= 5 and 20 in slots:
                keep(c, gx - 2, mag)
        for k in slots:
            gs = [g[k, t] for t in range(6)]
            pairs = [gs[t] + gs[t + 1] for t in range(5)]
            for x in range(4):
                total = pairs[x] + pairs[x + 1]
                box = (pltpu.roll(total, 2, 1) + pltpu.roll(total, 126, 1)) + (total + total)
                hi = box.astype(BF16)
                bh[k, pl.ds(y0, 16), pl.ds(x * 128, 128)] = hi
                bl[k, pl.ds(y0, 16), pl.ds(x * 128, 128)] = (box - hi.astype(F32)).astype(BF16)

    def keep(c, x, mag):
        block = jnp.where(c // 8 == h, 2 * c - 16 * h, 16)
        mg[block, x] = mag[:8]
        mg[block + 1, x] = mag[8:]

    def early(t, _):
        strip(9 * h + t, range(21))
        return 0

    def late_a(t, _):
        strip(7 * other + t, range(EARLY))
        return 0

    def late_b(t, _):
        strip(7 * other + t, range(EARLY, 21))
        return 0

    def products(half, slots):
        for k in slots:
            hi = bh[k, :, pl.ds(half * 256, 256)]
            lo = bl[k, :, pl.ds(half * 256, 256)]
            both = jnp.dot(ww[...], hi, preferred_element_type=F32)
            rest = jnp.dot(ww[0:128, :], lo, preferred_element_type=F32)
            ff[half, k] = both[:128] + (both[128:] + rest)

    def lengths(k):
        return send(mg.at[mate(k)], om_ref.at[i], sm.at[k], rm.at[k], (px, h * 16 + mate(k)))

    across(0).wait_recv()
    across(4).wait_recv()
    across(5).wait_recv()
    for k in ORDER:
        theirs(0, k).start()
    there(0).start()
    here.wait()
    for k in range(1, 16):
        own(k).wait_recv()
    lax.fori_loop(0, 7, early, 0)
    across(1).wait_recv()
    for k in ORDER:
        theirs(1, k).start()
    there(1).start()
    for k in ORDER:

        @pl.when(mate(k) // 2 != 7 * other)
        def _(k=k):
            lengths(k).start()

    across(2).wait_recv()
    for k in ORDER:

        @pl.when(mate(k) <= 8)
        def _(k=k):
            theirs(2, k).start()

    across(3).wait_recv()
    for k in ORDER:

        @pl.when(mate(k) > 8)
        def _(k=k):
            theirs(2, k).start()

    there(2).start()
    for f in range(2):
        there(f).wait()
        for k in range(1, 16):
            theirs(f, k).wait_recv()
    lax.fori_loop(0, 9, late_a, 0)
    products(0, range(EARLY))
    products(1, range(EARLY))
    there(2).wait()
    for k in range(1, 16):
        theirs(2, k).wait_recv()
    lax.fori_loop(0, 9, late_b, 0)

    lanes = lax.broadcasted_iota(jnp.int32, (8, 128), 1)

    def contracts(x0, sums):
        def contract(c, sums):
            y0 = pl.multiple_of(c * 8, 8)
            lm_sum, mm_sum = 0.0, 0.0
            for x in range(2):
                f = [ff[x0 // 2, SLOT[k], pl.ds(y0, 8), pl.ds(x * 128, 128)] for k in range(21)]
                a, b, d = f[0], f[1], f[2]
                t, p, m = f[3:9], f[9:15], f[15:21]
                uu = [a * a, b * b, d * d, a * b, a * d, b * d]
                fmag = 4.0 * twice_norm(t)
                lm, mm = [], []
                for k in range(6):
                    stress = p[k] - uu[k]
                    leo[c, x0 + x, k] = stress
                    mod = m[k] - fmag * t[k]
                    lm.append(stress * mod)
                    mm.append(mod * mod)
                lm_sum += lm[0] + lm[1] + lm[2] + lm[3] + lm[4] + lm[5]
                mm_sum += 2.0 * (mm[0] + mm[1] + mm[2]) + (mm[3] + mm[4] + mm[5])
            hot = bins[1, pl.ds(pl.multiple_of(r0 + y0, 8), 8), :] == lanes
            num = sums[0] + jnp.where(hot, jnp.sum(lm_sum, axis=1, keepdims=True), 0.0)
            den = sums[1] + jnp.where(hot, jnp.sum(mm_sum, axis=1, keepdims=True), 0.0)
            return num, den

        return lax.fori_loop(0, 16, contract, sums)

    def big(half, k):
        return send(
            leo.at[mate(k), pl.ds(half * 2, 2)], o_ref.at[i, pl.ds(half * 2, 2)],
            sb.at[half, k], rb.at[half, k], (px, h * 16 + mate(k)),
        )

    def small(k):
        return send(part, a1.at[h * 8 + px], ss1.at[k], rs1.at[k], twin(k))

    def second(k):
        return send(s1, a2.at[i], ss2.at[k], rs2.at[k], (px, h * 16 + mate(k)))

    zero = jnp.zeros((8, 128), F32)
    products(0, range(EARLY, 21))
    sums = contracts(0, (zero, zero))
    products(1, range(EARLY, EARLY + 4))
    for k in ORDER:

        @pl.when(mate(k) // 2 == 7 * other)
        def _(k=k):
            lengths(k).start()

    for k in ORDER:
        big(0, k).start()
    products(1, range(EARLY + 4, 21))
    num, den = contracts(2, sums)
    row = lax.broadcasted_iota(jnp.int32, (8, 128), 0)
    num = jnp.sum(num, axis=0, keepdims=True) * 0.25
    den = jnp.sum(den, axis=0, keepdims=True) * 0.03125
    mine = jnp.where(row == 0, num, jnp.where(row == 1, den, 0.0))
    part[...] = mine
    a1[h * 8 + px] = mine
    for n in range(6):
        across(n).wait_send()
    for n in range(2):
        sideways(n).wait_send()
    for k in range(1, 16):
        own(k).wait_send()
        for f in range(3):
            theirs(f, k).wait_send()
    for k in range(1, 16):
        small(k).start()
    for k in ORDER[:6]:
        big(1, k).start()
    keep_here = pltpu.make_async_copy(leo.at[i], o_ref.at[i], local.at[0])
    keep_here.start()
    keep_length = pltpu.make_async_copy(mg.at[i], om_ref.at[i], local.at[1])
    keep_length.start()
    for k in range(1, 16):
        small(k).wait_recv()
    total = a1[0]
    for q in range(1, 16):
        total = total + a1[q]
    s1[...] = total
    a2[i] = total
    for k in range(1, 16):
        small(k).wait_send()
    for k in range(1, 16):
        second(k).start()
    for k in ORDER[6:]:
        big(1, k).start()
    for k in range(1, 16):
        second(k).wait_recv()
    total = a2[0]
    for q in range(1, 16):
        total = total + a2[q]
    tot_ref[...] = total
    keep_here.wait()
    keep_length.wait()
    for k in range(1, 16):
        second(k).wait_send()
        lengths(k).wait()
    for half in range(2):
        for k in range(1, 16):
            big(half, k).wait()


def to_planes(tot_ref, pb_ref, o_ref, om_ref, leo_ref, visc_ref, coef_ref, mix):
    pz = lax.axis_index("pz")
    per_bin = tot_ref[0:1, :] / jnp.maximum(tot_ref[1:2, :], 65536.0)
    per_bin = jnp.broadcast_to(per_bin, (128, 128)).T
    hot = lax.broadcasted_iota(jnp.int32, (128, 256), 0) == pb_ref[...]
    both = jnp.concatenate([per_bin, per_bin], axis=1)
    coef = jnp.sum(jnp.where(hot, both, 0.0), axis=0, keepdims=True)
    coef_ref[...] = coef
    at = lax.broadcasted_iota(jnp.int32, (1, 256), 1) - pz * 8
    low = lax.broadcasted_iota(jnp.int32, (64, 128), 1) < 64
    y0 = pl.program_id(0) * 4

    def plane(t, _):
        y = y0 + t
        mine = jnp.sum(jnp.where(at == y, coef, 0.0), axis=1, keepdims=True)
        for f in range(7):
            if f < 6:
                m = o_ref[pl.ds(f * 8 + y, 64, stride=48), :]
            else:
                m = om_ref[pl.ds(y, 64, stride=8), :]
            mix[f] = jnp.concatenate([m, m], axis=0).T
            v = jnp.where(low, mix[f, pl.ds(0, 64, stride=2), :], mix[f, pl.ds(1, 64, stride=2), :])
            if f < 6:
                leo_ref[f, t] = v
            else:
                visc_ref[t] = mine * 0.5 * v
        return 0

    lax.fori_loop(0, 4, plane, 0)


def spec(space):
    return pl.BlockSpec(memory_space=space)


def params(**kw):
    return pltpu.CompilerParams(vmem_limit_bytes=56 * 1024 * 1024, **kw)


DMA = pltpu.SemaphoreType.DMA


def local_step(velocity, filter_inverse, filter_block, plane_bin):
    bins = plane_bin.reshape(1, 256)
    part = VMEM((68, 3, 8, 128), F32)
    back, lengths, total = pl.pallas_call(
        core,
        out_shape=(
            jax.ShapeDtypeStruct((16, 4, 6, 8, 128), F32),
            jax.ShapeDtypeStruct((16, 4, 8, 128), F32),
            jax.ShapeDtypeStruct((8, 128), F32),
        ),
        in_specs=[spec(VMEM)] * 4,
        out_specs=(spec(pl.ANY), spec(pl.ANY), spec(VMEM)),
        scratch_shapes=[
            part,
            part,
            VMEM((2, 48, 128), F32),
            VMEM((2, 48, 128), F32),
            VMEM((3, 128, 128), F32),
            VMEM((8, 3, 256, 128), F32),
            VMEM((21, 6, 16, 128), F32),
            VMEM((21, 256, 512), BF16),
            VMEM((21, 256, 512), BF16),
            VMEM((2, 21, 128, 256), F32),
            VMEM((256, 256), BF16),
            VMEM((2, 256, 128), jnp.int32),
            VMEM((16, 4, 6, 8, 128), F32),
            VMEM((18, 4, 8, 128), F32),
            VMEM((8, 128), F32),
            VMEM((16, 8, 128), F32),
            VMEM((16, 8, 128), F32),
            VMEM((8, 128), F32),
            DMA((6,)),
            DMA((6,)),
            DMA((16,)),
            DMA((16,)),
            DMA((3, 16)),
            DMA((3, 16)),
            DMA((2,)),
            DMA((2,)),
            DMA((16,)),
            DMA((16,)),
            DMA((16,)),
            DMA((16,)),
            DMA((2, 16)),
            DMA((2, 16)),
            DMA((16,)),
            DMA((16,)),
            DMA((4,)),
        ],
        compiler_params=params(collective_id=0, has_side_effects=True),
        name="core",
    )(
        velocity,
        filter_inverse,
        filter_block.reshape(1, 256),
        bins,
    )
    leonard, viscosity, coefficient = pl.pallas_call(
        to_planes,
        out_shape=(
            jax.ShapeDtypeStruct((6, 8, 64, 128), F32),
            jax.ShapeDtypeStruct((8, 64, 128), F32),
            jax.ShapeDtypeStruct((1, 256), F32),
        ),
        grid=(2,),
        in_specs=[
            pl.BlockSpec((8, 128), lambda q: (0, 0)),
            pl.BlockSpec((1, 256), lambda q: (0, 0)),
            pl.BlockSpec((64 * 48, 128), lambda q: (0, 0)),
            pl.BlockSpec((64 * 8, 128), lambda q: (0, 0)),
        ],
        out_specs=(
            pl.BlockSpec((6, 4, 64, 128), lambda q: (0, q, 0, 0)),
            pl.BlockSpec((4, 64, 128), lambda q: (q, 0, 0)),
            pl.BlockSpec((1, 256), lambda q: (0, 0)),
        ),
        scratch_shapes=[VMEM((7, 128, 128), F32)],
        compiler_params=params(),
        name="to_planes",
    )(total, bins, back.reshape(64 * 48, 128), lengths.reshape(64 * 8, 128))
    return leonard, viscosity, coefficient.reshape(256)


def solution(mesh):
    return jax.shard_map(
        local_step,
        mesh=mesh,
        in_specs=(P(None, "pz", None, "px"), P(), P(), P()),
        out_specs=(P(None, "pz", None, "px"), P("pz", None, "px"), P()),
        check_vma=False,
    )
```

```python
import functools

import jax
import jax.numpy as jnp
from jax import lax
from jax.experimental import pallas as pl
from jax.experimental.pallas import tpu as pltpu
from jax.sharding import PartitionSpec as P

NBIN = 64
MESH = pl.DeviceIdType.MESH
F32 = jnp.float32
BF16 = jnp.bfloat16
VMEM = pltpu.VMEM
ORDER = (10, 6, 14, 8, 9, 11, 2, 5, 15, 13, 7, 1, 3, 4, 12)


WINDOWS = (12, 13, 10, 11, 14, 15, 4, 5, 2, 3, 6, 7, 8, 9, 0, 1)


def where_am_i():
    px, pz = lax.axis_index("px"), lax.axis_index("pz")
    return px, pz, pz // 16, (pz % 16) // 4, pz % 4


SLOT = (0, 1, 8, 2, 3, 9, 4, 10, 11, 5, 6, 12, 7, 13, 14, 15, 16, 17, 18, 19, 20)
EARLY = 8


def fields_of(u, gx, up, down):
    def d_x(f):
        return u[f][gx + 1] - u[f][gx - 1]

    def d_z(f):
        return pltpu.roll(u[f][gx], 126, 1) - pltpu.roll(u[f][gx], 2, 1)

    def d_y(f):
        return up[f] - down[f]

    t = [d_x(0), d_y(1), d_z(2), d_y(0) + d_x(1), d_z(0) + d_x(2), d_z(1) + d_y(2)]
    mag = twice_norm(t)
    a, b, c = u[0][gx], u[1][gx], u[2][gx]
    return [a, b, c] + t + [a * a, b * b, c * c, a * b, a * c, b * c] + [mag * q for q in t], mag


def twice_norm(t):
    return jnp.sqrt(
        2.0 * (t[0] * t[0] + t[1] * t[1] + t[2] * t[2]) + (t[3] * t[3] + t[4] * t[4] + t[5] * t[5])
    )


def column(row):
    return jnp.broadcast_to(row, (128, 256)).T


def core(
    vel_ref, inv_ref, fb_ref, pb_ref, o_ref, om_ref, tot_ref,
    rows, partner, edge, near, mix, r, g, bh, bl, ff, ww, bins, leo, mg, part, a1, a2, s1,
    send_a, recv_a, send_b, recv_b, send_c, recv_c, ss0, rs0, sw, rw, ss1, rs1, ss2, rs2, sb, rb, sm, rm, local,
):
    px, pz, h, yy, xx = where_am_i()
    i = pz % 16
    other = 1 - h

    def mate(k):
        return ((yy + k // 4) % 4) * 4 + (xx + k % 4) % 4

    def twin(k):
        return (px + k % 8) % 8, ((h + k // 8) % 2) * 16 + i

    def send(src, dst, sems, recvs, where):
        return pltpu.make_async_remote_copy(
            src_ref=src, dst_ref=dst, send_sem=sems, recv_sem=recvs, device_id=where, device_id_type=MESH
        )

    core_of = px % 2
    base = px - core_of
    mixed = xx % 2 != core_of
    slot = 2 * (2 * yy + xx // 2) + core_of

    def window(k):
        y2, x2 = (yy + (k // 2) % 4) % 4, (xx // 2 + k // 8) % 2
        t = 2 * (2 * y2 + x2) + k % 2
        return t, (base + k % 2, h * 16 + y2 * 4 + 2 * x2 + core_of)

    def start_of(t):
        return 8 * (t // 2) + 6 * (t % 2)

    def leaves(k):
        return jnp.logical_or(mixed, core_of != k)

    def each(ks, act, also=None):
        for k in ks:
            keep = None if k > 1 else leaves(k)
            if also is not None:
                keep = also(k) if keep is None else jnp.logical_and(keep, also(k))
            if keep is None:
                act(k)
            else:
                pl.when(keep)(functools.partial(act, k))

    def from_all(act):
        for q in range(16):
            pl.when(jnp.logical_or(mixed, i != q))(functools.partial(act, q))

    barrier = pltpu.get_barrier_semaphore()
    for k in range(16):
        for c in range(2):
            if k or c:
                place = (base + (core_of + c) % 2, h * 16 + mate(k))
                pl.semaphore_signal(barrier, inc=1, device_id=place, device_id_type=MESH)
    for k in range(1, 16):
        pl.semaphore_signal(barrier, inc=1, device_id=twin(k), device_id_type=MESH)

    flat = rows.reshape(68 * 24, 128)
    lane = lax.broadcasted_iota(jnp.int32, (64, 128), 1)
    even = lane % 2 == 0

    def plane(y, _):
        for f in range(3):
            v = vel_ref[f, y]
            mix[f, pl.ds(0, 64, stride=2), :] = v
            mix[f, pl.ds(1, 64, stride=2), :] = v
            t = mix[f].T
            flat[pl.ds(48 + f * 8 + y, 64, stride=24), :] = jnp.where(even, t[:64], t[64:])
        return 0

    lax.fori_loop(0, 8, plane, 0)
    first, last = flat[48:96, :], flat[64 * 24 : 66 * 24, :]
    edge[0] = pltpu.roll(last, 127, 1)
    edge[1] = pltpu.roll(first, 1, 1)
    pl.semaphore_wait(barrier, 46)

    own_planes = pl.ds(pl.multiple_of(pz * 8, 8), 8)
    their_planes = pl.ds(pl.multiple_of((other * 16 + i) * 8, 8), 8)

    def across(n):
        piece = (
            (pl.ds(2, 64), 0),
            (pl.ds(2, 64), 1),
            (pl.ds(2, 40), 2),
            (pl.ds(42, 24), 2),
            (pl.ds(0, 2), slice(None)),
            (pl.ds(66, 2), slice(None)),
        )[n]
        return send(rows.at[piece], partner.at[piece], send_a.at[n], recv_a.at[n], (px, other * 16 + i))

    def sideways(n):
        return send(edge.at[n], near.at[n], ss0.at[n], rs0.at[n], ((px + (1, 7)[n]) % 8, pz))

    def own(k, q=0):
        t, place = window(k)
        return send(
            rows.at[pl.ds(start_of(t), 6)], r.at[pl.ds(2 * (k % 2), 6), :, own_planes, :],
            send_b.at[k], recv_b.at[q], place,
        )

    def theirs(f, k, q=0):
        t, place = window(k)
        return send(
            partner.at[pl.ds(start_of(t), 6), f], r.at[pl.ds(2 * (k % 2), 6), f, their_planes, :],
            send_c.at[f, k], recv_c.at[f, q], place,
        )

    def here():
        return pltpu.make_async_copy(
            rows.at[pl.ds(start_of(slot), 6)], r.at[pl.ds(2 * core_of, 6), :, own_planes, :], local.at[0]
        )

    def there(f):
        return pltpu.make_async_copy(
            partner.at[pl.ds(start_of(slot), 6), f],
            r.at[pl.ds(2 * core_of, 6), f, their_planes, :],
            local.at[1 + f],
        )

    def swap(n):
        half = h if n == 0 else other
        which = (slice(None) if n == 0 else n - 1, pl.ds(pl.multiple_of(half * 128, 128), 128), slice(None))
        return send(
            r.at[(pl.ds(4 - 2 * core_of, 2), *which)], r.at[(pl.ds(6 * core_of, 2), *which)],
            sw.at[n], rw.at[n], (base + 1 - core_of, pz),
        )

    def alone(act):
        pl.when(jnp.logical_not(mixed))(act)

    sideways(0).start()
    sideways(1).start()
    across(0).start()
    each(WINDOWS, lambda k: own(k, i).start(), lambda k: window(k)[0] % 15 != 0)
    sideways(0).wait_recv()
    sideways(1).wait_recv()
    even = lax.broadcasted_iota(jnp.int32, (48, 128), 1) % 2 == 0
    flat[0:48, :] = jnp.where(even, near[0], pltpu.roll(last, 1, 1))
    flat[66 * 24 : 68 * 24, :] = jnp.where(even, pltpu.roll(first, 127, 1), near[1])

    r0 = pl.multiple_of(h * 128, 128)
    bins[0] = column(fb_ref[...])
    bins[1] = column(pb_ref[...])
    mine = bins[0, pl.ds(r0, 128), :]
    masked = jnp.where(jnp.concatenate([mine, mine], axis=1) == fb_ref[...], inv_ref[pl.ds(r0, 128), :], 0.0)
    w = masked / jnp.sum(masked, axis=1, keepdims=True) * 0.0625
    w_hi = w.astype(BF16)
    ww[0:128, :] = w_hi
    ww[128:256, :] = (w - w_hi.astype(F32)).astype(BF16)

    for n in (4, 5, 1, 2, 3):
        across(n).start()
    each(WINDOWS, lambda k: own(k, i).start(), lambda k: window(k)[0] % 15 == 0)
    alone(lambda: here().start())

    def strip(c, slots):
        y0 = pl.multiple_of(c * 16, 16)
        before = pl.multiple_of(jnp.maximum(y0 - 8, 0), 8)
        after = pl.multiple_of(jnp.minimum(y0 + 16, 248), 8)
        first, last = c == 0, c == 15
        u = [[r[x, f, pl.ds(y0, 16), :] for x in range(8)] for f in range(3)]
        for gx in range(1, 7):
            up, down = [], []
            for f in range(3):
                prev = jnp.where(first, 0.0, r[gx, f, pl.ds(before, 8), :])
                succ = jnp.where(last, 0.0, r[gx, f, pl.ds(after, 8), :])
                down.append(jnp.concatenate([prev[7:], u[f][gx][:15]], axis=0))
                up.append(jnp.concatenate([u[f][gx][1:], succ[:1]], axis=0))
            out, mag = fields_of(u, gx, up, down)
            for k in range(21):
                if SLOT[k] in slots:
                    g[SLOT[k], gx - 1] = out[k]
            if 2 <= gx <= 5 and 20 in slots:
                keep(c, gx - 2, mag)
        for k in slots:
            gs = [g[k, t] for t in range(6)]
            pairs = [gs[t] + gs[t + 1] for t in range(5)]
            for x in range(4):
                total = pairs[x] + pairs[x + 1]
                box = (pltpu.roll(total, 2, 1) + pltpu.roll(total, 126, 1)) + (total + total)
                hi = box.astype(BF16)
                bh[k, pl.ds(y0, 16), pl.ds(x * 128, 128)] = hi
                bl[k, pl.ds(y0, 16), pl.ds(x * 128, 128)] = (box - hi.astype(F32)).astype(BF16)

    def keep(c, x, mag):
        block = jnp.where(c // 8 == h, 2 * c - 16 * h, 16)
        mg[block, x] = mag[:8]
        mg[block + 1, x] = mag[8:]

    def early(t, _):
        strip(9 * h + t, range(21))
        return 0

    def late_a(t, _):
        strip(7 * other + t, range(EARLY))
        return 0

    def late_b(t, _):
        strip(7 * other + t, range(EARLY, 21))
        return 0

    def products(half, slots):
        for k in slots:
            hi = bh[k, :, pl.ds(half * 256, 256)]
            lo = bl[k, :, pl.ds(half * 256, 256)]
            both = jnp.dot(ww[...], hi, preferred_element_type=F32)
            rest = jnp.dot(ww[0:128, :], lo, preferred_element_type=F32)
            ff[half, k] = both[:128] + (both[128:] + rest)

    def owner(k):
        return (base + xx % 2, h * 16 + mate(k))

    def goes(k):
        return True if k else mixed

    def lengths(k, t=0):
        return send(mg.at[mate(k)], om_ref.at[slot], sm.at[k], rm.at[t], owner(k))

    across(0).wait_recv()
    across(4).wait_recv()
    across(5).wait_recv()
    each(WINDOWS, lambda k: theirs(0, k, i).start())
    alone(lambda: there(0).start())
    alone(lambda: here().wait())
    from_all(lambda q: own(0, q).wait_recv())
    swap(0).start()
    swap(0).wait_recv()
    lax.fori_loop(0, 7, early, 0)
    across(1).wait_recv()
    each(WINDOWS, lambda k: theirs(1, k, i).start())
    alone(lambda: there(1).start())
    for k in ORDER + (0,):
        pl.when(jnp.logical_and(goes(k), mate(k) // 2 != 7 * other))(lambda k=k: lengths(k, slot).start())

    across(2).wait_recv()
    each(WINDOWS, lambda k: theirs(2, k, i).start(), lambda k: window(k)[0] <= 8)
    across(3).wait_recv()
    each(WINDOWS, lambda k: theirs(2, k, i).start(), lambda k: window(k)[0] > 8)
    alone(lambda: there(2).start())
    for f in range(2):
        alone(lambda f=f: there(f).wait())
        from_all(lambda q, f=f: theirs(f, 0, q).wait_recv())
        swap(1 + f).start()
    swap(1).wait_recv()
    swap(2).wait_recv()
    lax.fori_loop(0, 9, late_a, 0)
    products(0, range(EARLY))
    products(1, range(EARLY))
    alone(lambda: there(2).wait())
    from_all(lambda q: theirs(2, 0, q).wait_recv())
    swap(3).start()
    swap(3).wait_recv()
    lax.fori_loop(0, 9, late_b, 0)

    lanes = lax.broadcasted_iota(jnp.int32, (8, 128), 1)

    def contracts(x0, sums):
        def contract(c, sums):
            y0 = pl.multiple_of(c * 8, 8)
            lm_sum, mm_sum = 0.0, 0.0
            for x in range(2):
                f = [ff[x0 // 2, SLOT[k], pl.ds(y0, 8), pl.ds(x * 128, 128)] for k in range(21)]
                a, b, d = f[0], f[1], f[2]
                t, p, m = f[3:9], f[9:15], f[15:21]
                uu = [a * a, b * b, d * d, a * b, a * d, b * d]
                fmag = 4.0 * twice_norm(t)
                lm, mm = [], []
                for k in range(6):
                    stress = p[k] - uu[k]
                    leo[c, x0 + x, k] = stress
                    mod = m[k] - fmag * t[k]
                    lm.append(stress * mod)
                    mm.append(mod * mod)
                lm_sum += lm[0] + lm[1] + lm[2] + lm[3] + lm[4] + lm[5]
                mm_sum += 2.0 * (mm[0] + mm[1] + mm[2]) + (mm[3] + mm[4] + mm[5])
            hot = bins[1, pl.ds(pl.multiple_of(r0 + y0, 8), 8), :] == lanes
            num = sums[0] + jnp.where(hot, jnp.sum(lm_sum, axis=1, keepdims=True), 0.0)
            den = sums[1] + jnp.where(hot, jnp.sum(mm_sum, axis=1, keepdims=True), 0.0)
            return num, den

        return lax.fori_loop(0, 16, contract, sums)

    def big(half, k, t=0):
        return send(
            leo.at[mate(k), pl.ds(half * 2, 2)], o_ref.at[slot, pl.ds(half * 2, 2)],
            sb.at[half, k], rb.at[half, t], owner(k),
        )

    def small(k):
        return send(part, a1.at[h * 8 + px], ss1.at[k], rs1.at[k], twin(k))

    def second(k):
        return send(s1, a2.at[i], ss2.at[k], rs2.at[k], (px, h * 16 + mate(k)))

    zero = jnp.zeros((8, 128), F32)
    products(0, range(EARLY, 21))
    sums = contracts(0, (zero, zero))
    products(1, range(EARLY, EARLY + 4))
    for k in ORDER + (0,):
        pl.when(jnp.logical_and(goes(k), mate(k) // 2 == 7 * other))(lambda k=k: lengths(k, slot).start())
    for k in ORDER:
        big(0, k, slot).start()
    pl.when(mixed)(lambda: big(0, 0, slot).start())
    products(1, range(EARLY + 4, 21))
    num, den = contracts(2, sums)
    row = lax.broadcasted_iota(jnp.int32, (8, 128), 0)
    num = jnp.sum(num, axis=0, keepdims=True) * 0.25
    den = jnp.sum(den, axis=0, keepdims=True) * 0.03125
    mine = jnp.where(row == 0, num, jnp.where(row == 1, den, 0.0))
    part[...] = mine
    a1[h * 8 + px] = mine
    for n in range(6):
        across(n).wait_send()
    for n in range(2):
        sideways(n).wait_send()
    for n in range(4):
        swap(n).wait_send()
    each(range(16), lambda k: own(k).wait_send())
    for f in range(3):
        each(range(16), lambda k, f=f: theirs(f, k).wait_send())
    for k in range(1, 16):
        small(k).start()
    for k in ORDER[:6]:
        big(1, k, slot).start()
    keep_here = pltpu.make_async_copy(leo.at[i], o_ref.at[slot], local.at[0])
    alone(keep_here.start)
    keep_length = pltpu.make_async_copy(mg.at[i], om_ref.at[slot], local.at[1])
    alone(keep_length.start)
    for k in range(1, 16):
        small(k).wait_recv()
    total = a1[0]
    for q in range(1, 16):
        total = total + a1[q]
    s1[...] = total
    a2[i] = total
    for k in range(1, 16):
        small(k).wait_send()
    for k in range(1, 16):
        second(k).start()
    for k in ORDER[6:]:
        big(1, k, slot).start()
    pl.when(mixed)(lambda: big(1, 0, slot).start())
    for k in range(1, 16):
        second(k).wait_recv()
    total = a2[0]
    for q in range(1, 16):
        total = total + a2[q]
    tot_ref[...] = total
    alone(keep_here.wait)
    alone(keep_length.wait)
    for k in range(1, 16):
        second(k).wait_send()
        lengths(k).wait_send()
        for half in range(2):
            big(half, k).wait_send()
    pl.when(mixed)(lambda: lengths(0).wait_send())
    for half in range(2):
        pl.when(mixed)(lambda half=half: big(half, 0).wait_send())

    def arrive(t):
        lengths(0, t).wait_recv()
        for half in range(2):
            big(half, 0, t).wait_recv()

    for t in range(16):
        pl.when(jnp.logical_or(mixed, slot != t))(functools.partial(arrive, t))


def to_planes(tot_ref, pb_ref, o_ref, om_ref, leo_ref, visc_ref, coef_ref, mix):
    pz = lax.axis_index("pz")
    per_bin = tot_ref[0:1, :] / jnp.maximum(tot_ref[1:2, :], 65536.0)
    per_bin = jnp.broadcast_to(per_bin, (128, 128)).T
    hot = lax.broadcasted_iota(jnp.int32, (128, 256), 0) == pb_ref[...]
    both = jnp.concatenate([per_bin, per_bin], axis=1)
    coef = jnp.sum(jnp.where(hot, both, 0.0), axis=0, keepdims=True)
    coef_ref[...] = coef
    at = lax.broadcasted_iota(jnp.int32, (1, 256), 1) - pz * 8
    low = lax.broadcasted_iota(jnp.int32, (64, 128), 1) < 64
    y0 = pl.program_id(0) * 4

    def plane(t, _):
        y = y0 + t
        mine = jnp.sum(jnp.where(at == y, coef, 0.0), axis=1, keepdims=True)
        for f in range(7):
            if f < 6:
                m = o_ref[pl.ds(f * 8 + y, 64, stride=48), :]
            else:
                m = om_ref[pl.ds(y, 64, stride=8), :]
            mix[f] = jnp.concatenate([m, m], axis=0).T
            v = jnp.where(low, mix[f, pl.ds(0, 64, stride=2), :], mix[f, pl.ds(1, 64, stride=2), :])
            if f < 6:
                leo_ref[f, t] = v
            else:
                visc_ref[t] = mine * 0.5 * v
        return 0

    lax.fori_loop(0, 4, plane, 0)


def spec(space):
    return pl.BlockSpec(memory_space=space)


def params(**kw):
    return pltpu.CompilerParams(vmem_limit_bytes=56 * 1024 * 1024, **kw)


DMA = pltpu.SemaphoreType.DMA


def local_step(velocity, filter_inverse, filter_block, plane_bin):
    bins = plane_bin.reshape(1, 256)
    part = VMEM((68, 3, 8, 128), F32)
    back, lengths, total = pl.pallas_call(
        core,
        out_shape=(
            jax.ShapeDtypeStruct((16, 4, 6, 8, 128), F32),
            jax.ShapeDtypeStruct((16, 4, 8, 128), F32),
            jax.ShapeDtypeStruct((8, 128), F32),
        ),
        in_specs=[spec(VMEM)] * 4,
        out_specs=(spec(pl.ANY), spec(pl.ANY), spec(VMEM)),
        scratch_shapes=[
            part,
            part,
            VMEM((2, 48, 128), F32),
            VMEM((2, 48, 128), F32),
            VMEM((3, 128, 128), F32),
            VMEM((8, 3, 256, 128), F32),
            VMEM((21, 6, 16, 128), F32),
            VMEM((21, 256, 512), BF16),
            VMEM((21, 256, 512), BF16),
            VMEM((2, 21, 128, 256), F32),
            VMEM((256, 256), BF16),
            VMEM((2, 256, 128), jnp.int32),
            VMEM((16, 4, 6, 8, 128), F32),
            VMEM((18, 4, 8, 128), F32),
            VMEM((8, 128), F32),
            VMEM((16, 8, 128), F32),
            VMEM((16, 8, 128), F32),
            VMEM((8, 128), F32),
            DMA((6,)),
            DMA((6,)),
            DMA((16,)),
            DMA((16,)),
            DMA((3, 16)),
            DMA((3, 16)),
            DMA((2,)),
            DMA((2,)),
            DMA((4,)),
            DMA((4,)),
            DMA((16,)),
            DMA((16,)),
            DMA((16,)),
            DMA((16,)),
            DMA((2, 16)),
            DMA((2, 16)),
            DMA((16,)),
            DMA((16,)),
            DMA((4,)),
        ],
        compiler_params=params(collective_id=0, has_side_effects=True),
        name="core",
    )(
        velocity,
        filter_inverse,
        filter_block.reshape(1, 256),
        bins,
    )
    leonard, viscosity, coefficient = pl.pallas_call(
        to_planes,
        out_shape=(
            jax.ShapeDtypeStruct((6, 8, 64, 128), F32),
            jax.ShapeDtypeStruct((8, 64, 128), F32),
            jax.ShapeDtypeStruct((1, 256), F32),
        ),
        grid=(2,),
        in_specs=[
            pl.BlockSpec((8, 128), lambda q: (0, 0)),
            pl.BlockSpec((1, 256), lambda q: (0, 0)),
            pl.BlockSpec((64 * 48, 128), lambda q: (0, 0)),
            pl.BlockSpec((64 * 8, 128), lambda q: (0, 0)),
        ],
        out_specs=(
            pl.BlockSpec((6, 4, 64, 128), lambda q: (0, q, 0, 0)),
            pl.BlockSpec((4, 64, 128), lambda q: (q, 0, 0)),
            pl.BlockSpec((1, 256), lambda q: (0, 0)),
        ),
        scratch_shapes=[VMEM((7, 128, 128), F32)],
        compiler_params=params(),
        name="to_planes",
    )(total, bins, back.reshape(64 * 48, 128), lengths.reshape(64 * 8, 128))
    return leonard, viscosity, coefficient.reshape(256)


def solution(mesh):
    return jax.shard_map(
        local_step,
        mesh=mesh,
        in_specs=(P(None, "pz", None, "px"), P(), P(), P()),
        out_specs=(P(None, "pz", None, "px"), P("pz", None, "px"), P()),
        check_vma=False,
    )
```

```python
import functools

import jax
import jax.numpy as jnp
from jax import lax
from jax.experimental import pallas as pl
from jax.experimental.pallas import tpu as pltpu
from jax.sharding import PartitionSpec as P

NBIN = 64
MESH = pl.DeviceIdType.MESH
F32 = jnp.float32
BF16 = jnp.bfloat16
VMEM = pltpu.VMEM
ORDER = (10, 6, 14, 8, 9, 11, 2, 5, 15, 13, 7, 1, 3, 4, 12)


WINDOWS = (12, 13, 10, 11, 14, 15, 4, 5, 2, 3, 6, 7, 8, 9, 0, 1)


def where_am_i():
    px, pz = lax.axis_index("px"), lax.axis_index("pz")
    return px, pz, pz // 16, (pz % 16) // 4, pz % 4


SLOT = (0, 1, 8, 2, 3, 9, 4, 10, 11, 5, 6, 12, 7, 13, 14, 15, 16, 17, 18, 19, 20)
EARLY = 8


def fields_of(u, gx, up, down):
    def d_x(f):
        return u[f][gx + 1] - u[f][gx - 1]

    def d_z(f):
        return pltpu.roll(u[f][gx], 126, 1) - pltpu.roll(u[f][gx], 2, 1)

    def d_y(f):
        return up[f] - down[f]

    t = [d_x(0), d_y(1), d_z(2), d_y(0) + d_x(1), d_z(0) + d_x(2), d_z(1) + d_y(2)]
    mag = twice_norm(t)
    a, b, c = u[0][gx], u[1][gx], u[2][gx]
    return [a, b, c] + t + [a * a, b * b, c * c, a * b, a * c, b * c] + [mag * q for q in t], mag


def twice_norm(t):
    return jnp.sqrt(
        2.0 * (t[0] * t[0] + t[1] * t[1] + t[2] * t[2]) + (t[3] * t[3] + t[4] * t[4] + t[5] * t[5])
    )


def column(row):
    return jnp.broadcast_to(row, (128, 256)).T


def core(
    vel_ref, inv_ref, fb_ref, pb_ref, o_ref, om_ref, tot_ref,
    rows, partner, edge, near, mix, r, g, bh, bl, ff, ww, bins, leo, mg, part, a1, a2, s1,
    send_a, recv_a, send_b, recv_b, send_c, recv_c, ss0, rs0, sw, rw, ss1, rs1, ss2, rs2, sb, rb, sm, rm, local,
):
    px, pz, h, yy, xx = where_am_i()
    i = pz % 16
    other = 1 - h

    def mate(k):
        return ((yy + k // 4) % 4) * 4 + (xx + k % 4) % 4

    def twin(k):
        return (px + k % 8) % 8, ((h + k // 8) % 2) * 16 + i

    def send(src, dst, sems, recvs, where):
        return pltpu.make_async_remote_copy(
            src_ref=src, dst_ref=dst, send_sem=sems, recv_sem=recvs, device_id=where, device_id_type=MESH
        )

    core_of = px % 2
    base = px - core_of
    mixed = xx % 2 != core_of
    slot = 2 * (2 * yy + xx // 2) + core_of

    def window(k):
        y2, x2 = (yy + (k // 2) % 4) % 4, (xx // 2 + k // 8) % 2
        t = 2 * (2 * y2 + x2) + k % 2
        return t, (base + k % 2, h * 16 + y2 * 4 + 2 * x2 + core_of)

    def start_of(t):
        return 8 * (t // 2) + 6 * (t % 2)

    def leaves(k):
        return jnp.logical_or(mixed, core_of != k)

    def each(ks, act, also=None):
        for k in ks:
            keep = None if k > 1 else leaves(k)
            if also is not None:
                keep = also(k) if keep is None else jnp.logical_and(keep, also(k))
            if keep is None:
                act(k)
            else:
                pl.when(keep)(functools.partial(act, k))

    def from_all(act):
        for q in range(16):
            pl.when(jnp.logical_or(mixed, i != q))(functools.partial(act, q))

    barrier = pltpu.get_barrier_semaphore()
    for k in range(16):
        for c in range(2):
            if k or c:
                place = (base + (core_of + c) % 2, h * 16 + mate(k))
                pl.semaphore_signal(barrier, inc=1, device_id=place, device_id_type=MESH)
    for k in range(1, 16):
        pl.semaphore_signal(barrier, inc=1, device_id=twin(k), device_id_type=MESH)

    flat = rows.reshape(68 * 24, 128)
    lane = lax.broadcasted_iota(jnp.int32, (64, 128), 1)
    even = lane % 2 == 0

    def plane(y, _):
        for f in range(3):
            v = vel_ref[f, y]
            mix[f, pl.ds(0, 64, stride=2), :] = v
            mix[f, pl.ds(1, 64, stride=2), :] = v
            t = mix[f].T
            flat[pl.ds(48 + f * 8 + y, 64, stride=24), :] = jnp.where(even, t[:64], t[64:])
        return 0

    lax.fori_loop(0, 8, plane, 0)
    first, last = flat[48:96, :], flat[64 * 24 : 66 * 24, :]
    edge[0] = pltpu.roll(last, 127, 1)
    edge[1] = pltpu.roll(first, 1, 1)
    pl.semaphore_wait(barrier, 46)

    own_planes = pl.ds(pl.multiple_of(pz * 8, 8), 8)
    their_planes = pl.ds(pl.multiple_of((other * 16 + i) * 8, 8), 8)

    def across(n):
        piece = (
            (pl.ds(2, 64), 0),
            (pl.ds(2, 64), 1),
            (pl.ds(2, 40), 2),
            (pl.ds(42, 24), 2),
            (pl.ds(0, 2), slice(None)),
            (pl.ds(66, 2), slice(None)),
        )[n]
        return send(rows.at[piece], partner.at[piece], send_a.at[n], recv_a.at[n], (px, other * 16 + i))

    def sideways(n):
        return send(edge.at[n], near.at[n], ss0.at[n], rs0.at[n], ((px + (1, 7)[n]) % 8, pz))

    def own(k, q=0):
        t, place = window(k)
        return send(
            rows.at[pl.ds(start_of(t), 6)], r.at[pl.ds(2 * (k % 2), 6), :, own_planes, :],
            send_b.at[k], recv_b.at[q], place,
        )

    def theirs(f, k, q=0):
        t, place = window(k)
        return send(
            partner.at[pl.ds(start_of(t), 6), f], r.at[pl.ds(2 * (k % 2), 6), f, their_planes, :],
            send_c.at[f, k], recv_c.at[f, q], place,
        )

    def here():
        return pltpu.make_async_copy(
            rows.at[pl.ds(start_of(slot), 6)], r.at[pl.ds(2 * core_of, 6), :, own_planes, :], local.at[0]
        )

    def there(f):
        return pltpu.make_async_copy(
            partner.at[pl.ds(start_of(slot), 6), f],
            r.at[pl.ds(2 * core_of, 6), f, their_planes, :],
            local.at[1 + f],
        )

    def swap(n):
        half = h if n == 0 else other
        which = (slice(None) if n == 0 else n - 1, pl.ds(pl.multiple_of(half * 128, 128), 128), slice(None))
        return send(
            r.at[(pl.ds(4 - 2 * core_of, 2), *which)], r.at[(pl.ds(6 * core_of, 2), *which)],
            sw.at[n], rw.at[n], (base + 1 - core_of, pz),
        )

    def alone(act):
        pl.when(jnp.logical_not(mixed))(act)

    sideways(0).start()
    sideways(1).start()
    across(0).start()
    each(WINDOWS, lambda k: own(k, i).start(), lambda k: window(k)[0] % 15 != 0)
    sideways(0).wait_recv()
    sideways(1).wait_recv()
    even = lax.broadcasted_iota(jnp.int32, (48, 128), 1) % 2 == 0
    flat[0:48, :] = jnp.where(even, near[0], pltpu.roll(last, 1, 1))
    flat[66 * 24 : 68 * 24, :] = jnp.where(even, pltpu.roll(first, 127, 1), near[1])

    r0 = pl.multiple_of(h * 128, 128)
    bins[0] = column(fb_ref[...])
    bins[1] = column(pb_ref[...])
    mine = bins[0, pl.ds(r0, 128), :]
    masked = jnp.where(jnp.concatenate([mine, mine], axis=1) == fb_ref[...], inv_ref[pl.ds(r0, 128), :], 0.0)
    w = masked / jnp.sum(masked, axis=1, keepdims=True) * 0.0625
    w_hi = w.astype(BF16)
    ww[0:128, :] = w_hi
    ww[128:256, :] = (w - w_hi.astype(F32)).astype(BF16)

    for n in (4, 5, 1, 2, 3):
        across(n).start()
    each(WINDOWS, lambda k: own(k, i).start(), lambda k: window(k)[0] % 15 == 0)
    alone(lambda: here().start())

    def strip(c, slots, t=0, xs=range(4)):
        y0 = pl.multiple_of(c * 16, 16)
        before = pl.multiple_of(jnp.maximum(y0 - 8, 0), 8)
        after = pl.multiple_of(jnp.minimum(y0 + 16, 248), 8)
        first, last = c == 0, c == 15
        u = [[r[x, f, pl.ds(y0, 16), :] for x in range(8)] for f in range(3)]
        for gx in range(1, 7):
            up, down = [], []
            for f in range(3):
                prev = jnp.where(first, 0.0, r[gx, f, pl.ds(before, 8), :])
                succ = jnp.where(last, 0.0, r[gx, f, pl.ds(after, 8), :])
                down.append(jnp.concatenate([prev[7:], u[f][gx][:15]], axis=0))
                up.append(jnp.concatenate([u[f][gx][1:], succ[:1]], axis=0))
            out, mag = fields_of(u, gx, up, down)
            for k in range(21):
                if SLOT[k] in slots:
                    g[t, SLOT[k], gx - 1] = out[k]
            if 2 <= gx <= 5 and 20 in slots:
                keep(c, gx - 2, mag)
        box(c, slots, t, xs)

    def box(c, slots, t, xs):
        y0 = pl.multiple_of(c * 16, 16)
        for k in slots:
            gs = {n: g[t, k, n] for n in range(xs[0], xs[-1] + 3)}
            pairs = {n: gs[n] + gs[n + 1] for n in range(xs[0], xs[-1] + 2)}
            for x in xs:
                total = pairs[x] + pairs[x + 1]
                both = (pltpu.roll(total, 2, 1) + pltpu.roll(total, 126, 1)) + (total + total)
                hi = both.astype(BF16)
                bh[k, pl.ds(y0, 16), pl.ds(x * 128, 128)] = hi
                bl[k, pl.ds(y0, 16), pl.ds(x * 128, 128)] = (both - hi.astype(F32)).astype(BF16)

    def keep(c, x, mag):
        block = jnp.where(c // 8 == h, 2 * c - 16 * h, 16)
        mg[block, x] = mag[:8]
        mg[block + 1, x] = mag[8:]

    def early(t, _):
        strip(9 * h + t, range(21))
        return 0

    def late_a(t, _):
        strip(7 * other + t, range(EARLY))
        return 0

    def late_b(t, _):
        strip(7 * other + t, range(EARLY, 21), t, range(2))
        return 0

    def late_c(t, _):
        box(7 * other + t, range(EARLY, 21), t, range(2, 4))
        return 0

    def products(half, slots):
        for k in slots:
            hi = bh[k, :, pl.ds(half * 256, 256)]
            lo = bl[k, :, pl.ds(half * 256, 256)]
            both = jnp.dot(ww[...], hi, preferred_element_type=F32)
            rest = jnp.dot(ww[0:128, :], lo, preferred_element_type=F32)
            ff[half, k] = both[:128] + (both[128:] + rest)

    def owner(k):
        return (base + xx % 2, h * 16 + mate(k))

    def goes(k):
        return True if k else mixed

    def lengths(k, t=0):
        return send(mg.at[mate(k)], om_ref.at[slot], sm.at[k], rm.at[t], owner(k))

    across(0).wait_recv()
    across(4).wait_recv()
    across(5).wait_recv()
    each(WINDOWS, lambda k: theirs(0, k, i).start())
    alone(lambda: there(0).start())
    alone(lambda: here().wait())
    from_all(lambda q: own(0, q).wait_recv())
    swap(0).start()
    swap(0).wait_recv()
    lax.fori_loop(0, 7, early, 0)
    across(1).wait_recv()
    each(WINDOWS, lambda k: theirs(1, k, i).start())
    alone(lambda: there(1).start())
    for k in ORDER + (0,):
        pl.when(jnp.logical_and(goes(k), mate(k) // 2 != 7 * other))(lambda k=k: lengths(k, slot).start())

    alone(lambda: there(0).wait())
    from_all(lambda q: theirs(0, 0, q).wait_recv())
    swap(1).start()
    across(2).wait_recv()
    each(WINDOWS, lambda k: theirs(2, k, i).start(), lambda k: window(k)[0] <= 8)
    alone(lambda: there(1).wait())
    from_all(lambda q: theirs(1, 0, q).wait_recv())
    swap(2).start()
    across(3).wait_recv()
    each(WINDOWS, lambda k: theirs(2, k, i).start(), lambda k: window(k)[0] > 8)
    alone(lambda: there(2).start())
    swap(1).wait_recv()
    swap(2).wait_recv()
    lax.fori_loop(0, 9, late_a, 0)
    products(0, range(EARLY))
    products(1, range(EARLY))
    alone(lambda: there(2).wait())
    from_all(lambda q: theirs(2, 0, q).wait_recv())
    swap(3).start()
    swap(3).wait_recv()
    lax.fori_loop(0, 9, late_b, 0)

    lanes = lax.broadcasted_iota(jnp.int32, (8, 128), 1)

    def contracts(x0, sums):
        def contract(c, sums):
            y0 = pl.multiple_of(c * 8, 8)
            lm_sum, mm_sum = 0.0, 0.0
            for x in range(2):
                f = [ff[x0 // 2, SLOT[k], pl.ds(y0, 8), pl.ds(x * 128, 128)] for k in range(21)]
                a, b, d = f[0], f[1], f[2]
                t, p, m = f[3:9], f[9:15], f[15:21]
                uu = [a * a, b * b, d * d, a * b, a * d, b * d]
                fmag = 4.0 * twice_norm(t)
                lm, mm = [], []
                for k in range(6):
                    stress = p[k] - uu[k]
                    leo[c, x0 + x, k] = stress
                    mod = m[k] - fmag * t[k]
                    lm.append(stress * mod)
                    mm.append(mod * mod)
                lm_sum += lm[0] + lm[1] + lm[2] + lm[3] + lm[4] + lm[5]
                mm_sum += 2.0 * (mm[0] + mm[1] + mm[2]) + (mm[3] + mm[4] + mm[5])
            hot = bins[1, pl.ds(pl.multiple_of(r0 + y0, 8), 8), :] == lanes
            num = sums[0] + jnp.where(hot, jnp.sum(lm_sum, axis=1, keepdims=True), 0.0)
            den = sums[1] + jnp.where(hot, jnp.sum(mm_sum, axis=1, keepdims=True), 0.0)
            return num, den

        return lax.fori_loop(0, 16, contract, sums)

    def big(half, k, t=0):
        return send(
            leo.at[mate(k), pl.ds(half * 2, 2)], o_ref.at[slot, pl.ds(half * 2, 2)],
            sb.at[half, k], rb.at[half, t], owner(k),
        )

    def small(k):
        return send(part, a1.at[h * 8 + px], ss1.at[k], rs1.at[k], twin(k))

    def second(k):
        return send(s1, a2.at[i], ss2.at[k], rs2.at[k], (px, h * 16 + mate(k)))

    zero = jnp.zeros((8, 128), F32)
    products(0, range(EARLY, 21))
    sums = contracts(0, (zero, zero))
    lax.fori_loop(0, 1, late_c, 0)
    for k in ORDER + (0,):
        pl.when(jnp.logical_and(goes(k), mate(k) // 2 == 7 * other))(lambda k=k: lengths(k, slot).start())
    for k in ORDER:
        big(0, k, slot).start()
    pl.when(mixed)(lambda: big(0, 0, slot).start())
    lax.fori_loop(1, 9, late_c, 0)
    products(1, range(EARLY, 21))
    num, den = contracts(2, sums)
    row = lax.broadcasted_iota(jnp.int32, (8, 128), 0)
    num = jnp.sum(num, axis=0, keepdims=True) * 0.25
    den = jnp.sum(den, axis=0, keepdims=True) * 0.03125
    mine = jnp.where(row == 0, num, jnp.where(row == 1, den, 0.0))
    part[...] = mine
    a1[h * 8 + px] = mine
    for n in range(6):
        across(n).wait_send()
    for n in range(2):
        sideways(n).wait_send()
    for n in range(4):
        swap(n).wait_send()
    each(range(16), lambda k: own(k).wait_send())
    for f in range(3):
        each(range(16), lambda k, f=f: theirs(f, k).wait_send())
    for k in range(1, 16):
        small(k).start()
    for k in ORDER[:6]:
        big(1, k, slot).start()
    keep_here = pltpu.make_async_copy(leo.at[i], o_ref.at[slot], local.at[0])
    alone(keep_here.start)
    keep_length = pltpu.make_async_copy(mg.at[i], om_ref.at[slot], local.at[1])
    alone(keep_length.start)
    for k in range(1, 16):
        small(k).wait_recv()
    total = a1[0]
    for q in range(1, 16):
        total = total + a1[q]
    s1[...] = total
    a2[i] = total
    for k in range(1, 16):
        small(k).wait_send()
    for k in range(1, 16):
        second(k).start()
    for k in ORDER[6:]:
        big(1, k, slot).start()
    pl.when(mixed)(lambda: big(1, 0, slot).start())
    for k in range(1, 16):
        second(k).wait_recv()
    total = a2[0]
    for q in range(1, 16):
        total = total + a2[q]
    tot_ref[...] = total
    alone(keep_here.wait)
    alone(keep_length.wait)
    for k in range(1, 16):
        second(k).wait_send()
        lengths(k).wait_send()
        for half in range(2):
            big(half, k).wait_send()
    pl.when(mixed)(lambda: lengths(0).wait_send())
    for half in range(2):
        pl.when(mixed)(lambda half=half: big(half, 0).wait_send())

    def arrive(t):
        lengths(0, t).wait_recv()
        for half in range(2):
            big(half, 0, t).wait_recv()

    for t in range(16):
        pl.when(jnp.logical_or(mixed, slot != t))(functools.partial(arrive, t))


def to_planes(tot_ref, pb_ref, o_ref, om_ref, leo_ref, visc_ref, coef_ref, mix):
    pz = lax.axis_index("pz")
    per_bin = tot_ref[0:1, :] / jnp.maximum(tot_ref[1:2, :], 65536.0)
    per_bin = jnp.broadcast_to(per_bin, (128, 128)).T
    hot = lax.broadcasted_iota(jnp.int32, (128, 256), 0) == pb_ref[...]
    both = jnp.concatenate([per_bin, per_bin], axis=1)
    coef = jnp.sum(jnp.where(hot, both, 0.0), axis=0, keepdims=True)
    coef_ref[...] = coef
    at = lax.broadcasted_iota(jnp.int32, (1, 256), 1) - pz * 8
    low = lax.broadcasted_iota(jnp.int32, (64, 128), 1) < 64
    y0 = pl.program_id(0) * 4

    def plane(t, _):
        y = y0 + t
        mine = jnp.sum(jnp.where(at == y, coef, 0.0), axis=1, keepdims=True)
        for f in range(7):
            if f < 6:
                m = o_ref[pl.ds(f * 8 + y, 64, stride=48), :]
            else:
                m = om_ref[pl.ds(y, 64, stride=8), :]
            mix[f] = jnp.concatenate([m, m], axis=0).T
            v = jnp.where(low, mix[f, pl.ds(0, 64, stride=2), :], mix[f, pl.ds(1, 64, stride=2), :])
            if f < 6:
                leo_ref[f, t] = v
            else:
                visc_ref[t] = mine * 0.5 * v
        return 0

    lax.fori_loop(0, 4, plane, 0)


def spec(space):
    return pl.BlockSpec(memory_space=space)


def params(**kw):
    return pltpu.CompilerParams(vmem_limit_bytes=56 * 1024 * 1024, **kw)


DMA = pltpu.SemaphoreType.DMA


def local_step(velocity, filter_inverse, filter_block, plane_bin):
    bins = plane_bin.reshape(1, 256)
    part = VMEM((68, 3, 8, 128), F32)
    back, lengths, total = pl.pallas_call(
        core,
        out_shape=(
            jax.ShapeDtypeStruct((16, 4, 6, 8, 128), F32),
            jax.ShapeDtypeStruct((16, 4, 8, 128), F32),
            jax.ShapeDtypeStruct((8, 128), F32),
        ),
        in_specs=[spec(VMEM)] * 4,
        out_specs=(spec(pl.ANY), spec(pl.ANY), spec(VMEM)),
        scratch_shapes=[
            part,
            part,
            VMEM((2, 48, 128), F32),
            VMEM((2, 48, 128), F32),
            VMEM((3, 128, 128), F32),
            VMEM((8, 3, 256, 128), F32),
            VMEM((9, 21, 6, 16, 128), F32),
            VMEM((21, 256, 512), BF16),
            VMEM((21, 256, 512), BF16),
            VMEM((2, 21, 128, 256), F32),
            VMEM((256, 256), BF16),
            VMEM((2, 256, 128), jnp.int32),
            VMEM((16, 4, 6, 8, 128), F32),
            VMEM((18, 4, 8, 128), F32),
            VMEM((8, 128), F32),
            VMEM((16, 8, 128), F32),
            VMEM((16, 8, 128), F32),
            VMEM((8, 128), F32),
            DMA((6,)),
            DMA((6,)),
            DMA((16,)),
            DMA((16,)),
            DMA((3, 16)),
            DMA((3, 16)),
            DMA((2,)),
            DMA((2,)),
            DMA((4,)),
            DMA((4,)),
            DMA((16,)),
            DMA((16,)),
            DMA((16,)),
            DMA((16,)),
            DMA((2, 16)),
            DMA((2, 16)),
            DMA((16,)),
            DMA((16,)),
            DMA((4,)),
        ],
        compiler_params=params(collective_id=0, has_side_effects=True),
        name="core",
    )(
        velocity,
        filter_inverse,
        filter_block.reshape(1, 256),
        bins,
    )
    leonard, viscosity, coefficient = pl.pallas_call(
        to_planes,
        out_shape=(
            jax.ShapeDtypeStruct((6, 8, 64, 128), F32),
            jax.ShapeDtypeStruct((8, 64, 128), F32),
            jax.ShapeDtypeStruct((1, 256), F32),
        ),
        grid=(2,),
        in_specs=[
            pl.BlockSpec((8, 128), lambda q: (0, 0)),
            pl.BlockSpec((1, 256), lambda q: (0, 0)),
            pl.BlockSpec((64 * 48, 128), lambda q: (0, 0)),
            pl.BlockSpec((64 * 8, 128), lambda q: (0, 0)),
        ],
        out_specs=(
            pl.BlockSpec((6, 4, 64, 128), lambda q: (0, q, 0, 0)),
            pl.BlockSpec((4, 64, 128), lambda q: (q, 0, 0)),
            pl.BlockSpec((1, 256), lambda q: (0, 0)),
        ),
        scratch_shapes=[VMEM((7, 128, 128), F32)],
        compiler_params=params(),
        name="to_planes",
    )(total, bins, back.reshape(64 * 48, 128), lengths.reshape(64 * 8, 128))
    return leonard, viscosity, coefficient.reshape(256)


def solution(mesh):
    return jax.shard_map(
        local_step,
        mesh=mesh,
        in_specs=(P(None, "pz", None, "px"), P(), P(), P()),
        out_specs=(P(None, "pz", None, "px"), P("pz", None, "px"), P()),
        check_vma=False,
    )
```

```python
import functools

import jax
import jax.numpy as jnp
from jax import lax
from jax.experimental import pallas as pl
from jax.experimental.pallas import tpu as pltpu
from jax.sharding import PartitionSpec as P

NBIN = 64
MESH = pl.DeviceIdType.MESH
F32 = jnp.float32
BF16 = jnp.bfloat16
VMEM = pltpu.VMEM
ORDER = (10, 6, 14, 8, 9, 11, 2, 5, 15, 13, 7, 1, 3, 4, 12)


WINDOWS = (12, 13, 10, 11, 14, 15, 4, 5, 2, 3, 6, 7, 8, 9, 0, 1)


def where_am_i():
    px, pz = lax.axis_index("px"), lax.axis_index("pz")
    return px, pz, pz // 16, (pz % 16) // 4, pz % 4


SLOT = (0, 1, 8, 2, 3, 9, 4, 10, 11, 5, 6, 12, 7, 13, 14, 15, 16, 17, 18, 19, 20)
EARLY = 8


def fields_of(u, gx, up, down):
    def d_x(f):
        return u[f][gx + 1] - u[f][gx - 1]

    def d_z(f):
        return pltpu.roll(u[f][gx], 126, 1) - pltpu.roll(u[f][gx], 2, 1)

    def d_y(f):
        return up[f] - down[f]

    t = [d_x(0), d_y(1), d_z(2), d_y(0) + d_x(1), d_z(0) + d_x(2), d_z(1) + d_y(2)]
    mag = twice_norm(t)
    a, b, c = u[0][gx], u[1][gx], u[2][gx]
    return [a, b, c] + t + [a * a, b * b, c * c, a * b, a * c, b * c] + [mag * q for q in t], mag


def twice_norm(t):
    return jnp.sqrt(
        2.0 * (t[0] * t[0] + t[1] * t[1] + t[2] * t[2]) + (t[3] * t[3] + t[4] * t[4] + t[5] * t[5])
    )


def column(row):
    return jnp.broadcast_to(row, (128, 256)).T


def core(
    vel_ref, inv_ref, fb_ref, pb_ref, o_ref, om_ref, tot_ref,
    rows, partner, edge, near, mix, r, g, bh, bl, ff, ww, bins, leo, mg, part, a1, a2, s1,
    send_a, recv_a, send_b, recv_b, send_c, recv_c, ss0, rs0, sw, rw, ss1, rs1, ss2, rs2, sb, rb, sm, rm, local,
):
    px, pz, h, yy, xx = where_am_i()
    i = pz % 16
    other = 1 - h

    def mate(k):
        return ((yy + k // 4) % 4) * 4 + (xx + k % 4) % 4

    def twin(k):
        return (px + k % 8) % 8, ((h + k // 8) % 2) * 16 + i

    def send(src, dst, sems, recvs, where):
        return pltpu.make_async_remote_copy(
            src_ref=src, dst_ref=dst, send_sem=sems, recv_sem=recvs, device_id=where, device_id_type=MESH
        )

    core_of = px % 2
    base = px - core_of
    mixed = xx % 2 != core_of
    slot = 2 * (2 * yy + xx // 2) + core_of

    def window(k):
        y2, x2 = (yy + (k // 2) % 4) % 4, (xx // 2 + k // 8) % 2
        t = 2 * (2 * y2 + x2) + k % 2
        return t, (base + k % 2, h * 16 + y2 * 4 + 2 * x2 + core_of)

    def start_of(t):
        return 8 * (t // 2) + 6 * (t % 2)

    def leaves(k):
        return jnp.logical_or(mixed, core_of != k)

    def each(ks, act, also=None):
        for k in ks:
            keep = None if k > 1 else leaves(k)
            if also is not None:
                keep = also(k) if keep is None else jnp.logical_and(keep, also(k))
            if keep is None:
                act(k)
            else:
                pl.when(keep)(functools.partial(act, k))

    def from_all(act):
        for q in range(16):
            pl.when(jnp.logical_or(mixed, i != q))(functools.partial(act, q))

    barrier = pltpu.get_barrier_semaphore()
    for k in range(16):
        for c in range(2):
            if k or c:
                place = (base + (core_of + c) % 2, h * 16 + mate(k))
                pl.semaphore_signal(barrier, inc=1, device_id=place, device_id_type=MESH)
    for k in range(1, 16):
        pl.semaphore_signal(barrier, inc=1, device_id=twin(k), device_id_type=MESH)

    flat = rows.reshape(68 * 24, 128)
    lane = lax.broadcasted_iota(jnp.int32, (64, 128), 1)
    even = lane % 2 == 0

    def plane(y, _):
        for f in range(3):
            v = vel_ref[f, y]
            mix[f, pl.ds(0, 64, stride=2), :] = v
            mix[f, pl.ds(1, 64, stride=2), :] = v
            t = mix[f].T
            flat[pl.ds(48 + f * 8 + y, 64, stride=24), :] = jnp.where(even, t[:64], t[64:])
        return 0

    lax.fori_loop(0, 8, plane, 0)
    first, last = flat[48:96, :], flat[64 * 24 : 66 * 24, :]
    edge[0] = pltpu.roll(last, 127, 1)
    edge[1] = pltpu.roll(first, 1, 1)
    pl.semaphore_wait(barrier, 46)

    own_planes = pl.ds(pl.multiple_of(pz * 8, 8), 8)
    their_planes = pl.ds(pl.multiple_of((other * 16 + i) * 8, 8), 8)

    def across(n):
        piece = (
            (pl.ds(2, 64), 0),
            (pl.ds(2, 64), 1),
            (pl.ds(2, 40), 2),
            (pl.ds(42, 24), 2),
            (pl.ds(0, 2), slice(None)),
            (pl.ds(66, 2), slice(None)),
        )[n]
        return send(rows.at[piece], partner.at[piece], send_a.at[n], recv_a.at[n], (px, other * 16 + i))

    def sideways(n):
        return send(edge.at[n], near.at[n], ss0.at[n], rs0.at[n], ((px + (1, 7)[n]) % 8, pz))

    def own(k, q=0):
        t, place = window(k)
        return send(
            rows.at[pl.ds(start_of(t), 6)], r.at[pl.ds(2 * (k % 2), 6), :, own_planes, :],
            send_b.at[k], recv_b.at[q], place,
        )

    def theirs(f, k, q=0):
        t, place = window(k)
        return send(
            partner.at[pl.ds(start_of(t), 6), f], r.at[pl.ds(2 * (k % 2), 6), f, their_planes, :],
            send_c.at[f, k], recv_c.at[f, q], place,
        )

    def here():
        return pltpu.make_async_copy(
            rows.at[pl.ds(start_of(slot), 6)], r.at[pl.ds(2 * core_of, 6), :, own_planes, :], local.at[0]
        )

    def there(f):
        return pltpu.make_async_copy(
            partner.at[pl.ds(start_of(slot), 6), f],
            r.at[pl.ds(2 * core_of, 6), f, their_planes, :],
            local.at[1 + f],
        )

    def swap(n):
        half = h if n == 0 else other
        which = (slice(None) if n == 0 else n - 1, pl.ds(pl.multiple_of(half * 128, 128), 128), slice(None))
        return send(
            r.at[(pl.ds(4 - 2 * core_of, 2), *which)], r.at[(pl.ds(6 * core_of, 2), *which)],
            sw.at[n], rw.at[n], (base + 1 - core_of, pz),
        )

    def alone(act):
        pl.when(jnp.logical_not(mixed))(act)

    sideways(0).start()
    sideways(1).start()
    across(0).start()
    each(WINDOWS, lambda k: own(k, i).start(), lambda k: window(k)[0] % 15 != 0)
    sideways(0).wait_recv()
    sideways(1).wait_recv()
    even = lax.broadcasted_iota(jnp.int32, (48, 128), 1) % 2 == 0
    flat[0:48, :] = jnp.where(even, near[0], pltpu.roll(last, 1, 1))
    flat[66 * 24 : 68 * 24, :] = jnp.where(even, pltpu.roll(first, 127, 1), near[1])

    r0 = pl.multiple_of(h * 128, 128)
    bins[0] = column(fb_ref[...])
    bins[1] = column(pb_ref[...])
    mine = bins[0, pl.ds(r0, 128), :]
    masked = jnp.where(jnp.concatenate([mine, mine], axis=1) == fb_ref[...], inv_ref[pl.ds(r0, 128), :], 0.0)
    w = masked / jnp.sum(masked, axis=1, keepdims=True) * 0.0625
    w_hi = w.astype(BF16)
    ww[0:128, :] = w_hi
    ww[128:256, :] = (w - w_hi.astype(F32)).astype(BF16)

    for n in (4, 5, 1, 2, 3):
        across(n).start()
    each(WINDOWS, lambda k: own(k, i).start(), lambda k: window(k)[0] % 15 == 0)
    alone(lambda: here().start())

    def strip(c, slots, t=0, xs=range(4)):
        y0 = pl.multiple_of(c * 16, 16)
        before = pl.multiple_of(jnp.maximum(y0 - 8, 0), 8)
        after = pl.multiple_of(jnp.minimum(y0 + 16, 248), 8)
        first, last = c == 0, c == 15
        u = [[r[x, f, pl.ds(y0, 16), :] for x in range(8)] for f in range(3)]
        for gx in range(1, 7):
            up, down = [], []
            for f in range(3):
                prev = jnp.where(first, 0.0, r[gx, f, pl.ds(before, 8), :])
                succ = jnp.where(last, 0.0, r[gx, f, pl.ds(after, 8), :])
                down.append(jnp.concatenate([prev[7:], u[f][gx][:15]], axis=0))
                up.append(jnp.concatenate([u[f][gx][1:], succ[:1]], axis=0))
            out, mag = fields_of(u, gx, up, down)
            for k in range(21):
                if SLOT[k] in slots:
                    g[t, SLOT[k], gx - 1] = out[k]
            if 2 <= gx <= 5 and 20 in slots:
                keep(c, gx - 2, mag)
        box(c, slots, t, xs)

    def box(c, slots, t, xs):
        y0 = pl.multiple_of(c * 16, 16)
        for k in slots:
            gs = {n: g[t, k, n] for n in range(xs[0], xs[-1] + 3)}
            pairs = {n: gs[n] + gs[n + 1] for n in range(xs[0], xs[-1] + 2)}
            for x in xs:
                total = pairs[x] + pairs[x + 1]
                both = (pltpu.roll(total, 2, 1) + pltpu.roll(total, 126, 1)) + (total + total)
                hi = both.astype(BF16)
                bh[k, pl.ds(y0, 16), pl.ds(x * 128, 128)] = hi
                bl[k, pl.ds(y0, 16), pl.ds(x * 128, 128)] = (both - hi.astype(F32)).astype(BF16)

    def keep(c, x, mag):
        block = jnp.where(c // 8 == h, 2 * c - 16 * h, 16)
        mg[block, x] = mag[:8]
        mg[block + 1, x] = mag[8:]

    def early(t, _):
        strip(9 * h + t, range(21))
        return 0

    def late_a(t, _):
        strip(7 * other + t, range(EARLY))
        return 0

    def late_b(t, _):
        strip(7 * other + t, range(EARLY, 21), t, range(2))
        return 0

    def late_c(t, _):
        box(7 * other + t, range(EARLY, 21), t, range(2, 4))
        return 0

    def products(half, slots):
        for k in slots:
            hi = bh[k, :, pl.ds(half * 256, 256)]
            lo = bl[k, :, pl.ds(half * 256, 256)]
            both = jnp.dot(ww[...], hi, preferred_element_type=F32)
            rest = jnp.dot(ww[0:128, :], lo, preferred_element_type=F32)
            ff[half, k] = both[:128] + (both[128:] + rest)

    def owner(k):
        return (base + xx % 2, h * 16 + mate(k))

    def goes(k):
        return True if k else mixed

    def lengths(k, t=0):
        return send(mg.at[mate(k)], om_ref.at[slot], sm.at[k], rm.at[t], owner(k))

    across(0).wait_recv()
    across(4).wait_recv()
    across(5).wait_recv()
    each(WINDOWS, lambda k: theirs(0, k, i).start())
    alone(lambda: there(0).start())
    alone(lambda: here().wait())
    from_all(lambda q: own(0, q).wait_recv())
    swap(0).start()
    swap(0).wait_recv()
    lax.fori_loop(0, 7, early, 0)
    alone(lambda: there(0).wait())
    from_all(lambda q: theirs(0, 0, q).wait_recv())
    swap(1).start()
    for k in ORDER + (0,):
        pl.when(jnp.logical_and(goes(k), mate(k) // 2 != 7 * other))(lambda k=k: lengths(k, slot).start())
    across(1).wait_recv()
    each(WINDOWS, lambda k: theirs(1, k, i).start())
    alone(lambda: there(1).start())
    across(2).wait_recv()
    each(WINDOWS, lambda k: theirs(2, k, i).start(), lambda k: window(k)[0] <= 8)
    across(3).wait_recv()
    each(WINDOWS, lambda k: theirs(2, k, i).start(), lambda k: window(k)[0] > 8)
    alone(lambda: there(2).start())
    alone(lambda: there(1).wait())
    from_all(lambda q: theirs(1, 0, q).wait_recv())
    swap(2).start()
    swap(1).wait_recv()
    swap(2).wait_recv()
    lax.fori_loop(0, 9, late_a, 0)
    products(0, range(EARLY))
    products(1, range(EARLY))
    alone(lambda: there(2).wait())
    from_all(lambda q: theirs(2, 0, q).wait_recv())
    swap(3).start()
    swap(3).wait_recv()
    lax.fori_loop(0, 9, late_b, 0)

    lanes = lax.broadcasted_iota(jnp.int32, (8, 128), 1)

    def contracts(x0, sums):
        def contract(c, sums):
            y0 = pl.multiple_of(c * 8, 8)
            lm_sum, mm_sum = 0.0, 0.0
            for x in range(2):
                f = [ff[x0 // 2, SLOT[k], pl.ds(y0, 8), pl.ds(x * 128, 128)] for k in range(21)]
                a, b, d = f[0], f[1], f[2]
                t, p, m = f[3:9], f[9:15], f[15:21]
                uu = [a * a, b * b, d * d, a * b, a * d, b * d]
                fmag = 4.0 * twice_norm(t)
                lm, mm = [], []
                for k in range(6):
                    stress = p[k] - uu[k]
                    leo[c, x0 + x, k] = stress
                    mod = m[k] - fmag * t[k]
                    lm.append(stress * mod)
                    mm.append(mod * mod)
                lm_sum += lm[0] + lm[1] + lm[2] + lm[3] + lm[4] + lm[5]
                mm_sum += 2.0 * (mm[0] + mm[1] + mm[2]) + (mm[3] + mm[4] + mm[5])
            hot = bins[1, pl.ds(pl.multiple_of(r0 + y0, 8), 8), :] == lanes
            num = sums[0] + jnp.where(hot, jnp.sum(lm_sum, axis=1, keepdims=True), 0.0)
            den = sums[1] + jnp.where(hot, jnp.sum(mm_sum, axis=1, keepdims=True), 0.0)
            return num, den

        return lax.fori_loop(0, 16, contract, sums)

    def big(half, k, t=0):
        return send(
            leo.at[mate(k), pl.ds(half * 2, 2)], o_ref.at[slot, pl.ds(half * 2, 2)],
            sb.at[half, k], rb.at[half, t], owner(k),
        )

    def small(k):
        return send(part, a1.at[h * 8 + px], ss1.at[k], rs1.at[k], twin(k))

    def second(k):
        return send(s1, a2.at[i], ss2.at[k], rs2.at[k], (px, h * 16 + mate(k)))

    zero = jnp.zeros((8, 128), F32)
    products(0, range(EARLY, 21))
    sums = contracts(0, (zero, zero))
    lax.fori_loop(0, 1, late_c, 0)
    for k in ORDER + (0,):
        pl.when(jnp.logical_and(goes(k), mate(k) // 2 == 7 * other))(lambda k=k: lengths(k, slot).start())
    for k in ORDER:
        big(0, k, slot).start()
    pl.when(mixed)(lambda: big(0, 0, slot).start())
    lax.fori_loop(1, 9, late_c, 0)
    products(1, range(EARLY, 21))
    num, den = contracts(2, sums)
    row = lax.broadcasted_iota(jnp.int32, (8, 128), 0)
    num = jnp.sum(num, axis=0, keepdims=True) * 0.25
    den = jnp.sum(den, axis=0, keepdims=True) * 0.03125
    mine = jnp.where(row == 0, num, jnp.where(row == 1, den, 0.0))
    part[...] = mine
    a1[h * 8 + px] = mine
    for n in range(6):
        across(n).wait_send()
    for n in range(2):
        sideways(n).wait_send()
    for n in range(4):
        swap(n).wait_send()
    each(range(16), lambda k: own(k).wait_send())
    for f in range(3):
        each(range(16), lambda k, f=f: theirs(f, k).wait_send())
    for k in range(1, 16):
        small(k).start()
    for k in ORDER[:6]:
        big(1, k, slot).start()
    keep_here = pltpu.make_async_copy(leo.at[i], o_ref.at[slot], local.at[0])
    alone(keep_here.start)
    keep_length = pltpu.make_async_copy(mg.at[i], om_ref.at[slot], local.at[1])
    alone(keep_length.start)
    for k in range(1, 16):
        small(k).wait_recv()
    total = a1[0]
    for q in range(1, 16):
        total = total + a1[q]
    s1[...] = total
    a2[i] = total
    for k in range(1, 16):
        small(k).wait_send()
    for k in range(1, 16):
        second(k).start()
    for k in ORDER[6:]:
        big(1, k, slot).start()
    pl.when(mixed)(lambda: big(1, 0, slot).start())
    for k in range(1, 16):
        second(k).wait_recv()
    total = a2[0]
    for q in range(1, 16):
        total = total + a2[q]
    tot_ref[...] = total
    alone(keep_here.wait)
    alone(keep_length.wait)
    for k in range(1, 16):
        second(k).wait_send()
        lengths(k).wait_send()
        for half in range(2):
            big(half, k).wait_send()
    pl.when(mixed)(lambda: lengths(0).wait_send())
    for half in range(2):
        pl.when(mixed)(lambda half=half: big(half, 0).wait_send())

    def arrive(t):
        lengths(0, t).wait_recv()
        for half in range(2):
            big(half, 0, t).wait_recv()

    for t in range(16):
        pl.when(jnp.logical_or(mixed, slot != t))(functools.partial(arrive, t))


def to_planes(tot_ref, pb_ref, o_ref, om_ref, leo_ref, visc_ref, coef_ref, mix):
    pz = lax.axis_index("pz")
    per_bin = tot_ref[0:1, :] / jnp.maximum(tot_ref[1:2, :], 65536.0)
    per_bin = jnp.broadcast_to(per_bin, (128, 128)).T
    hot = lax.broadcasted_iota(jnp.int32, (128, 256), 0) == pb_ref[...]
    both = jnp.concatenate([per_bin, per_bin], axis=1)
    coef = jnp.sum(jnp.where(hot, both, 0.0), axis=0, keepdims=True)
    coef_ref[...] = coef
    at = lax.broadcasted_iota(jnp.int32, (1, 256), 1) - pz * 8
    low = lax.broadcasted_iota(jnp.int32, (64, 128), 1) < 64
    y0 = pl.program_id(0) * 4

    def plane(t, _):
        y = y0 + t
        mine = jnp.sum(jnp.where(at == y, coef, 0.0), axis=1, keepdims=True)
        for f in range(7):
            if f < 6:
                m = o_ref[pl.ds(f * 8 + y, 64, stride=48), :]
            else:
                m = om_ref[pl.ds(y, 64, stride=8), :]
            mix[f] = jnp.concatenate([m, m], axis=0).T
            v = jnp.where(low, mix[f, pl.ds(0, 64, stride=2), :], mix[f, pl.ds(1, 64, stride=2), :])
            if f < 6:
                leo_ref[f, t] = v
            else:
                visc_ref[t] = mine * 0.5 * v
        return 0

    lax.fori_loop(0, 4, plane, 0)


def spec(space):
    return pl.BlockSpec(memory_space=space)


def params(**kw):
    return pltpu.CompilerParams(vmem_limit_bytes=56 * 1024 * 1024, **kw)


DMA = pltpu.SemaphoreType.DMA


def local_step(velocity, filter_inverse, filter_block, plane_bin):
    bins = plane_bin.reshape(1, 256)
    part = VMEM((68, 3, 8, 128), F32)
    back, lengths, total = pl.pallas_call(
        core,
        out_shape=(
            jax.ShapeDtypeStruct((16, 4, 6, 8, 128), F32),
            jax.ShapeDtypeStruct((16, 4, 8, 128), F32),
            jax.ShapeDtypeStruct((8, 128), F32),
        ),
        in_specs=[spec(VMEM)] * 4,
        out_specs=(spec(pl.ANY), spec(pl.ANY), spec(VMEM)),
        scratch_shapes=[
            part,
            part,
            VMEM((2, 48, 128), F32),
            VMEM((2, 48, 128), F32),
            VMEM((3, 128, 128), F32),
            VMEM((8, 3, 256, 128), F32),
            VMEM((9, 21, 6, 16, 128), F32),
            VMEM((21, 256, 512), BF16),
            VMEM((21, 256, 512), BF16),
            VMEM((2, 21, 128, 256), F32),
            VMEM((256, 256), BF16),
            VMEM((2, 256, 128), jnp.int32),
            VMEM((16, 4, 6, 8, 128), F32),
            VMEM((18, 4, 8, 128), F32),
            VMEM((8, 128), F32),
            VMEM((16, 8, 128), F32),
            VMEM((16, 8, 128), F32),
            VMEM((8, 128), F32),
            DMA((6,)),
            DMA((6,)),
            DMA((16,)),
            DMA((16,)),
            DMA((3, 16)),
            DMA((3, 16)),
            DMA((2,)),
            DMA((2,)),
            DMA((4,)),
            DMA((4,)),
            DMA((16,)),
            DMA((16,)),
            DMA((16,)),
            DMA((16,)),
            DMA((2, 16)),
            DMA((2, 16)),
            DMA((16,)),
            DMA((16,)),
            DMA((4,)),
        ],
        compiler_params=params(collective_id=0, has_side_effects=True),
        name="core",
    )(
        velocity,
        filter_inverse,
        filter_block.reshape(1, 256),
        bins,
    )
    leonard, viscosity, coefficient = pl.pallas_call(
        to_planes,
        out_shape=(
            jax.ShapeDtypeStruct((6, 8, 64, 128), F32),
            jax.ShapeDtypeStruct((8, 64, 128), F32),
            jax.ShapeDtypeStruct((1, 256), F32),
        ),
        grid=(2,),
        in_specs=[
            pl.BlockSpec((8, 128), lambda q: (0, 0)),
            pl.BlockSpec((1, 256), lambda q: (0, 0)),
            pl.BlockSpec((64 * 48, 128), lambda q: (0, 0)),
            pl.BlockSpec((64 * 8, 128), lambda q: (0, 0)),
        ],
        out_specs=(
            pl.BlockSpec((6, 4, 64, 128), lambda q: (0, q, 0, 0)),
            pl.BlockSpec((4, 64, 128), lambda q: (q, 0, 0)),
            pl.BlockSpec((1, 256), lambda q: (0, 0)),
        ),
        scratch_shapes=[VMEM((7, 128, 128), F32)],
        compiler_params=params(),
        name="to_planes",
    )(total, bins, back.reshape(64 * 48, 128), lengths.reshape(64 * 8, 128))
    return leonard, viscosity, coefficient.reshape(256)


def solution(mesh):
    return jax.shard_map(
        local_step,
        mesh=mesh,
        in_specs=(P(None, "pz", None, "px"), P(), P(), P()),
        out_specs=(P(None, "pz", None, "px"), P("pz", None, "px"), P()),
        check_vma=False,
    )
```

```python
import functools

import jax
import jax.numpy as jnp
from jax import lax
from jax.experimental import pallas as pl
from jax.experimental.pallas import tpu as pltpu
from jax.sharding import PartitionSpec as P

NBIN = 64
MESH = pl.DeviceIdType.MESH
F32 = jnp.float32
BF16 = jnp.bfloat16
VMEM = pltpu.VMEM
ORDER = (10, 6, 14, 8, 9, 11, 2, 5, 15, 13, 7, 1, 3, 4, 12)


WINDOWS = (12, 13, 10, 11, 14, 15, 4, 5, 2, 3, 6, 7, 8, 9, 0, 1)


def where_am_i():
    px, pz = lax.axis_index("px"), lax.axis_index("pz")
    return px, pz, pz // 16, (pz % 16) // 4, pz % 4


SLOT = (0, 1, 8, 2, 3, 9, 4, 10, 11, 5, 6, 12, 7, 13, 14, 15, 16, 17, 18, 19, 20)
EARLY = 8


def fields_of(u, gx, up, down):
    def d_x(f):
        return u[f][gx + 1] - u[f][gx - 1]

    def d_z(f):
        return pltpu.roll(u[f][gx], 126, 1) - pltpu.roll(u[f][gx], 2, 1)

    def d_y(f):
        return up[f] - down[f]

    t = [d_x(0), d_y(1), d_z(2), d_y(0) + d_x(1), d_z(0) + d_x(2), d_z(1) + d_y(2)]
    mag = twice_norm(t)
    a, b, c = u[0][gx], u[1][gx], u[2][gx]
    return [a, b, c] + t + [a * a, b * b, c * c, a * b, a * c, b * c] + [mag * q for q in t], mag


def twice_norm(t):
    return jnp.sqrt(
        2.0 * (t[0] * t[0] + t[1] * t[1] + t[2] * t[2]) + (t[3] * t[3] + t[4] * t[4] + t[5] * t[5])
    )


def column(row):
    return jnp.broadcast_to(row, (128, 256)).T


def core(
    vel_ref, inv_ref, fb_ref, pb_ref, o_ref, om_ref, tot_ref,
    rows, partner, edge, near, mix, r, g, bh, bl, ff, ww, bins, leo, mg, part, a1, a2, s1,
    send_a, recv_a, send_b, recv_b, send_c, recv_c, ss0, rs0, sw, rw, ss1, rs1, ss2, rs2, sb, rb, sm, rm, local,
):
    px, pz, h, yy, xx = where_am_i()
    i = pz % 16
    other = 1 - h

    def mate(k):
        return ((yy + k // 4) % 4) * 4 + (xx + k % 4) % 4

    def twin(k):
        return (px + k % 8) % 8, ((h + k // 8) % 2) * 16 + i

    def send(src, dst, sems, recvs, where):
        return pltpu.make_async_remote_copy(
            src_ref=src, dst_ref=dst, send_sem=sems, recv_sem=recvs, device_id=where, device_id_type=MESH
        )

    core_of = px % 2
    base = px - core_of
    mixed = xx % 2 != core_of
    slot = 2 * (2 * yy + xx // 2) + core_of

    def window(k):
        y2, x2 = (yy + (k // 2) % 4) % 4, (xx // 2 + k // 8) % 2
        t = 2 * (2 * y2 + x2) + k % 2
        return t, (base + k % 2, h * 16 + y2 * 4 + 2 * x2 + core_of)

    def start_of(t):
        return 8 * (t // 2) + 6 * (t % 2)

    def leaves(k):
        return jnp.logical_or(mixed, core_of != k)

    def each(ks, act, also=None):
        for k in ks:
            keep = None if k > 1 else leaves(k)
            if also is not None:
                keep = also(k) if keep is None else jnp.logical_and(keep, also(k))
            if keep is None:
                act(k)
            else:
                pl.when(keep)(functools.partial(act, k))

    def from_all(act):
        for q in range(16):
            pl.when(jnp.logical_or(mixed, i != q))(functools.partial(act, q))

    barrier = pltpu.get_barrier_semaphore()
    for k in range(16):
        for c in range(2):
            if k or c:
                place = (base + (core_of + c) % 2, h * 16 + mate(k))
                pl.semaphore_signal(barrier, inc=1, device_id=place, device_id_type=MESH)
    for k in range(1, 16):
        pl.semaphore_signal(barrier, inc=1, device_id=twin(k), device_id_type=MESH)

    flat = rows.reshape(68 * 24, 128)
    lane = lax.broadcasted_iota(jnp.int32, (64, 128), 1)
    even = lane % 2 == 0

    def plane(y, _):
        for f in range(3):
            v = vel_ref[f, y]
            mix[f, pl.ds(0, 64, stride=2), :] = v
            mix[f, pl.ds(1, 64, stride=2), :] = v
            t = mix[f].T
            flat[pl.ds(48 + f * 8 + y, 64, stride=24), :] = jnp.where(even, t[:64], t[64:])
        return 0

    lax.fori_loop(0, 8, plane, 0)
    first, last = flat[48:96, :], flat[64 * 24 : 66 * 24, :]
    edge[0] = pltpu.roll(last, 127, 1)
    edge[1] = pltpu.roll(first, 1, 1)
    pl.semaphore_wait(barrier, 46)

    own_planes = pl.ds(pl.multiple_of(pz * 8, 8), 8)
    their_planes = pl.ds(pl.multiple_of((other * 16 + i) * 8, 8), 8)

    def across(n):
        piece = (
            (pl.ds(2, 64), 0),
            (pl.ds(2, 64), 1),
            (pl.ds(2, 40), 2),
            (pl.ds(42, 24), 2),
            (pl.ds(0, 2), slice(None)),
            (pl.ds(66, 2), slice(None)),
        )[n]
        return send(rows.at[piece], partner.at[piece], send_a.at[n], recv_a.at[n], (px, other * 16 + i))

    def sideways(n):
        return send(edge.at[n], near.at[n], ss0.at[n], rs0.at[n], ((px + (1, 7)[n]) % 8, pz))

    def own(k, q=0):
        t, place = window(k)
        return send(
            rows.at[pl.ds(start_of(t), 6)], r.at[pl.ds(2 * (k % 2), 6), :, own_planes, :],
            send_b.at[k], recv_b.at[q], place,
        )

    def theirs(f, k, q=0):
        t, place = window(k)
        return send(
            partner.at[pl.ds(start_of(t), 6), f], r.at[pl.ds(2 * (k % 2), 6), f, their_planes, :],
            send_c.at[f, k], recv_c.at[f, q], place,
        )

    def here():
        return pltpu.make_async_copy(
            rows.at[pl.ds(start_of(slot), 6)], r.at[pl.ds(2 * core_of, 6), :, own_planes, :], local.at[0]
        )

    def there(f):
        return pltpu.make_async_copy(
            partner.at[pl.ds(start_of(slot), 6), f],
            r.at[pl.ds(2 * core_of, 6), f, their_planes, :],
            local.at[1 + f],
        )

    def swap(n):
        half = h if n == 0 else other
        which = (slice(None) if n == 0 else n - 1, pl.ds(pl.multiple_of(half * 128, 128), 128), slice(None))
        return send(
            r.at[(pl.ds(4 - 2 * core_of, 2), *which)], r.at[(pl.ds(6 * core_of, 2), *which)],
            sw.at[n], rw.at[n], (base + 1 - core_of, pz),
        )

    def alone(act):
        pl.when(jnp.logical_not(mixed))(act)

    sideways(0).start()
    sideways(1).start()
    across(0).start()
    each(WINDOWS, lambda k: own(k, i).start(), lambda k: window(k)[0] % 15 != 0)
    sideways(0).wait_recv()
    sideways(1).wait_recv()
    even = lax.broadcasted_iota(jnp.int32, (48, 128), 1) % 2 == 0
    flat[0:48, :] = jnp.where(even, near[0], pltpu.roll(last, 1, 1))
    flat[66 * 24 : 68 * 24, :] = jnp.where(even, pltpu.roll(first, 127, 1), near[1])

    r0 = pl.multiple_of(h * 128, 128)
    bins[0] = column(fb_ref[...])
    bins[1] = column(pb_ref[...])
    mine = bins[0, pl.ds(r0, 128), :]
    masked = jnp.where(jnp.concatenate([mine, mine], axis=1) == fb_ref[...], inv_ref[pl.ds(r0, 128), :], 0.0)
    w = masked / jnp.sum(masked, axis=1, keepdims=True) * 0.0625
    w_hi = w.astype(BF16)
    ww[0:128, :] = w_hi
    ww[128:256, :] = (w - w_hi.astype(F32)).astype(BF16)

    for n in (4, 5, 1, 2, 3):
        across(n).start()
    each(WINDOWS, lambda k: own(k, i).start(), lambda k: window(k)[0] % 15 == 0)
    alone(lambda: here().start())

    def fields(c, slots, t, x0, count):
        y0 = pl.multiple_of(c * 16, 16)
        before = pl.multiple_of(jnp.maximum(y0 - 8, 0), 8)
        after = pl.multiple_of(jnp.minimum(y0 + 16, 248), 8)
        first, last = c == 0, c == 15
        u = [[r[x0 + x, f, pl.ds(y0, 16), :] for x in range(count + 2)] for f in range(3)]
        for gx in range(1, count + 1):
            up, down = [], []
            for f in range(3):
                prev = jnp.where(first, 0.0, r[x0 + gx, f, pl.ds(before, 8), :])
                succ = jnp.where(last, 0.0, r[x0 + gx, f, pl.ds(after, 8), :])
                down.append(jnp.concatenate([prev[7:], u[f][gx][:15]], axis=0))
                up.append(jnp.concatenate([u[f][gx][1:], succ[:1]], axis=0))
            out, mag = fields_of(u, gx, up, down)
            for k in range(21):
                if SLOT[k] in slots:
                    g[t, SLOT[k], x0 + gx - 1] = out[k]
            if 20 in slots:
                block = jnp.where(c // 8 == h, 2 * c - 16 * h, 16)
                mg[block, x0 + gx - 1] = mag[:8]
                mg[block + 1, x0 + gx - 1] = mag[8:]

    def box(c, slots, t, x0, count):
        y0 = pl.multiple_of(c * 16, 16)
        for k in slots:
            gs = [g[t, k, x0 + n] for n in range(count + 2)]
            pairs = [gs[n] + gs[n + 1] for n in range(count + 1)]
            for x in range(count):
                total = pairs[x] + pairs[x + 1]
                both = (pltpu.roll(total, 2, 1) + pltpu.roll(total, 126, 1)) + (total + total)
                hi = both.astype(BF16)
                at = pl.ds(pl.multiple_of((x0 + x) * 128, 128), 128)
                bh[k, pl.ds(y0, 16), at] = hi
                bl[k, pl.ds(y0, 16), at] = (both - hi.astype(F32)).astype(BF16)

    def early(t, _):
        fields(9 * h + t, range(21), 0, 0, 6)
        box(9 * h + t, range(21), 0, 0, 4)
        return 0

    def late_a(t, _):
        fields(7 * other + t, range(EARLY), t, 0, 6)
        box(7 * other + t, range(EARLY), t, 0, 4)
        return 0

    near_pair = core_of
    far_pair = 1 - core_of

    def late_b(t, _):
        fields(7 * other + t, range(EARLY, 21), t, 2 * near_pair, 4)
        box(7 * other + t, range(EARLY, 21), t, 2 * near_pair, 2)
        return 0

    def late_c(t, _):
        fields(7 * other + t, range(EARLY, 21), t, 4 * far_pair, 2)
        box(7 * other + t, range(EARLY, 21), t, 2 * far_pair, 2)
        return 0

    def products(half, slots):
        for k in slots:
            at = pl.ds(pl.multiple_of(half * 256, 256), 256)
            hi, lo = bh[k, :, at], bl[k, :, at]
            both = jnp.dot(ww[...], hi, preferred_element_type=F32)
            rest = jnp.dot(ww[0:128, :], lo, preferred_element_type=F32)
            ff[half, k] = both[:128] + (both[128:] + rest)

    def owner(k):
        return (base + xx % 2, h * 16 + mate(k))

    def goes(k):
        return True if k else mixed

    def lengths(k, t=0):
        return send(mg.at[mate(k), pl.ds(1, 4)], om_ref.at[slot], sm.at[k], rm.at[t], owner(k))

    across(0).wait_recv()
    across(4).wait_recv()
    across(5).wait_recv()
    each(WINDOWS, lambda k: theirs(0, k, i).start())
    alone(lambda: there(0).start())
    alone(lambda: here().wait())
    from_all(lambda q: own(0, q).wait_recv())
    swap(0).start()
    swap(0).wait_recv()
    lax.fori_loop(0, 7, early, 0)
    alone(lambda: there(0).wait())
    from_all(lambda q: theirs(0, 0, q).wait_recv())
    swap(1).start()
    for k in ORDER + (0,):
        pl.when(jnp.logical_and(goes(k), mate(k) // 2 != 7 * other))(lambda k=k: lengths(k, slot).start())
    across(1).wait_recv()
    each(WINDOWS, lambda k: theirs(1, k, i).start())
    alone(lambda: there(1).start())
    across(2).wait_recv()
    each(WINDOWS, lambda k: theirs(2, k, i).start(), lambda k: window(k)[0] <= 8)
    across(3).wait_recv()
    each(WINDOWS, lambda k: theirs(2, k, i).start(), lambda k: window(k)[0] > 8)
    alone(lambda: there(2).start())
    alone(lambda: there(1).wait())
    from_all(lambda q: theirs(1, 0, q).wait_recv())
    swap(2).start()
    swap(1).wait_recv()
    swap(2).wait_recv()
    lax.fori_loop(0, 9, late_a, 0)
    products(0, range(EARLY))
    products(1, range(EARLY))
    alone(lambda: there(2).wait())
    from_all(lambda q: theirs(2, 0, q).wait_recv())
    swap(3).start()
    lax.fori_loop(0, 9, late_b, 0)

    lanes = lax.broadcasted_iota(jnp.int32, (8, 128), 1)

    def contracts(half, sums):
        x0 = 2 * half

        def contract(c, sums):
            y0 = pl.multiple_of(c * 8, 8)
            lm_sum, mm_sum = 0.0, 0.0
            for x in range(2):
                f = [ff[half, SLOT[k], pl.ds(y0, 8), pl.ds(x * 128, 128)] for k in range(21)]
                a, b, d = f[0], f[1], f[2]
                t, p, m = f[3:9], f[9:15], f[15:21]
                uu = [a * a, b * b, d * d, a * b, a * d, b * d]
                fmag = 4.0 * twice_norm(t)
                lm, mm = [], []
                for k in range(6):
                    stress = p[k] - uu[k]
                    leo[c, x0 + x, k] = stress
                    mod = m[k] - fmag * t[k]
                    lm.append(stress * mod)
                    mm.append(mod * mod)
                lm_sum += lm[0] + lm[1] + lm[2] + lm[3] + lm[4] + lm[5]
                mm_sum += 2.0 * (mm[0] + mm[1] + mm[2]) + (mm[3] + mm[4] + mm[5])
            hot = bins[1, pl.ds(pl.multiple_of(r0 + y0, 8), 8), :] == lanes
            num = sums[0] + jnp.where(hot, jnp.sum(lm_sum, axis=1, keepdims=True), 0.0)
            den = sums[1] + jnp.where(hot, jnp.sum(mm_sum, axis=1, keepdims=True), 0.0)
            return num, den

        return lax.fori_loop(0, 16, contract, sums)

    def big(n, k, t=0):
        pair = pl.ds(2 * (far_pair if n else near_pair), 2)
        return send(
            leo.at[mate(k), pair], o_ref.at[slot, pair], sb.at[n, k], rb.at[n, t], owner(k)
        )

    def small(k):
        return send(part, a1.at[h * 8 + px], ss1.at[k], rs1.at[k], twin(k))

    def second(k):
        return send(s1, a2.at[i], ss2.at[k], rs2.at[k], (px, h * 16 + mate(k)))

    zero = jnp.zeros((8, 128), F32)
    products(near_pair, range(EARLY, 21))
    sums = contracts(near_pair, (zero, zero))
    swap(3).wait_recv()
    lax.fori_loop(0, 1, late_c, 0)
    for k in ORDER:
        big(0, k, slot).start()
    pl.when(mixed)(lambda: big(0, 0, slot).start())
    lax.fori_loop(1, 9, late_c, 0)
    products(far_pair, range(EARLY, 21))
    for k in ORDER + (0,):
        pl.when(jnp.logical_and(goes(k), mate(k) // 2 == 7 * other))(lambda k=k: lengths(k, slot).start())
    num, den = contracts(far_pair, sums)
    row = lax.broadcasted_iota(jnp.int32, (8, 128), 0)
    num = jnp.sum(num, axis=0, keepdims=True) * 0.25
    den = jnp.sum(den, axis=0, keepdims=True) * 0.03125
    mine = jnp.where(row == 0, num, jnp.where(row == 1, den, 0.0))
    part[...] = mine
    a1[h * 8 + px] = mine
    for n in range(6):
        across(n).wait_send()
    for n in range(2):
        sideways(n).wait_send()
    for n in range(4):
        swap(n).wait_send()
    each(range(16), lambda k: own(k).wait_send())
    for f in range(3):
        each(range(16), lambda k, f=f: theirs(f, k).wait_send())
    for k in range(1, 16):
        small(k).start()
    for k in ORDER[:6]:
        big(1, k, slot).start()
    keep_here = pltpu.make_async_copy(leo.at[i], o_ref.at[slot], local.at[0])
    alone(keep_here.start)
    keep_length = pltpu.make_async_copy(mg.at[i, pl.ds(1, 4)], om_ref.at[slot], local.at[1])
    alone(keep_length.start)
    for k in range(1, 16):
        small(k).wait_recv()
    total = a1[0]
    for q in range(1, 16):
        total = total + a1[q]
    s1[...] = total
    a2[i] = total
    for k in range(1, 16):
        small(k).wait_send()
    for k in range(1, 16):
        second(k).start()
    for k in ORDER[6:]:
        big(1, k, slot).start()
    pl.when(mixed)(lambda: big(1, 0, slot).start())
    for k in range(1, 16):
        second(k).wait_recv()
    total = a2[0]
    for q in range(1, 16):
        total = total + a2[q]
    tot_ref[...] = total
    alone(keep_here.wait)
    alone(keep_length.wait)
    for k in range(1, 16):
        second(k).wait_send()
        lengths(k).wait_send()
        for half in range(2):
            big(half, k).wait_send()
    pl.when(mixed)(lambda: lengths(0).wait_send())
    for half in range(2):
        pl.when(mixed)(lambda half=half: big(half, 0).wait_send())

    def arrive(t):
        lengths(0, t).wait_recv()
        for half in range(2):
            big(half, 0, t).wait_recv()

    for t in range(16):
        pl.when(jnp.logical_or(mixed, slot != t))(functools.partial(arrive, t))


def to_planes(tot_ref, pb_ref, o_ref, om_ref, leo_ref, visc_ref, coef_ref, mix):
    pz = lax.axis_index("pz")
    per_bin = tot_ref[0:1, :] / jnp.maximum(tot_ref[1:2, :], 65536.0)
    per_bin = jnp.broadcast_to(per_bin, (128, 128)).T
    hot = lax.broadcasted_iota(jnp.int32, (128, 256), 0) == pb_ref[...]
    both = jnp.concatenate([per_bin, per_bin], axis=1)
    coef = jnp.sum(jnp.where(hot, both, 0.0), axis=0, keepdims=True)
    coef_ref[...] = coef
    at = lax.broadcasted_iota(jnp.int32, (1, 256), 1) - pz * 8
    low = lax.broadcasted_iota(jnp.int32, (64, 128), 1) < 64
    y0 = pl.program_id(0) * 4

    def plane(t, _):
        y = y0 + t
        mine = jnp.sum(jnp.where(at == y, coef, 0.0), axis=1, keepdims=True)
        for f in range(7):
            if f < 6:
                m = o_ref[pl.ds(f * 8 + y, 64, stride=48), :]
            else:
                m = om_ref[pl.ds(y, 64, stride=8), :]
            mix[f] = jnp.concatenate([m, m], axis=0).T
            v = jnp.where(low, mix[f, pl.ds(0, 64, stride=2), :], mix[f, pl.ds(1, 64, stride=2), :])
            if f < 6:
                leo_ref[f, t] = v
            else:
                visc_ref[t] = mine * 0.5 * v
        return 0

    lax.fori_loop(0, 4, plane, 0)


def spec(space):
    return pl.BlockSpec(memory_space=space)


def params(**kw):
    return pltpu.CompilerParams(vmem_limit_bytes=56 * 1024 * 1024, **kw)


DMA = pltpu.SemaphoreType.DMA


def local_step(velocity, filter_inverse, filter_block, plane_bin):
    bins = plane_bin.reshape(1, 256)
    part = VMEM((68, 3, 8, 128), F32)
    back, lengths, total = pl.pallas_call(
        core,
        out_shape=(
            jax.ShapeDtypeStruct((16, 4, 6, 8, 128), F32),
            jax.ShapeDtypeStruct((16, 4, 8, 128), F32),
            jax.ShapeDtypeStruct((8, 128), F32),
        ),
        in_specs=[spec(VMEM)] * 4,
        out_specs=(spec(pl.ANY), spec(pl.ANY), spec(VMEM)),
        scratch_shapes=[
            part,
            part,
            VMEM((2, 48, 128), F32),
            VMEM((2, 48, 128), F32),
            VMEM((3, 128, 128), F32),
            VMEM((8, 3, 256, 128), F32),
            VMEM((9, 21, 6, 16, 128), F32),
            VMEM((21, 256, 512), BF16),
            VMEM((21, 256, 512), BF16),
            VMEM((2, 21, 128, 256), F32),
            VMEM((256, 256), BF16),
            VMEM((2, 256, 128), jnp.int32),
            VMEM((16, 4, 6, 8, 128), F32),
            VMEM((18, 6, 8, 128), F32),
            VMEM((8, 128), F32),
            VMEM((16, 8, 128), F32),
            VMEM((16, 8, 128), F32),
            VMEM((8, 128), F32),
            DMA((6,)),
            DMA((6,)),
            DMA((16,)),
            DMA((16,)),
            DMA((3, 16)),
            DMA((3, 16)),
            DMA((2,)),
            DMA((2,)),
            DMA((4,)),
            DMA((4,)),
            DMA((16,)),
            DMA((16,)),
            DMA((16,)),
            DMA((16,)),
            DMA((2, 16)),
            DMA((2, 16)),
            DMA((16,)),
            DMA((16,)),
            DMA((4,)),
        ],
        compiler_params=params(collective_id=0, has_side_effects=True),
        name="core",
    )(
        velocity,
        filter_inverse,
        filter_block.reshape(1, 256),
        bins,
    )
    leonard, viscosity, coefficient = pl.pallas_call(
        to_planes,
        out_shape=(
            jax.ShapeDtypeStruct((6, 8, 64, 128), F32),
            jax.ShapeDtypeStruct((8, 64, 128), F32),
            jax.ShapeDtypeStruct((1, 256), F32),
        ),
        grid=(2,),
        in_specs=[
            pl.BlockSpec((8, 128), lambda q: (0, 0)),
            pl.BlockSpec((1, 256), lambda q: (0, 0)),
            pl.BlockSpec((64 * 48, 128), lambda q: (0, 0)),
            pl.BlockSpec((64 * 8, 128), lambda q: (0, 0)),
        ],
        out_specs=(
            pl.BlockSpec((6, 4, 64, 128), lambda q: (0, q, 0, 0)),
            pl.BlockSpec((4, 64, 128), lambda q: (q, 0, 0)),
            pl.BlockSpec((1, 256), lambda q: (0, 0)),
        ),
        scratch_shapes=[VMEM((7, 128, 128), F32)],
        compiler_params=params(),
        name="to_planes",
    )(total, bins, back.reshape(64 * 48, 128), lengths.reshape(64 * 8, 128))
    return leonard, viscosity, coefficient.reshape(256)


def solution(mesh):
    return jax.shard_map(
        local_step,
        mesh=mesh,
        in_specs=(P(None, "pz", None, "px"), P(), P(), P()),
        out_specs=(P(None, "pz", None, "px"), P("pz", None, "px"), P()),
        check_vma=False,
    )
```

```python
import functools

import jax
import jax.numpy as jnp
from jax import lax
from jax.experimental import pallas as pl
from jax.experimental.pallas import tpu as pltpu
from jax.sharding import PartitionSpec as P

NBIN = 64
MESH = pl.DeviceIdType.MESH
F32 = jnp.float32
BF16 = jnp.bfloat16
VMEM = pltpu.VMEM
ORDER = (10, 6, 14, 8, 9, 11, 2, 5, 15, 13, 7, 1, 3, 4, 12)


WINDOWS = (12, 10, 14, 13, 11, 15, 4, 2, 6, 8, 5, 3, 7, 9, 0, 1)


def where_am_i():
    px, pz = lax.axis_index("px"), lax.axis_index("pz")
    return px, pz, pz // 16, (pz % 16) // 4, pz % 4


SLOT = (0, 1, 8, 2, 3, 9, 4, 10, 11, 5, 6, 12, 7, 13, 14, 15, 16, 17, 18, 19, 20)
EARLY = 8


def fields_of(u, gx, up, down):
    def d_x(f):
        return u[f][gx + 1] - u[f][gx - 1]

    def d_z(f):
        return pltpu.roll(u[f][gx], 126, 1) - pltpu.roll(u[f][gx], 2, 1)

    def d_y(f):
        return up[f] - down[f]

    t = [d_x(0), d_y(1), d_z(2), d_y(0) + d_x(1), d_z(0) + d_x(2), d_z(1) + d_y(2)]
    mag = twice_norm(t)
    a, b, c = u[0][gx], u[1][gx], u[2][gx]
    return [a, b, c] + t + [a * a, b * b, c * c, a * b, a * c, b * c] + [mag * q for q in t], mag


def twice_norm(t):
    return jnp.sqrt(
        2.0 * (t[0] * t[0] + t[1] * t[1] + t[2] * t[2]) + (t[3] * t[3] + t[4] * t[4] + t[5] * t[5])
    )


def column(row):
    return jnp.broadcast_to(row, (128, 256)).T


def core(
    vel_ref, inv_ref, fb_ref, pb_ref, o_ref, om_ref, tot_ref,
    rows, partner, edge, near, mix, r, g, bh, bl, ff, ww, bins, leo, mg, part, a1, a2, s1,
    send_a, recv_a, send_b, recv_b, send_c, recv_c, ss0, rs0, sw, rw, ss1, rs1, ss2, rs2, sb, rb, sm, rm, local,
):
    px, pz, h, yy, xx = where_am_i()
    i = pz % 16
    other = 1 - h

    def mate(k):
        return ((yy + k // 4) % 4) * 4 + (xx + k % 4) % 4

    def twin(k):
        return (px + k % 8) % 8, ((h + k // 8) % 2) * 16 + i

    def send(src, dst, sems, recvs, where):
        return pltpu.make_async_remote_copy(
            src_ref=src, dst_ref=dst, send_sem=sems, recv_sem=recvs, device_id=where, device_id_type=MESH
        )

    core_of = px % 2
    base = px - core_of
    mixed = xx % 2 != core_of
    slot = 2 * (2 * yy + xx // 2) + core_of

    def window(k):
        y2, x2 = (yy + (k // 2) % 4) % 4, (xx // 2 + k // 8) % 2
        t = 2 * (2 * y2 + x2) + k % 2
        return t, (base + k % 2, h * 16 + y2 * 4 + 2 * x2 + core_of)

    def start_of(t):
        return 8 * (t // 2) + 6 * (t % 2)

    def leaves(k):
        return jnp.logical_or(mixed, core_of != k)

    def each(ks, act, also=None):
        for k in ks:
            keep = None if k > 1 else leaves(k)
            if also is not None:
                keep = also(k) if keep is None else jnp.logical_and(keep, also(k))
            if keep is None:
                act(k)
            else:
                pl.when(keep)(functools.partial(act, k))

    def from_all(act):
        for q in range(16):
            pl.when(jnp.logical_or(mixed, i != q))(functools.partial(act, q))

    barrier = pltpu.get_barrier_semaphore()
    for k in range(16):
        for c in range(2):
            if k or c:
                place = (base + (core_of + c) % 2, h * 16 + mate(k))
                pl.semaphore_signal(barrier, inc=1, device_id=place, device_id_type=MESH)
    for k in range(1, 16):
        pl.semaphore_signal(barrier, inc=1, device_id=twin(k), device_id_type=MESH)

    flat = rows.reshape(68 * 24, 128)
    lane = lax.broadcasted_iota(jnp.int32, (64, 128), 1)
    even = lane % 2 == 0

    def plane(y, _):
        for f in range(3):
            v = vel_ref[f, y]
            mix[f, pl.ds(0, 64, stride=2), :] = v
            mix[f, pl.ds(1, 64, stride=2), :] = v
            t = mix[f].T
            flat[pl.ds(48 + f * 8 + y, 64, stride=24), :] = jnp.where(even, t[:64], t[64:])
        return 0

    lax.fori_loop(0, 8, plane, 0)
    first, last = flat[48:96, :], flat[64 * 24 : 66 * 24, :]
    edge[0] = pltpu.roll(last, 127, 1)
    edge[1] = pltpu.roll(first, 1, 1)
    pl.semaphore_wait(barrier, 46)

    own_planes = pl.ds(pl.multiple_of(pz * 8, 8), 8)
    their_planes = pl.ds(pl.multiple_of((other * 16 + i) * 8, 8), 8)

    def across(n):
        piece = (
            (pl.ds(2, 64), 0),
            (pl.ds(2, 64), 1),
            (pl.ds(2, 40), 2),
            (pl.ds(42, 24), 2),
            (pl.ds(0, 2), slice(None)),
            (pl.ds(66, 2), slice(None)),
        )[n]
        return send(rows.at[piece], partner.at[piece], send_a.at[n], recv_a.at[n], (px, other * 16 + i))

    def sideways(n):
        return send(edge.at[n], near.at[n], ss0.at[n], rs0.at[n], ((px + (1, 7)[n]) % 8, pz))

    def own(k, q=0):
        t, place = window(k)
        return send(
            rows.at[pl.ds(start_of(t), 6)], r.at[pl.ds(2 * (k % 2), 6), :, own_planes, :],
            send_b.at[k], recv_b.at[q], place,
        )

    def theirs(f, k, q=0):
        t, place = window(k)
        return send(
            partner.at[pl.ds(start_of(t), 6), f], r.at[pl.ds(2 * (k % 2), 6), f, their_planes, :],
            send_c.at[f, k], recv_c.at[f, q], place,
        )

    def here():
        return pltpu.make_async_copy(
            rows.at[pl.ds(start_of(slot), 6)], r.at[pl.ds(2 * core_of, 6), :, own_planes, :], local.at[0]
        )

    def there(f):
        return pltpu.make_async_copy(
            partner.at[pl.ds(start_of(slot), 6), f],
            r.at[pl.ds(2 * core_of, 6), f, their_planes, :],
            local.at[1 + f],
        )

    def swap(n):
        half = h if n == 0 else other
        which = (slice(None) if n == 0 else n - 1, pl.ds(pl.multiple_of(half * 128, 128), 128), slice(None))
        return send(
            r.at[(pl.ds(4 - 2 * core_of, 2), *which)], r.at[(pl.ds(6 * core_of, 2), *which)],
            sw.at[n], rw.at[n], (base + 1 - core_of, pz),
        )

    def alone(act):
        pl.when(jnp.logical_not(mixed))(act)

    sideways(0).start()
    sideways(1).start()
    across(0).start()
    each(WINDOWS, lambda k: own(k, i).start(), lambda k: window(k)[0] % 15 != 0)
    sideways(0).wait_recv()
    sideways(1).wait_recv()
    even = lax.broadcasted_iota(jnp.int32, (48, 128), 1) % 2 == 0
    flat[0:48, :] = jnp.where(even, near[0], pltpu.roll(last, 1, 1))
    flat[66 * 24 : 68 * 24, :] = jnp.where(even, pltpu.roll(first, 127, 1), near[1])

    r0 = pl.multiple_of(h * 128, 128)
    bins[0] = column(fb_ref[...])
    bins[1] = column(pb_ref[...])
    mine = bins[0, pl.ds(r0, 128), :]
    masked = jnp.where(jnp.concatenate([mine, mine], axis=1) == fb_ref[...], inv_ref[pl.ds(r0, 128), :], 0.0)
    w = masked / jnp.sum(masked, axis=1, keepdims=True) * 0.0625
    w_hi = w.astype(BF16)
    ww[0:128, :] = w_hi
    ww[128:256, :] = (w - w_hi.astype(F32)).astype(BF16)

    for n in (4, 5, 1, 2, 3):
        across(n).start()
    each(WINDOWS, lambda k: own(k, i).start(), lambda k: window(k)[0] % 15 == 0)
    alone(lambda: here().start())

    def fields(c, slots, t, x0, count):
        y0 = pl.multiple_of(c * 16, 16)
        before = pl.multiple_of(jnp.maximum(y0 - 8, 0), 8)
        after = pl.multiple_of(jnp.minimum(y0 + 16, 248), 8)
        first, last = c == 0, c == 15
        u = [[r[x0 + x, f, pl.ds(y0, 16), :] for x in range(count + 2)] for f in range(3)]
        for gx in range(1, count + 1):
            up, down = [], []
            for f in range(3):
                prev = jnp.where(first, 0.0, r[x0 + gx, f, pl.ds(before, 8), :])
                succ = jnp.where(last, 0.0, r[x0 + gx, f, pl.ds(after, 8), :])
                down.append(jnp.concatenate([prev[7:], u[f][gx][:15]], axis=0))
                up.append(jnp.concatenate([u[f][gx][1:], succ[:1]], axis=0))
            out, mag = fields_of(u, gx, up, down)
            for k in range(21):
                if SLOT[k] in slots:
                    g[t, SLOT[k], x0 + gx - 1] = out[k]
            if 20 in slots:
                block = jnp.where(c // 8 == h, 2 * c - 16 * h, 16)
                mg[block, x0 + gx - 1] = mag[:8]
                mg[block + 1, x0 + gx - 1] = mag[8:]

    def box(c, slots, t, x0, count):
        y0 = pl.multiple_of(c * 16, 16)
        for k in slots:
            gs = [g[t, k, x0 + n] for n in range(count + 2)]
            pairs = [gs[n] + gs[n + 1] for n in range(count + 1)]
            for x in range(count):
                total = pairs[x] + pairs[x + 1]
                both = (pltpu.roll(total, 2, 1) + pltpu.roll(total, 126, 1)) + (total + total)
                hi = both.astype(BF16)
                at = pl.ds(pl.multiple_of((x0 + x) * 128, 128), 128)
                bh[k, pl.ds(y0, 16), at] = hi
                bl[k, pl.ds(y0, 16), at] = (both - hi.astype(F32)).astype(BF16)

    def early(t, _):
        fields(9 * h + t, range(21), 0, 0, 6)
        box(9 * h + t, range(21), 0, 0, 4)
        return 0

    def late_a(t, _):
        fields(7 * other + t, range(EARLY), t, 0, 6)
        box(7 * other + t, range(EARLY), t, 0, 4)
        return 0

    near_pair = core_of
    far_pair = 1 - core_of

    def late_b(t, _):
        fields(7 * other + t, range(EARLY, 21), t, 2 * near_pair, 4)
        box(7 * other + t, range(EARLY, 21), t, 2 * near_pair, 2)
        return 0

    def late_c(t, _):
        fields(7 * other + t, range(EARLY, 21), t, 4 * far_pair, 2)
        box(7 * other + t, range(EARLY, 21), t, 2 * far_pair, 2)
        return 0

    def products(half, slots):
        for k in slots:
            at = pl.ds(pl.multiple_of(half * 256, 256), 256)
            hi, lo = bh[k, :, at], bl[k, :, at]
            both = jnp.dot(ww[...], hi, preferred_element_type=F32)
            rest = jnp.dot(ww[0:128, :], lo, preferred_element_type=F32)
            ff[half, k] = both[:128] + (both[128:] + rest)

    def owner(k):
        return (base + xx % 2, h * 16 + mate(k))

    def goes(k):
        return True if k else mixed

    def lengths(k, t=0):
        return send(mg.at[mate(k), pl.ds(1, 4)], om_ref.at[slot], sm.at[k], rm.at[t], owner(k))

    across(0).wait_recv()
    across(4).wait_recv()
    across(5).wait_recv()
    each(WINDOWS, lambda k: theirs(0, k, i).start())
    alone(lambda: there(0).start())
    alone(lambda: here().wait())
    from_all(lambda q: own(0, q).wait_recv())
    swap(0).start()
    swap(0).wait_recv()
    lax.fori_loop(0, 7, early, 0)
    alone(lambda: there(0).wait())
    from_all(lambda q: theirs(0, 0, q).wait_recv())
    swap(1).start()
    for k in ORDER + (0,):
        pl.when(jnp.logical_and(goes(k), mate(k) // 2 != 7 * other))(lambda k=k: lengths(k, slot).start())
    across(1).wait_recv()
    each(WINDOWS, lambda k: theirs(1, k, i).start())
    alone(lambda: there(1).start())
    across(2).wait_recv()
    each(WINDOWS, lambda k: theirs(2, k, i).start(), lambda k: window(k)[0] <= 8)
    across(3).wait_recv()
    each(WINDOWS, lambda k: theirs(2, k, i).start(), lambda k: window(k)[0] > 8)
    alone(lambda: there(2).start())
    alone(lambda: there(1).wait())
    from_all(lambda q: theirs(1, 0, q).wait_recv())
    swap(2).start()
    swap(1).wait_recv()
    swap(2).wait_recv()
    lax.fori_loop(0, 9, late_a, 0)
    products(0, range(EARLY))
    products(1, range(EARLY))
    alone(lambda: there(2).wait())
    from_all(lambda q: theirs(2, 0, q).wait_recv())
    swap(3).start()
    lax.fori_loop(0, 9, late_b, 0)

    lanes = lax.broadcasted_iota(jnp.int32, (8, 128), 1)

    def contracts(half, sums):
        x0 = 2 * half

        def contract(c, sums):
            y0 = pl.multiple_of(c * 8, 8)
            lm_sum, mm_sum = 0.0, 0.0
            for x in range(2):
                f = [ff[half, SLOT[k], pl.ds(y0, 8), pl.ds(x * 128, 128)] for k in range(21)]
                a, b, d = f[0], f[1], f[2]
                t, p, m = f[3:9], f[9:15], f[15:21]
                uu = [a * a, b * b, d * d, a * b, a * d, b * d]
                fmag = 4.0 * twice_norm(t)
                lm, mm = [], []
                for k in range(6):
                    stress = p[k] - uu[k]
                    leo[c, x0 + x, k] = stress
                    mod = m[k] - fmag * t[k]
                    lm.append(stress * mod)
                    mm.append(mod * mod)
                lm_sum += lm[0] + lm[1] + lm[2] + lm[3] + lm[4] + lm[5]
                mm_sum += 2.0 * (mm[0] + mm[1] + mm[2]) + (mm[3] + mm[4] + mm[5])
            hot = bins[1, pl.ds(pl.multiple_of(r0 + y0, 8), 8), :] == lanes
            num = sums[0] + jnp.where(hot, jnp.sum(lm_sum, axis=1, keepdims=True), 0.0)
            den = sums[1] + jnp.where(hot, jnp.sum(mm_sum, axis=1, keepdims=True), 0.0)
            return num, den

        return lax.fori_loop(0, 16, contract, sums)

    def big(n, k, t=0):
        pair = pl.ds(2 * (far_pair if n else near_pair), 2)
        return send(
            leo.at[mate(k), pair], o_ref.at[slot, pair], sb.at[n, k], rb.at[n, t], owner(k)
        )

    def small(k):
        return send(part, a1.at[h * 8 + px], ss1.at[k], rs1.at[k], twin(k))

    def second(k):
        return send(s1, a2.at[i], ss2.at[k], rs2.at[k], (px, h * 16 + mate(k)))

    zero = jnp.zeros((8, 128), F32)
    products(near_pair, range(EARLY, 21))
    sums = contracts(near_pair, (zero, zero))
    swap(3).wait_recv()
    lax.fori_loop(0, 1, late_c, 0)
    for k in ORDER:
        big(0, k, slot).start()
    pl.when(mixed)(lambda: big(0, 0, slot).start())
    lax.fori_loop(1, 9, late_c, 0)
    products(far_pair, range(EARLY, 21))
    for k in ORDER + (0,):
        pl.when(jnp.logical_and(goes(k), mate(k) // 2 == 7 * other))(lambda k=k: lengths(k, slot).start())
    num, den = contracts(far_pair, sums)
    row = lax.broadcasted_iota(jnp.int32, (8, 128), 0)
    num = jnp.sum(num, axis=0, keepdims=True) * 0.25
    den = jnp.sum(den, axis=0, keepdims=True) * 0.03125
    mine = jnp.where(row == 0, num, jnp.where(row == 1, den, 0.0))
    part[...] = mine
    a1[h * 8 + px] = mine
    for n in range(6):
        across(n).wait_send()
    for n in range(2):
        sideways(n).wait_send()
    for n in range(4):
        swap(n).wait_send()
    each(range(16), lambda k: own(k).wait_send())
    for f in range(3):
        each(range(16), lambda k, f=f: theirs(f, k).wait_send())
    for k in range(1, 16):
        small(k).start()
    for k in ORDER[:6]:
        big(1, k, slot).start()
    keep_here = pltpu.make_async_copy(leo.at[i], o_ref.at[slot], local.at[0])
    alone(keep_here.start)
    keep_length = pltpu.make_async_copy(mg.at[i, pl.ds(1, 4)], om_ref.at[slot], local.at[1])
    alone(keep_length.start)
    for k in range(1, 16):
        small(k).wait_recv()
    total = a1[0]
    for q in range(1, 16):
        total = total + a1[q]
    s1[...] = total
    a2[i] = total
    for k in range(1, 16):
        small(k).wait_send()
    for k in range(1, 16):
        second(k).start()
    for k in ORDER[6:]:
        big(1, k, slot).start()
    pl.when(mixed)(lambda: big(1, 0, slot).start())
    for k in range(1, 16):
        second(k).wait_recv()
    total = a2[0]
    for q in range(1, 16):
        total = total + a2[q]
    tot_ref[...] = total
    alone(keep_here.wait)
    alone(keep_length.wait)
    for k in range(1, 16):
        second(k).wait_send()
        lengths(k).wait_send()
        for half in range(2):
            big(half, k).wait_send()
    pl.when(mixed)(lambda: lengths(0).wait_send())
    for half in range(2):
        pl.when(mixed)(lambda half=half: big(half, 0).wait_send())

    def arrive(t):
        lengths(0, t).wait_recv()
        for half in range(2):
            big(half, 0, t).wait_recv()

    for t in range(16):
        pl.when(jnp.logical_or(mixed, slot != t))(functools.partial(arrive, t))


def to_planes(tot_ref, pb_ref, o_ref, om_ref, leo_ref, visc_ref, coef_ref, mix):
    pz = lax.axis_index("pz")
    per_bin = tot_ref[0:1, :] / jnp.maximum(tot_ref[1:2, :], 65536.0)
    per_bin = jnp.broadcast_to(per_bin, (128, 128)).T
    hot = lax.broadcasted_iota(jnp.int32, (128, 256), 0) == pb_ref[...]
    both = jnp.concatenate([per_bin, per_bin], axis=1)
    coef = jnp.sum(jnp.where(hot, both, 0.0), axis=0, keepdims=True)
    coef_ref[...] = coef
    at = lax.broadcasted_iota(jnp.int32, (1, 256), 1) - pz * 8
    low = lax.broadcasted_iota(jnp.int32, (64, 128), 1) < 64
    y0 = pl.program_id(0) * 4

    def plane(t, _):
        y = y0 + t
        mine = jnp.sum(jnp.where(at == y, coef, 0.0), axis=1, keepdims=True)
        for f in range(7):
            if f < 6:
                m = o_ref[pl.ds(f * 8 + y, 64, stride=48), :]
            else:
                m = om_ref[pl.ds(y, 64, stride=8), :]
            mix[f] = jnp.concatenate([m, m], axis=0).T
            v = jnp.where(low, mix[f, pl.ds(0, 64, stride=2), :], mix[f, pl.ds(1, 64, stride=2), :])
            if f < 6:
                leo_ref[f, t] = v
            else:
                visc_ref[t] = mine * 0.5 * v
        return 0

    lax.fori_loop(0, 4, plane, 0)


def spec(space):
    return pl.BlockSpec(memory_space=space)


def params(**kw):
    return pltpu.CompilerParams(vmem_limit_bytes=56 * 1024 * 1024, **kw)


DMA = pltpu.SemaphoreType.DMA


def local_step(velocity, filter_inverse, filter_block, plane_bin):
    bins = plane_bin.reshape(1, 256)
    part = VMEM((68, 3, 8, 128), F32)
    back, lengths, total = pl.pallas_call(
        core,
        out_shape=(
            jax.ShapeDtypeStruct((16, 4, 6, 8, 128), F32),
            jax.ShapeDtypeStruct((16, 4, 8, 128), F32),
            jax.ShapeDtypeStruct((8, 128), F32),
        ),
        in_specs=[spec(VMEM)] * 4,
        out_specs=(spec(pl.ANY), spec(pl.ANY), spec(VMEM)),
        scratch_shapes=[
            part,
            part,
            VMEM((2, 48, 128), F32),
            VMEM((2, 48, 128), F32),
            VMEM((3, 128, 128), F32),
            VMEM((8, 3, 256, 128), F32),
            VMEM((9, 21, 6, 16, 128), F32),
            VMEM((21, 256, 512), BF16),
            VMEM((21, 256, 512), BF16),
            VMEM((2, 21, 128, 256), F32),
            VMEM((256, 256), BF16),
            VMEM((2, 256, 128), jnp.int32),
            VMEM((16, 4, 6, 8, 128), F32),
            VMEM((18, 6, 8, 128), F32),
            VMEM((8, 128), F32),
            VMEM((16, 8, 128), F32),
            VMEM((16, 8, 128), F32),
            VMEM((8, 128), F32),
            DMA((6,)),
            DMA((6,)),
            DMA((16,)),
            DMA((16,)),
            DMA((3, 16)),
            DMA((3, 16)),
            DMA((2,)),
            DMA((2,)),
            DMA((4,)),
            DMA((4,)),
            DMA((16,)),
            DMA((16,)),
            DMA((16,)),
            DMA((16,)),
            DMA((2, 16)),
            DMA((2, 16)),
            DMA((16,)),
            DMA((16,)),
            DMA((4,)),
        ],
        compiler_params=params(collective_id=0, has_side_effects=True),
        name="core",
    )(
        velocity,
        filter_inverse,
        filter_block.reshape(1, 256),
        bins,
    )
    leonard, viscosity, coefficient = pl.pallas_call(
        to_planes,
        out_shape=(
            jax.ShapeDtypeStruct((6, 8, 64, 128), F32),
            jax.ShapeDtypeStruct((8, 64, 128), F32),
            jax.ShapeDtypeStruct((1, 256), F32),
        ),
        grid=(2,),
        in_specs=[
            pl.BlockSpec((8, 128), lambda q: (0, 0)),
            pl.BlockSpec((1, 256), lambda q: (0, 0)),
            pl.BlockSpec((64 * 48, 128), lambda q: (0, 0)),
            pl.BlockSpec((64 * 8, 128), lambda q: (0, 0)),
        ],
        out_specs=(
            pl.BlockSpec((6, 4, 64, 128), lambda q: (0, q, 0, 0)),
            pl.BlockSpec((4, 64, 128), lambda q: (q, 0, 0)),
            pl.BlockSpec((1, 256), lambda q: (0, 0)),
        ),
        scratch_shapes=[VMEM((7, 128, 128), F32)],
        compiler_params=params(),
        name="to_planes",
    )(total, bins, back.reshape(64 * 48, 128), lengths.reshape(64 * 8, 128))
    return leonard, viscosity, coefficient.reshape(256)


def solution(mesh):
    return jax.shard_map(
        local_step,
        mesh=mesh,
        in_specs=(P(None, "pz", None, "px"), P(), P(), P()),
        out_specs=(P(None, "pz", None, "px"), P("pz", None, "px"), P()),
        check_vma=False,
    )
```
